8 devices in a mesh: dp: 2 (over z, y), sh: 4 (over x, core).
Axes of the slice: x: 2, y: 2, z: 1, core: 2. Of those that a mesh axis runs over, the one named last changes fastest.
Arguments:
- k_prefill: bfloat16 [24, 10240, 4, 256], P('dp', None, 'sh'), parts along dimension 0
- v_prefill: bfloat16 [24, 10240, 4, 256], P('dp', None, 'sh'), parts along dimension 0
- lengths: int32 [24], P('dp'), parts along dimension 0
- residual: bfloat16 [24, 2304], P(('dp', 'sh')), parts along dimension 0
- norm_gain: bfloat16 [2304], replicated
- w_query: bfloat16 [2304, 2048], replicated
- w_key: bfloat16 [2304, 1024], replicated
- w_value: bfloat16 [2304, 1024], replicated
- w_out: bfloat16 [2048, 2304], replicated
Outputs:
- output 1: bfloat16 [24, 2304], P(('dp', 'sh')), parts along dimension 0
- output 2: bfloat16 [24, 4096, 4, 256], P(('dp', 'sh')), parts along dimension 0
- output 3: bfloat16 [24, 4096, 4, 256], P(('dp', 'sh')), parts along dimension 0
There are 2 independent parts. The reference program is written for one: setup_inputs(seed, part) draws one part's arguments, and reference() takes and returns one part's arrays. A program takes and returns all parts, laid end to end along the dimension named above; an argument that names none is the same for every part.
All inputs are finite; a program needn't handle non-finite values.
Results may differ from the reference program's by a relative error of at most 0.0047.
Values are sent between devices in bfloat16 or wider.
A program may use at most 1 GiB of HBM per device.

```python
import jax
import jax.numpy as jnp
from jax import lax

MODEL_DIM = 2304
HEADS = 8
KV_HEADS = 4
HEAD_DIM = 256
WINDOW = 4096
SEQ_LEN = 10240
BATCH = 12
Q_GROUP = HEADS // KV_HEADS
Q_WIDTH = HEADS * HEAD_DIM
KV_WIDTH = KV_HEADS * HEAD_DIM
THETA = 10000.0
EPS = 1e-5


def setup_inputs(seed: int = 0, part: int = 0) -> dict:
    root_key = jax.random.key(seed)
    part_root, shared_root = jax.random.split(root_key)
    part_keys = jax.random.split(jax.random.fold_in(part_root, part), 4)
    shared_keys = jax.random.split(shared_root, 5)
    kv_shape = (BATCH, SEQ_LEN, KV_HEADS, HEAD_DIM)
    k_prefill = jax.random.normal(part_keys[0], kv_shape, jnp.float32).astype(jnp.bfloat16)
    v_prefill = jax.random.normal(part_keys[1], kv_shape, jnp.float32).astype(jnp.bfloat16)
    lengths = jax.random.randint(part_keys[2], (BATCH,), 1, SEQ_LEN + 1, dtype=jnp.int32)
    lengths = lengths.at[0].set(SEQ_LEN).at[1].set(1)
    residual = jax.random.normal(part_keys[3], (BATCH, MODEL_DIM), jnp.float32).astype(jnp.bfloat16)
    norm_gain = (1.0 + 0.3 * jax.random.normal(shared_keys[0], (MODEL_DIM,), jnp.float32)).astype(jnp.bfloat16)
    w_query = (jax.random.normal(shared_keys[1], (MODEL_DIM, Q_WIDTH), jnp.float32) * (2.0 / MODEL_DIM ** 0.5)).astype(jnp.bfloat16)
    w_key = (jax.random.normal(shared_keys[2], (MODEL_DIM, KV_WIDTH), jnp.float32) * (3.0 / MODEL_DIM ** 0.5)).astype(jnp.bfloat16)
    w_value = (jax.random.normal(shared_keys[3], (MODEL_DIM, KV_WIDTH), jnp.float32) * (3.0 / MODEL_DIM ** 0.5)).astype(jnp.bfloat16)
    w_out = (jax.random.normal(shared_keys[4], (Q_WIDTH, MODEL_DIM), jnp.float32) * (2.0 / Q_WIDTH ** 0.5)).astype(jnp.bfloat16)
    return {'k_prefill': k_prefill, 'v_prefill': v_prefill, 'lengths': lengths, 'residual': residual, 'norm_gain': norm_gain, 'w_query': w_query, 'w_key': w_key, 'w_value': w_value, 'w_out': w_out}


def rolling_cache(prefill, lengths):
    slot_ids = jnp.arange(WINDOW, dtype=jnp.int32)
    last_pos = lengths[:, None] - 1
    held_pos = last_pos - jnp.remainder(last_pos - slot_ids[None, :], WINDOW)
    held = jax.vmap(lambda row_vals, row_idx: jnp.take(row_vals, row_idx, axis=0))(prefill, jnp.maximum(held_pos, 0))
    return jnp.where((held_pos >= 0)[:, :, None, None], held, jnp.zeros((), prefill.dtype))


def rotate(heads, positions):
    half_dim = HEAD_DIM // 2
    inv_freq = THETA ** (-2.0 * jnp.arange(half_dim, dtype=jnp.float32) / HEAD_DIM)
    angles = positions.astype(jnp.float32).reshape(positions.shape + (1,) * (heads.ndim - 1)) * inv_freq
    cos_part = jnp.cos(angles)
    sin_part = jnp.sin(angles)
    first_half = heads[..., :half_dim].astype(jnp.float32)
    second_half = heads[..., half_dim:].astype(jnp.float32)
    return jnp.concatenate([first_half * cos_part - second_half * sin_part, second_half * cos_part + first_half * sin_part], axis=-1).astype(jnp.bfloat16)


def attend_row(row_args):
    q_row, k_row, v_row, live_row = row_args
    q_grouped = q_row.reshape(KV_HEADS, Q_GROUP, HEAD_DIM).astype(jnp.float32)
    scores = jnp.einsum('kgd,wkd->kgw', q_grouped, k_row.astype(jnp.float32)) / HEAD_DIM ** 0.5
    scores = jnp.where(live_row[None, None, :], scores, -jnp.inf)
    weights = jax.nn.softmax(scores, axis=-1).astype(jnp.bfloat16)
    mixed = jnp.einsum('kgw,wkd->kgd', weights.astype(jnp.float32), v_row.astype(jnp.float32))
    return mixed.astype(jnp.bfloat16).reshape(Q_WIDTH)


def reference(k_prefill, v_prefill, lengths, residual, norm_gain, w_query, w_key, w_value, w_out):
    k_cache = rolling_cache(k_prefill, lengths)
    v_cache = rolling_cache(v_prefill, lengths)
    resid_f32 = residual.astype(jnp.float32)
    inv_rms = lax.rsqrt(jnp.mean(resid_f32 * resid_f32, axis=-1, keepdims=True) + EPS)
    normed = (resid_f32 * inv_rms * norm_gain.astype(jnp.float32)).astype(jnp.bfloat16)
    q_heads = jnp.dot(normed, w_query, preferred_element_type=jnp.float32).astype(jnp.bfloat16).reshape(BATCH, HEADS, HEAD_DIM)
    k_new = jnp.dot(normed, w_key, preferred_element_type=jnp.float32).astype(jnp.bfloat16).reshape(BATCH, KV_HEADS, HEAD_DIM)
    v_new = jnp.dot(normed, w_value, preferred_element_type=jnp.float32).astype(jnp.bfloat16).reshape(BATCH, KV_HEADS, HEAD_DIM)
    q_heads = rotate(q_heads, lengths)
    k_new = rotate(k_new, lengths)
    slot_ids = jnp.arange(WINDOW, dtype=jnp.int32)
    new_slot = (slot_ids[None, :] == (lengths % WINDOW)[:, None])[:, :, None, None]
    k_cache = jnp.where(new_slot, k_new[:, None], k_cache)
    v_cache = jnp.where(new_slot, v_new[:, None], v_cache)
    live_slot = (lengths[:, None] - jnp.remainder(lengths[:, None] - slot_ids[None, :], WINDOW)) >= 0
    attn_out = lax.map(attend_row, (q_heads, k_cache, v_cache, live_slot))
    resid_out = (resid_f32 + jnp.dot(attn_out, w_out, preferred_element_type=jnp.float32)).astype(jnp.bfloat16)
    return (resid_out, k_cache, v_cache)
```

```python
import functools

import jax
import jax.numpy as jnp
from jax import lax
from jax.experimental import pallas as pl
from jax.experimental.pallas import tpu as pltpu
from jax.sharding import PartitionSpec as P

WINDOW = 4096
THETA = 10000.0
EPS = 1e-5
BLK = 16
CHUNK = 512
CB = CHUNK // BLK
NCH = WINDOW // CHUNK


def rotate(heads, positions):
    head_dim = heads.shape[-1]
    half_dim = head_dim // 2
    inv_freq = THETA ** (-2.0 * jnp.arange(half_dim, dtype=jnp.float32) / head_dim)
    angles = positions.astype(jnp.float32).reshape(positions.shape + (1,) * (heads.ndim - 1)) * inv_freq
    cos_part = jnp.cos(angles)
    sin_part = jnp.sin(angles)
    first_half = heads[..., :half_dim].astype(jnp.float32)
    second_half = heads[..., half_dim:].astype(jnp.float32)
    return jnp.concatenate([first_half * cos_part - second_half * sin_part, second_half * cos_part + first_half * sin_part], axis=-1).astype(jnp.bfloat16)


def blank(shape, dtype):
    return pl.pallas_call(
        lambda o_ref: None,
        out_shape=jax.ShapeDtypeStruct(shape, dtype),
        out_specs=pl.BlockSpec(memory_space=pl.ANY),
        name="blank",
    )()


def pick_kernel(ways, n_ref, me_ref, *refs):
    x_refs, y_refs, o_refs = refs[:ways], refs[ways:2 * ways], refs[-ways:]
    c = pl.program_id(0)
    s0 = c * CHUNK
    for d in range(ways):
        n = n_ref[d]
        lap, m = n // WINDOW, lax.rem(n, WINDOW)
        cb = m // CHUNK

        @pl.when((c != cb) & ((c < cb) | (lap >= 1)))
        def _():
            o_refs[d][...] = x_refs[d][0]

        @pl.when((c > cb) & (lap == 0))
        def _():
            o_refs[d][...] = jnp.zeros(o_refs[d].shape, o_refs[d].dtype)

        @pl.when(c == cb)
        def _():
            shape = (CB, BLK, 256)
            slots = s0 + BLK * lax.broadcasted_iota(jnp.int32, shape, 0) + lax.broadcasted_iota(jnp.int32, shape, 1)
            old = jnp.where(lap >= 1, y_refs[d][0].astype(jnp.float32), 0.0)
            o_refs[d][...] = jnp.where(slots < m, x_refs[d][0].astype(jnp.float32), old).astype(jnp.bfloat16)


def pick(prefill, lens, rows, after):
    ways = rows.shape[0]
    seq_blocks = prefill.shape[1]

    def x_map(d):
        def index(c, n_ref, r_ref):
            n = n_ref[d]
            lap, m = n // WINDOW, lax.rem(n, WINDOW)
            from_lap = jnp.where(c <= m // CHUNK, lap, jnp.maximum(lap - 1, 0))
            return r_ref[d], jnp.minimum(from_lap * NCH + c, seq_blocks // CB - 1), 0, 0
        return pl.BlockSpec((1, CB, BLK, 256), index)

    def y_map(d):
        def index(c, n_ref, r_ref):
            n = n_ref[d]
            lap, m = n // WINDOW, lax.rem(n, WINDOW)
            return r_ref[d], jnp.maximum(lap - 1, 0) * NCH + m // CHUNK, 0, 0
        return pl.BlockSpec((1, CB, BLK, 256), index)

    return pl.pallas_call(
        functools.partial(pick_kernel, ways),
        grid_spec=pltpu.PrefetchScalarGridSpec(
            num_scalar_prefetch=2,
            grid=(NCH,),
            in_specs=[x_map(d) for d in range(ways)] + [y_map(d) for d in range(ways)] + [pl.BlockSpec(memory_space=pl.ANY)] * len(after),
            out_specs=[pl.BlockSpec((CB, BLK, 256), lambda c, n_ref, r_ref: (c, 0, 0))] * ways,
        ),
        out_shape=[jax.ShapeDtypeStruct((WINDOW // BLK, BLK, 256), prefill.dtype)] * ways,
        compiler_params=pltpu.CompilerParams(dimension_semantics=("arbitrary",), vmem_limit_bytes=60 * 1024 * 1024),
        cost_estimate=pl.CostEstimate(flops=1_000_000, bytes_accessed=16_000_000, transcendentals=0),
        name="pick",
    )(lens, rows, *([prefill] * (2 * ways)), *after)


def assemble_kernel(is_key, ways, n_ref, me_ref, *refs):
    x_refs = refs[:ways]
    new_ref, qp_ref, _, cache_ref, res_ref, acc = refs[ways:]
    c = pl.program_id(0)
    s0 = c * CHUNK
    me = me_ref[0]
    n = n_ref[0]
    lap, m = n // WINDOW, lax.rem(n, WINDOW)

    @pl.when((s0 <= m) & (m < s0 + CHUNK))
    def _():
        b = (m - s0) // BLK
        here = lax.broadcasted_iota(jnp.int32, (BLK, 256), 0) == lax.rem(m, BLK)
        for d in range(ways):
            new = jnp.broadcast_to(new_ref[me ^ d], (BLK, 256))
            x_refs[d][b] = jnp.where(here, new, x_refs[d][b].astype(jnp.float32)).astype(jnp.bfloat16)

    xs = [x_refs[d][...].reshape(CHUNK, 256) for d in range(ways)]
    if is_key:
        cols = s0 + lax.broadcasted_iota(jnp.int32, (8, CHUNK), 1)
        live = (lap >= 1) | (cols <= n)
        for d in range(ways):
            s = lax.dot_general(qp_ref[me ^ d], xs[d], (((1,), (1,)), ((), ())), preferred_element_type=jnp.float32)
            res_ref[me ^ d] = jnp.where(live, s / 16.0, -jnp.inf)
    else:
        @pl.when(c == 0)
        def _():
            acc[...] = jnp.zeros_like(acc)

        for d in range(ways):
            acc[me ^ d] += jnp.dot(qp_ref[me ^ d], xs[d], preferred_element_type=jnp.float32)

        @pl.when(c == NCH - 1)
        def _():
            res_ref[...] = acc[...]

    for bit in (1, 2):
        swap = (me & bit) != 0
        xs = [jnp.where(swap, xs[h ^ bit], xs[h]) for h in range(ways)]
    cache_ref[0] = jnp.stack(xs, axis=1)


def assemble(is_key, row, n, me, parts, new, qp, cache):
    ways = len(parts)
    whole = lambda *shape: pl.BlockSpec(shape, lambda c, n_ref, me_ref: (0,) * len(shape))
    by_chunk = pl.BlockSpec((ways, 8, CHUNK), lambda c, n_ref, me_ref: (0, 0, c))
    if is_key:
        qp_spec = whole(ways, 8, 256)
        res_shape, res_spec = jax.ShapeDtypeStruct((ways, 8, WINDOW), jnp.float32), by_chunk
    else:
        qp_spec = by_chunk
        res_shape, res_spec = jax.ShapeDtypeStruct((ways, 8, 256), jnp.float32), whole(ways, 8, 256)
    return pl.pallas_call(
        functools.partial(assemble_kernel, is_key, ways),
        grid_spec=pltpu.PrefetchScalarGridSpec(
            num_scalar_prefetch=2,
            grid=(NCH,),
            in_specs=[pl.BlockSpec((CB, BLK, 256), lambda c, n_ref, me_ref: (c, 0, 0))] * ways + [whole(ways, 1, 256), qp_spec, pl.BlockSpec(memory_space=pl.ANY)],
            out_specs=[pl.BlockSpec((1, CHUNK, ways, 256), lambda c, n_ref, me_ref: (row, c, 0, 0)), res_spec],
            scratch_shapes=[pltpu.VMEM((ways, 8, 256), jnp.float32)],
        ),
        out_shape=[jax.ShapeDtypeStruct(cache.shape, cache.dtype), res_shape],
        input_output_aliases={2 + ways + 2: 0},
        compiler_params=pltpu.CompilerParams(dimension_semantics=("arbitrary",), vmem_limit_bytes=60 * 1024 * 1024),
        cost_estimate=pl.CostEstimate(flops=20_000_000_000, bytes_accessed=16_000_000, transcendentals=0),
        name="assemble_keys" if is_key else "assemble_values",
    )(n, me, *parts, new, qp, cache)


def solution(mesh):
    head_spec = P('dp', None, 'sh', None)
    row_spec = P(('dp', 'sh'))
    full_spec = P(None, None)
    ways = mesh.shape['sh']

    def per_device(k_prefill, v_prefill, lengths, residual, norm_gain, w_query, w_key, w_value, w_out):
        num_rows = residual.shape[0]
        all_rows, seq = k_prefill.shape[0], k_prefill.shape[1]
        heads = ways
        me = lax.axis_index('sh').astype(jnp.int32)
        my_lengths = lax.dynamic_slice_in_dim(lengths, me * num_rows, num_rows)
        peers = me ^ jnp.arange(ways, dtype=jnp.int32)
        k_blocks = k_prefill.reshape(all_rows, seq // BLK, BLK, 256)
        v_blocks = v_prefill.reshape(all_rows, seq // BLK, BLK, 256)

        stages = []
        for is_key in (True, False):
            for r in range(num_rows):
                rows = peers * num_rows + r
                after = list(stages[-2][1:]) if len(stages) >= 2 else []
                sent = pick(k_blocks if is_key else v_blocks, lengths[rows], rows, after)
                got = [sent[0]] + [lax.ppermute(sent[d], 'sh', [(i, i ^ d) for i in range(ways)]) for d in range(1, ways)]
                stages.append(got)

        resid_f32 = residual.astype(jnp.float32)
        inv_rms = lax.rsqrt(jnp.mean(resid_f32 * resid_f32, axis=-1, keepdims=True) + EPS)
        normed = (resid_f32 * inv_rms * norm_gain.astype(jnp.float32)).astype(jnp.bfloat16)
        q_group = w_query.shape[1] // (heads * 256)
        q_heads = jnp.dot(normed, w_query, preferred_element_type=jnp.float32).astype(jnp.bfloat16).reshape(num_rows, heads, q_group, 256)
        k_new = jnp.dot(normed, w_key, preferred_element_type=jnp.float32).astype(jnp.bfloat16).reshape(num_rows, heads, 256)
        v_new = jnp.dot(normed, w_value, preferred_element_type=jnp.float32).astype(jnp.bfloat16).reshape(num_rows, heads, 256)
        q_heads = rotate(q_heads, my_lengths)
        k_new = rotate(k_new, my_lengths)
        k_new, v_new = k_new.astype(jnp.float32)[:, :, None], v_new.astype(jnp.float32)[:, :, None]
        q_pad = jnp.pad(q_heads, ((0, 0), (0, 0), (0, 8 - q_group), (0, 0)))

        me1 = me.reshape(1)
        cache_shape = (num_rows, WINDOW, heads, 256)
        k_cache, v_cache = blank(cache_shape, jnp.bfloat16), blank(cache_shape, jnp.bfloat16)
        weights, attn = [], []
        for r in range(num_rows):
            k_cache, scores = assemble(True, r, my_lengths[r:r + 1], me1, stages[r], k_new[r], q_pad[r], k_cache)
            exp_scores = jnp.exp(scores - jnp.max(scores, axis=-1, keepdims=True))
            weights.append((exp_scores / jnp.sum(exp_scores, axis=-1, keepdims=True)).astype(jnp.bfloat16))
        for r in range(num_rows):
            v_cache, mixed = assemble(False, r, my_lengths[r:r + 1], me1, stages[num_rows + r], v_new[r], weights[r], v_cache)
            attn.append(mixed[:, :q_group].astype(jnp.bfloat16).reshape(1, heads * q_group * 256))
        attn_out = jnp.concatenate(attn, axis=0)
        resid_out = (resid_f32 + jnp.dot(attn_out, w_out, preferred_element_type=jnp.float32)).astype(jnp.bfloat16)
        return resid_out, k_cache, v_cache
    return jax.shard_map(per_device, mesh=mesh, in_specs=(head_spec, head_spec, P('dp'), P(('dp', 'sh'), None), P(None), full_spec, full_spec, full_spec, full_spec), out_specs=(P(('dp', 'sh'), None), row_spec, row_spec), check_vma=False)
```

```python
import functools

import jax
import jax.numpy as jnp
from jax import lax
from jax.experimental import pallas as pl
from jax.experimental.pallas import tpu as pltpu
from jax.sharding import PartitionSpec as P


WINDOW = 4096
THETA = 10000.0
EPS = 1e-5
BLK = 16
CHUNK = 512
CB = CHUNK // BLK
NCH = WINDOW // CHUNK
PLAN = (
    (True, 0, 0, 1), (True, 0, 1, 3), (True, 0, 4, 4), (True, 1, 0, 4), (True, 1, 4, 4), (True, 2, 0, 4), (True, 2, 4, 4),
    (False, 0, 0, 4), (False, 0, 4, 4), (False, 1, 0, 4), (False, 1, 4, 4), (False, 2, 0, 4), (False, 2, 4, 2), (False, 2, 6, 1), (False, 2, 7, 1),
)


def rotate(heads, positions):
    head_dim = heads.shape[-1]
    half_dim = head_dim // 2
    inv_freq = THETA ** (-2.0 * jnp.arange(half_dim, dtype=jnp.float32) / head_dim)
    angles = positions.astype(jnp.float32).reshape(positions.shape + (1,) * (heads.ndim - 1)) * inv_freq
    cos_part = jnp.cos(angles)
    sin_part = jnp.sin(angles)
    first_half = heads[..., :half_dim].astype(jnp.float32)
    second_half = heads[..., half_dim:].astype(jnp.float32)
    return jnp.concatenate([first_half * cos_part - second_half * sin_part, second_half * cos_part + first_half * sin_part], axis=-1).astype(jnp.bfloat16)


def blank(shape, dtype):
    return pl.pallas_call(
        lambda o_ref: None,
        out_shape=jax.ShapeDtypeStruct(shape, dtype),
        out_specs=pl.BlockSpec(memory_space=pl.ANY),
        name="blank",
    )()


def pick_kernel(ways, first, n_ref, r_ref, *refs):
    x_refs, y_refs, o_refs = refs[:ways], refs[ways:2 * ways], refs[-ways:]
    c = first + pl.program_id(0)
    s0 = c * CHUNK
    for d in range(ways):
        n = n_ref[d]
        lap, m = n // WINDOW, lax.rem(n, WINDOW)
        cb = m // CHUNK

        @pl.when((c != cb) & ((c < cb) | (lap >= 1)))
        def _():
            o_refs[d][...] = x_refs[d][0]

        @pl.when((c > cb) & (lap == 0))
        def _():
            o_refs[d][...] = jnp.zeros(o_refs[d].shape, o_refs[d].dtype)

        @pl.when(c == cb)
        def _():
            shape = (CB, BLK, 256)
            slots = s0 + BLK * lax.broadcasted_iota(jnp.int32, shape, 0) + lax.broadcasted_iota(jnp.int32, shape, 1)
            old = jnp.where(lap >= 1, y_refs[d][0].astype(jnp.float32), 0.0)
            o_refs[d][...] = jnp.where(slots < m, x_refs[d][0].astype(jnp.float32), old).astype(jnp.bfloat16)


def pick(prefill, lens, rows, first, count):
    ways = rows.shape[0]
    seq_blocks = prefill.shape[1]

    def x_map(d):
        def index(i, n_ref, r_ref):
            c, n = first + i, n_ref[d]
            lap, m = n // WINDOW, lax.rem(n, WINDOW)
            from_lap = jnp.where(c <= m // CHUNK, lap, jnp.maximum(lap - 1, 0))
            return r_ref[d], jnp.minimum(from_lap * NCH + c, seq_blocks // CB - 1), 0, 0

        return pl.BlockSpec((1, CB, BLK, 256), index)

    def y_map(d):
        def index(i, n_ref, r_ref):
            n = n_ref[d]
            lap, m = n // WINDOW, lax.rem(n, WINDOW)
            return r_ref[d], jnp.maximum(lap - 1, 0) * NCH + m // CHUNK, 0, 0

        return pl.BlockSpec((1, CB, BLK, 256), index)

    return pl.pallas_call(
        functools.partial(pick_kernel, ways, first),
        grid_spec=pltpu.PrefetchScalarGridSpec(
            num_scalar_prefetch=2,
            grid=(count,),
            in_specs=[x_map(d) for d in range(ways)] + [y_map(d) for d in range(ways)],
            out_specs=[pl.BlockSpec((CB, BLK, 256), lambda i, n_ref, r_ref: (i, 0, 0))] * ways,
        ),
        out_shape=[jax.ShapeDtypeStruct((count * CB, BLK, 256), prefill.dtype)] * ways,
        compiler_params=pltpu.CompilerParams(dimension_semantics=("arbitrary",), vmem_limit_bytes=67_043_328),
        cost_estimate=pl.CostEstimate(flops=10_000_000, bytes_accessed=count * 4_000_000, transcendentals=0),
        name="pick",
    )(lens, rows, *([prefill] * (2 * ways)))


def assemble_kernel(is_key, ways, first, count, n_ref, me_ref, *refs):
    x_refs = refs[:ways]
    new_ref, qp_ref, prev_ref, _, _, cache_ref, res_ref, acc, mix = refs[ways:ways + 9]
    i = pl.program_id(0)
    s0 = (first + i) * CHUNK
    me = me_ref[0]
    n = n_ref[0]
    lap, m = n // WINDOW, lax.rem(n, WINDOW)

    @pl.when((s0 <= m) & (m < s0 + CHUNK))
    def _():
        b = (m - s0) // BLK
        here = lax.broadcasted_iota(jnp.int32, (BLK, 256), 0) == lax.rem(m, BLK)
        for d in range(ways):
            new = jnp.broadcast_to(new_ref[me ^ d], (BLK, 256))
            x_refs[d][b] = jnp.where(here, new, x_refs[d][b].astype(jnp.float32)).astype(jnp.bfloat16)

    xs = [x_refs[d][...].reshape(CHUNK, 256) for d in range(ways)]
    if is_key:
        cols = s0 + lax.broadcasted_iota(jnp.int32, (8, CHUNK), 1)
        live = (lap >= 1) | (cols <= n)
        for d in range(ways):
            s = lax.dot_general(qp_ref[me ^ d], xs[d], (((1,), (1,)), ((), ())), preferred_element_type=jnp.float32)
            res_ref[me ^ d] = jnp.where(live, s / 16.0, -jnp.inf)
    else:
        @pl.when(i == 0)
        def _():
            acc[...] = prev_ref[...]

        for d in range(ways):
            acc[me ^ d] += jnp.dot(qp_ref[me ^ d], xs[d], preferred_element_type=jnp.float32)

        @pl.when(i == count - 1)
        def _():
            res_ref[...] = acc[...]

    for d in range(ways):
        x = xs[d].astype(jnp.float32)
        for half in range(2):
            mix[half, pl.ds(me ^ d, CHUNK, stride=ways), :] = x[:, half * 128:(half + 1) * 128]
    joined = jnp.concatenate([mix[half].astype(jnp.bfloat16) for half in range(2)], axis=1)
    cache_ref[0] = joined.reshape(CHUNK, ways, 256)


def assemble(is_key, row, first, n, me, parts, new, qp, prev, cache, after):
    ways = len(parts)
    count = parts[0].shape[0] // CB
    whole = lambda *shape: pl.BlockSpec(shape, lambda i, n_ref, me_ref: (0,) * len(shape))
    by_chunk = pl.BlockSpec((ways, 8, CHUNK), lambda i, n_ref, me_ref: (0, 0, first + i))
    anywhere = pl.BlockSpec(memory_space=pl.ANY)
    if is_key:
        qp_spec, prev_spec, res_spec = whole(ways, 8, 256), anywhere, by_chunk
    else:
        qp_spec, prev_spec, res_spec = by_chunk, whole(ways, 8, 256), whole(ways, 8, 256)
    aliases = {2 + ways + 3: 0}
    if is_key:
        aliases[2 + ways + 2] = 1
    return pl.pallas_call(
        functools.partial(assemble_kernel, is_key, ways, first, count),
        grid_spec=pltpu.PrefetchScalarGridSpec(
            num_scalar_prefetch=2,
            grid=(count,),
            in_specs=[pl.BlockSpec((CB, BLK, 256), lambda i, n_ref, me_ref: (i, 0, 0))] * ways + [whole(ways, 1, 256), qp_spec, prev_spec, anywhere, anywhere],
            out_specs=[pl.BlockSpec((1, CHUNK, ways, 256), lambda i, n_ref, me_ref: (row, first + i, 0, 0)), res_spec],
            scratch_shapes=[pltpu.VMEM((ways, 8, 256), jnp.float32), pltpu.VMEM((2, ways * CHUNK, 128), jnp.float32)],
        ),
        out_shape=[jax.ShapeDtypeStruct(cache.shape, cache.dtype), jax.ShapeDtypeStruct(prev.shape, prev.dtype)],
        input_output_aliases=aliases,
        compiler_params=pltpu.CompilerParams(dimension_semantics=("arbitrary",), vmem_limit_bytes=67_043_328),
        cost_estimate=pl.CostEstimate(flops=10_000_000, bytes_accessed=count * 4_000_000, transcendentals=0),
        name="assemble_keys" if is_key else "assemble_values",
    )(n, me, *parts, new, qp, prev, cache, after)


def solution(mesh):
    head_spec = P('dp', None, 'sh', None)
    row_spec = P(('dp', 'sh'))
    full_spec = P(None, None)
    ways = mesh.shape['sh']

    def step(k_prefill, v_prefill, lengths, residual, norm_gain, w_query, w_key, w_value, w_out):
        num_rows = residual.shape[0]
        all_rows, seq = k_prefill.shape[0], k_prefill.shape[1]
        heads = ways
        me = lax.axis_index('sh').astype(jnp.int32)
        my_lengths = lax.dynamic_slice_in_dim(lengths, me * num_rows, num_rows)
        peers = me ^ jnp.arange(ways, dtype=jnp.int32)
        k_blocks = k_prefill.reshape(all_rows, seq // BLK, BLK, 256)
        v_blocks = v_prefill.reshape(all_rows, seq // BLK, BLK, 256)

        stages = []
        for is_key, r, first, count in PLAN:
            rows = peers * num_rows + r
            sent = pick(k_blocks if is_key else v_blocks, lengths[rows], rows, first, count)
            got = [sent[0]]
            for d in range(1, ways):
                got.append(lax.ppermute(sent[d], 'sh', [(i, i ^ d) for i in range(ways)]))
            stages.append(got)
        last_sent = sent[0]

        resid_f32 = residual.astype(jnp.float32)
        inv_rms = lax.rsqrt(jnp.mean(resid_f32 * resid_f32, axis=-1, keepdims=True) + EPS)
        normed = (resid_f32 * inv_rms * norm_gain.astype(jnp.float32)).astype(jnp.bfloat16)
        q_group = w_query.shape[1] // (heads * 256)
        q_heads = jnp.dot(normed, w_query, preferred_element_type=jnp.float32).astype(jnp.bfloat16).reshape(num_rows, heads, q_group, 256)
        k_new = jnp.dot(normed, w_key, preferred_element_type=jnp.float32).astype(jnp.bfloat16).reshape(num_rows, heads, 256)
        v_new = jnp.dot(normed, w_value, preferred_element_type=jnp.float32).astype(jnp.bfloat16).reshape(num_rows, heads, 256)
        q_heads = rotate(q_heads, my_lengths)
        k_new = rotate(k_new, my_lengths)
        k_new, v_new = k_new.astype(jnp.float32)[:, :, None], v_new.astype(jnp.float32)[:, :, None]
        q_pad = jnp.pad(q_heads, ((0, 0), (0, 0), (0, 8 - q_group), (0, 0)))

        me1 = me.reshape(1)
        cache_shape = (num_rows, WINDOW, heads, 256)
        k_cache, v_cache = blank(cache_shape, jnp.bfloat16), blank(cache_shape, jnp.bfloat16)
        scores = [blank((heads, 8, WINDOW), jnp.float32) for _ in range(num_rows)]
        sums = [jnp.zeros((heads, 8, 256), jnp.float32) for _ in range(num_rows)]
        weights = [None] * num_rows
        for (is_key, r, first, count), got in zip(PLAN, stages):
            if is_key:
                k_cache, scores[r] = assemble(True, r, first, my_lengths[r:r + 1], me1, got, k_new[r], q_pad[r], scores[r], k_cache, last_sent)
                if first + count == NCH:
                    exp_scores = jnp.exp(scores[r] - jnp.max(scores[r], axis=-1, keepdims=True))
                    weights[r] = (exp_scores / jnp.sum(exp_scores, axis=-1, keepdims=True)).astype(jnp.bfloat16)
            else:
                v_cache, sums[r] = assemble(False, r, first, my_lengths[r:r + 1], me1, got, v_new[r], weights[r], sums[r], v_cache, last_sent)
        attn = [x[:, :q_group].astype(jnp.bfloat16).reshape(1, heads * q_group * 256) for x in sums]
        attn_out = jnp.concatenate(attn, axis=0)
        resid_out = (resid_f32 + jnp.dot(attn_out, w_out, preferred_element_type=jnp.float32)).astype(jnp.bfloat16)
        return resid_out, k_cache, v_cache

    return jax.shard_map(step, mesh=mesh, in_specs=(head_spec, head_spec, P('dp'), P(('dp', 'sh'), None), P(None), full_spec, full_spec, full_spec, full_spec), out_specs=(P(('dp', 'sh'), None), row_spec, row_spec), check_vma=False)
```

```python
import functools

import jax
import jax.numpy as jnp
from jax import lax
from jax.experimental import pallas as pl
from jax.experimental.pallas import tpu as pltpu
from jax.sharding import PartitionSpec as P


WINDOW = 4096
THETA = 10000.0
EPS = 1e-5
GRAN = 64
WIN_G = WINDOW // GRAN
STEP = 8
FIXED = 128
UNITS = (32, 16, 8, 8)
SPARE = sum(UNITS)
LEVELS = SPARE // 8 + 1
K_PIECES = (8, 24, 96)
V_PIECES = (64, 32, 16, 8, 8)
WAYS, ROWS = 4, 3
VMEM_LIMIT = 67_043_328
ANYWHERE = pl.BlockSpec(memory_space=pl.ANY)


def starts_of(sizes):
    return [sum(sizes[:i]) for i in range(len(sizes))]


def active_units(level):
    full = level == LEVELS - 1
    return [full | (((level >> 2) & 1) == 1), full | (((level >> 1) & 1) == 1), full | ((level & 1) == 1), full]


def rotate(heads, positions):
    head_dim = heads.shape[-1]
    half_dim = head_dim // 2
    inv_freq = THETA ** (-2.0 * jnp.arange(half_dim, dtype=jnp.float32) / head_dim)
    angles = positions.astype(jnp.float32).reshape(positions.shape + (1,) * (heads.ndim - 1)) * inv_freq
    cos_part = jnp.cos(angles)
    sin_part = jnp.sin(angles)
    first_half = heads[..., :half_dim].astype(jnp.float32)
    second_half = heads[..., half_dim:].astype(jnp.float32)
    return jnp.concatenate([first_half * cos_part - second_half * sin_part, second_half * cos_part + first_half * sin_part], axis=-1).astype(jnp.bfloat16)


def blank(shape, dtype):
    return pl.pallas_call(
        lambda o_ref: None,
        out_shape=jax.ShapeDtypeStruct(shape, dtype),
        out_specs=ANYWHERE,
        name="blank",
    )()


def cleared_kernel(n_ref, k_ref, v_ref, zeros, sem):
    zeros[...] = jnp.zeros_like(zeros)

    def each(act):
        for r in range(ROWS):
            def one(g, carry):
                for ref in (k_ref, v_ref):
                    act(pltpu.make_async_copy(zeros, ref.at[r, pl.ds(g * GRAN, GRAN)], sem))
                return carry

            lax.fori_loop(jnp.minimum(n_ref[r] // GRAN + 1, WIN_G), WIN_G, one, 0)

    each(lambda copy: copy.start())
    each(lambda copy: copy.wait())


def cleared(n, shape):
    return pl.pallas_call(
        cleared_kernel,
        grid_spec=pltpu.PrefetchScalarGridSpec(
            num_scalar_prefetch=1, grid=(1,), in_specs=[], out_specs=[ANYWHERE, ANYWHERE],
            scratch_shapes=[pltpu.VMEM((GRAN, WAYS, 256), jnp.bfloat16), pltpu.SemaphoreType.DMA]),
        out_shape=[jax.ShapeDtypeStruct(shape, jnp.bfloat16)] * 2,
        compiler_params=pltpu.CompilerParams(vmem_limit_bytes=VMEM_LIMIT),
        cost_estimate=pl.CostEstimate(flops=10_000_000, bytes_accessed=20_000_000, transcendentals=0),
        name="cleared",
    )(n)


class Lists:
    def __init__(self, n, row0, seq_g):
        self.n, self.row0, self.seq_g = n, row0, seq_g
        self.lap = n // WINDOW
        self.cut = n % WINDOW
        width = jnp.minimum(n // GRAN + 1, WIN_G)
        self.off1 = width[..., 0:1]
        self.off2 = self.off1 + width[..., 1:2]
        self.size = self.off2 + width[..., 2:3]

    def of_row(self, x, r):
        return jnp.where(r == 0, x[..., 0:1], jnp.where(r == 1, x[..., 1:2], x[..., 2:3]))

    def at(self, i):
        r = (i >= self.off1).astype(jnp.int32) + (i >= self.off2).astype(jnp.int32)
        return r, i - jnp.where(r == 0, 0, jnp.where(r == 1, self.off1, self.off2))

    def source(self, i):
        r, g = self.at(i)
        lap, cut = self.of_row(self.lap, r), self.of_row(self.cut, r)
        older = jnp.maximum(lap - 1, 0)
        base = (self.row0 + r) * self.seq_g
        src = base + jnp.minimum(jnp.where(g <= cut // GRAN, lap, older) * WIN_G + g, self.seq_g - 1)
        mixed = jnp.where(lap >= 1, base + older * WIN_G + g, -1)
        return src, jnp.where(g == cut // GRAN, (mixed + 1) * GRAN + cut % GRAN, -1)


def pack_kernel(base, src_ref, mix_ref, *refs):
    x_refs, prefill_ref, outs, older, sem = refs[:2 * STEP], refs[2 * STEP], refs[-4:-2], refs[-2], refs[-1]
    first = base + pl.program_id(0) * STEP
    for a in range(2):
        for t in range(STEP):
            outs[a][t] = x_refs[a * STEP + t][0]

        def patch(t, carry):
            code = mix_ref[a, first + t]

            @pl.when(code >= 0)
            def _():
                granule = code // GRAN - 1

                @pl.when(granule >= 0)
                def _():
                    copy = pltpu.make_async_copy(prefill_ref.at[granule], older, sem)
                    copy.start()
                    copy.wait()

                @pl.when(granule < 0)
                def _():
                    older[...] = jnp.zeros_like(older)

                newer = lax.broadcasted_iota(jnp.int32, (GRAN, 256), 0) < lax.rem(code, GRAN)
                outs[a][t] = jnp.where(newer, outs[a][t].astype(jnp.float32), older[...].astype(jnp.float32)).astype(jnp.bfloat16)

            return carry

        lax.fori_loop(0, STEP, patch, 0)


def pack(prefill, src, mix, base, count):
    def granule(a, t):
        return pl.BlockSpec((1, GRAN, 256), lambda i, src_ref, mix_ref: (src_ref[a, base + i * STEP + t], 0, 0))

    return pl.pallas_call(
        functools.partial(pack_kernel, base),
        grid_spec=pltpu.PrefetchScalarGridSpec(
            num_scalar_prefetch=2,
            grid=(count // STEP,),
            in_specs=[granule(a, t) for a in range(2) for t in range(STEP)] + [ANYWHERE],
            out_specs=[pl.BlockSpec((STEP, GRAN, 256), lambda i, src_ref, mix_ref: (i, 0, 0))] * 2,
            scratch_shapes=[pltpu.VMEM((GRAN, 256), jnp.bfloat16), pltpu.SemaphoreType.DMA],
        ),
        out_shape=[jax.ShapeDtypeStruct((count, GRAN, 256), prefill.dtype)] * 2,
        compiler_params=pltpu.CompilerParams(dimension_semantics=("arbitrary",), vmem_limit_bytes=VMEM_LIMIT),
        cost_estimate=pl.CostEstimate(flops=10_000_000, bytes_accessed=count * 130_000, transcendentals=0),
        name="pack",
    )(src, mix, *([prefill] * (2 * STEP + 1)))


def assemble_kernel(is_key, base, steps, code_ref, idx_ref, n_ref, me_ref, *refs):
    far_refs, near_refs, own_refs = refs[:2], refs[2:2 + STEP], refs[2 + STEP:2 + 2 * STEP]
    new_ref, qp_ref, prev_ref, _, cache_ref, res_ref, xb, mix, ob, acc, sems = refs[2 + 2 * STEP:]
    i = pl.program_id(0)
    first = base + i * STEP
    me = me_ref[0]
    slot = lax.rem(i, 2)
    codes = [code_ref[0, first + t] for t in range(STEP)]
    active = functools.reduce(jnp.maximum, codes) >= 0

    def writes(step, buf, act):
        def one(t, carry):
            code = code_ref[0, base + step * STEP + t]

            @pl.when(code >= 0)
            def _():
                act(pltpu.make_async_copy(ob.at[buf, t], cache_ref.at[code // WIN_G, pl.ds(lax.rem(code, WIN_G) * GRAN, GRAN)], sems.at[buf]))

            return carry

        lax.fori_loop(0, STEP, one, 0)

    if not is_key:
        @pl.when(i == 0)
        def _():
            acc[...] = prev_ref[...]

    @pl.when(i >= 2)
    def _():
        writes(i - 2, slot, lambda copy: copy.wait())

    @pl.when(active)
    def _():
        for d in range(2):
            xb[me ^ (2 + d)] = far_refs[d][...]
        for t in range(STEP):
            xb[me ^ 1, t] = near_refs[t][0]
            xb[me, t] = own_refs[t][0]

        for r in range(ROWS):
            cut = lax.rem(n_ref[r], WINDOW)
            target = r * WIN_G + cut // GRAN
            at = functools.reduce(jnp.add, [jnp.where(codes[t] == target, t + 1, 0) for t in range(STEP)])

            @pl.when(at > 0)
            def _():
                here = lax.broadcasted_iota(jnp.int32, (GRAN, 256), 0) == lax.rem(cut, GRAN)
                for h in range(WAYS):
                    new = jnp.broadcast_to(new_ref[r * WAYS + h], (GRAN, 256))
                    xb[h, at - 1] = jnp.where(here, new, xb[h, at - 1].astype(jnp.float32)).astype(jnp.bfloat16)

        lanes = STEP * GRAN
        xs = [xb[h].reshape(lanes, 256) for h in range(WAYS)]
        if is_key:
            lane = lax.broadcasted_iota(jnp.int32, (8, lanes), 1)
            row = lax.broadcasted_iota(jnp.int32, (8, lanes), 0) // 2
            code = jnp.full((8, lanes), -1, jnp.int32)
            for t in range(STEP):
                code = jnp.where(lane // GRAN == t, codes[t], code)
            length = jnp.where(row == 0, n_ref[0], jnp.where(row == 1, n_ref[1], n_ref[2]))
            place = (code % WIN_G) * GRAN + lane % GRAN
            live = (code >= 0) & (code // WIN_G == row) & ((length >= WINDOW) | (place <= length))
            for h in range(WAYS):
                s = lax.dot_general(qp_ref[h], xs[h], (((1,), (1,)), ((), ())), preferred_element_type=jnp.float32)
                res_ref[h] = jnp.where(live, s / 16.0, -jnp.inf)
        else:
            for h in range(WAYS):
                acc[h] += jnp.dot(qp_ref[h], xs[h], preferred_element_type=jnp.float32)

        for h in range(WAYS):
            x = xs[h].astype(jnp.float32)
            for half in range(2):
                mix[half, pl.ds(h, lanes, stride=WAYS), :] = x[:, half * 128:(half + 1) * 128]
        joined = jnp.concatenate([mix[half].astype(jnp.bfloat16) for half in range(2)], axis=1)
        ob[slot] = joined.reshape(STEP, GRAN, WAYS, 256)
        writes(i, slot, lambda copy: copy.start())

    if is_key:
        @pl.when(jnp.logical_not(active))
        def _():
            res_ref[...] = jnp.full_like(res_ref, -jnp.inf)
    else:
        @pl.when(i == steps - 1)
        def _():
            res_ref[...] = acc[...]

    @pl.when(i == steps - 1)
    def _():
        if steps >= 2:
            writes(i - 1, 1 - slot, lambda copy: copy.wait())
        writes(i, slot, lambda copy: copy.wait())


def assemble(is_key, base, codes, places, n, me, far, near, own, new, qp, prev, cache):
    steps = far[0].shape[0] // STEP
    whole = lambda *shape: pl.BlockSpec(shape, lambda i, *_: (0,) * len(shape))
    by_step = pl.BlockSpec((WAYS, 8, STEP * GRAN), lambda i, *_: (0, 0, base // STEP + i))
    single = [pl.BlockSpec((1, GRAN, 256), functools.partial(lambda t, i, code_ref, idx_ref, n_ref, me_ref: (idx_ref[0, base + i * STEP + t], 0, 0), t)) for t in range(STEP)]
    if is_key:
        qp_spec, prev_spec, res_spec = whole(WAYS, 8, 256), ANYWHERE, by_step
    else:
        qp_spec, prev_spec, res_spec = by_step, whole(WAYS, 8, 256), whole(WAYS, 8, 256)
    after = 4 + 2 + 2 * STEP
    aliases = {after + 3: 0}
    if is_key:
        aliases[after + 2] = 1
    return pl.pallas_call(
        functools.partial(assemble_kernel, is_key, base, steps),
        grid_spec=pltpu.PrefetchScalarGridSpec(
            num_scalar_prefetch=4,
            grid=(steps,),
            in_specs=[pl.BlockSpec((STEP, GRAN, 256), lambda i, *_: (i, 0, 0))] * 2 + single + single + [whole(ROWS * WAYS, 1, 256), qp_spec, prev_spec, ANYWHERE],
            out_specs=[ANYWHERE, res_spec],
            scratch_shapes=[
                pltpu.VMEM((WAYS, STEP, GRAN, 256), jnp.bfloat16),
                pltpu.VMEM((2, WAYS * STEP * GRAN, 128), jnp.float32),
                pltpu.VMEM((2, STEP, GRAN, WAYS, 256), jnp.bfloat16),
                pltpu.VMEM((WAYS, 8, 256), jnp.float32),
                pltpu.SemaphoreType.DMA((2,)),
            ],
        ),
        out_shape=[jax.ShapeDtypeStruct(cache.shape, cache.dtype), jax.ShapeDtypeStruct(prev.shape, prev.dtype)],
        input_output_aliases=aliases,
        compiler_params=pltpu.CompilerParams(dimension_semantics=("arbitrary",), vmem_limit_bytes=VMEM_LIMIT),
        cost_estimate=pl.CostEstimate(flops=10_000_000, bytes_accessed=steps * 4_000_000, transcendentals=0),
        name="assemble_keys" if is_key else "assemble_values",
    )(codes, places, n, me, *far, *([near] * STEP), *([own] * STEP), new, qp, prev, cache)


def solution(mesh):
    head_spec = P('dp', None, 'sh', None)
    row_spec = P(('dp', 'sh'))
    full_spec = P(None, None)

    def send(x, d):
        return lax.ppermute(x, 'sh', [(i, i ^ d) for i in range(WAYS)])

    def step(k_prefill, v_prefill, lengths, residual, norm_gain, w_query, w_key, w_value, w_out):
        seq_g = k_prefill.shape[1] // GRAN
        me = lax.axis_index('sh').astype(jnp.int32)
        peers = me ^ jnp.arange(WAYS, dtype=jnp.int32)
        by_peer = lengths[(peers[:, None] * ROWS + jnp.arange(ROWS, dtype=jnp.int32)).reshape(-1)].reshape(WAYS, ROWS)
        mine = by_peer[0]
        prefill = {True: k_prefill.reshape(-1, GRAN, 256), False: v_prefill.reshape(-1, GRAN, 256)}

        def lists(*ds):
            return Lists(jnp.stack([by_peer[d] for d in ds]), jnp.stack([(me ^ d) * ROWS for d in ds])[:, None], seq_g)

        def span(count):
            return jnp.arange(count, dtype=jnp.int32)[None, :]

        def held(which, i):
            src, mixed = which.source(i)
            valid = i < which.size
            return jnp.where(valid, src, 0), jnp.where(valid, mixed, -1)

        far, far_other, close, self_list = lists(2, 3), lists(3, 2), lists(1, 0), lists(0)
        fixed_src, fixed_mix = held(far, span(FIXED))
        close_src, close_mix = held(close, span(ROWS * WIN_G))

        sizes = jnp.sum(jnp.minimum(lengths // GRAN + 1, WIN_G).reshape(WAYS, ROWS), axis=1)
        excess = jnp.max(jnp.sum(jnp.maximum(sizes - FIXED, 0).reshape(WAYS // 2, 2), axis=1))
        level = lax.pmax((excess + 15) // 16, 'dp')
        spare = 8 * level
        on = active_units(level)
        column = span(SPARE)
        unit = functools.reduce(jnp.add, [(column >= s).astype(jnp.int32) for s in starts_of(UNITS)[1:]])
        skipped, used, place = 0, jnp.zeros_like(column, dtype=bool), column
        for u, size in enumerate(UNITS):
            used = jnp.where(unit == u, on[u], used)
            place = jnp.where(unit == u, column - skipped, place)
            skipped = skipped + jnp.where(on[u], 0, size)
        own_at, other_at = FIXED + place, FIXED + 2 * spare - 1 - place
        src_a, mix_a = held(far, own_at)
        src_b, mix_b = held(far_other, other_at)
        is_own = used & (own_at < far.size)
        is_other = used & (own_at >= far.size) & (other_at < far_other.size)
        spare_src = jnp.where(is_own, src_a, jnp.where(is_other, src_b, 0))
        spare_mix = jnp.where(is_own, mix_a, jnp.where(is_other, mix_b, -1))

        def belongs(i, valid):
            r, g = self_list.at(i)
            return jnp.where(valid & (i < self_list.size), r * WIN_G + g, -1), jnp.clip(i, 0, ROWS * WIN_G - 1)

        parts = [belongs(span(FIXED), True), belongs(own_at, used), belongs(other_at, used)]
        codes = jnp.concatenate([p[0] for p in parts], axis=1)
        places = jnp.concatenate([p[1] for p in parts], axis=1)

        fixed_got = {True: [], False: []}
        packed_values = []
        for base, count in zip(starts_of(K_PIECES), K_PIECES):
            out = pack(prefill[True], fixed_src, fixed_mix, base, count)
            a = send(out[0], 2)
            b = send(out[1], 3)
            fixed_got[True].append((a, b))
        close_got, spare_packed = {}, []
        for is_key in (True, False):
            spare_packed += [pack(prefill[is_key], spare_src, spare_mix, base, count) for base, count in zip(starts_of(UNITS), UNITS)]
        for is_key in (True, False):
            near, own = pack(prefill[is_key], close_src, close_mix, 0, ROWS * WIN_G)
            close_got[is_key] = (send(near, 1), own)
        for base, count in zip(starts_of(V_PIECES), V_PIECES):
            packed_values.append(pack(prefill[False], fixed_src, fixed_mix, base, count))

        resid_f32 = residual.astype(jnp.float32)
        inv_rms = lax.rsqrt(jnp.mean(resid_f32 * resid_f32, axis=-1, keepdims=True) + EPS)
        normed = (resid_f32 * inv_rms * norm_gain.astype(jnp.float32)).astype(jnp.bfloat16)
        q_group = w_query.shape[1] // (WAYS * 256)
        q_heads = jnp.dot(normed, w_query, preferred_element_type=jnp.float32).astype(jnp.bfloat16).reshape(ROWS, WAYS, q_group, 256)
        k_new = jnp.dot(normed, w_key, preferred_element_type=jnp.float32).astype(jnp.bfloat16).reshape(ROWS, WAYS, 256)
        v_new = jnp.dot(normed, w_value, preferred_element_type=jnp.float32).astype(jnp.bfloat16).reshape(ROWS, WAYS, 256)
        q_heads = rotate(q_heads, mine)
        k_new = rotate(k_new, mine)
        new = {True: k_new.astype(jnp.float32).reshape(-1, 1, 256), False: v_new.astype(jnp.float32).reshape(-1, 1, 256)}
        q_pad = jnp.pad(q_heads.transpose(1, 0, 2, 3).reshape(WAYS, ROWS * q_group, 256), ((0, 0), (0, 8 - ROWS * q_group), (0, 0)))
        k_cache, v_cache = cleared(mine, (ROWS, WINDOW, WAYS, 256))
        scores = blank((WAYS, 8, codes.shape[1] * GRAN), jnp.float32)

        def branch(lvl):
            keep = [bool(x) for x in active_units(lvl)] * 2

            def run(pairs):
                return [(send(a, 2), send(b, 3)) if k else (blank(a.shape, a.dtype), blank(b.shape, b.dtype)) for k, (a, b) in zip(keep, pairs)]

            return run

        spare_packed, packed_values, ready = lax.optimization_barrier((spare_packed, packed_values, (new, q_pad, k_cache, v_cache, scores, close_got[True][1], close_got[False][1])))
        new, q_pad, k_cache, v_cache, scores, own_k, own_v = ready
        own = {True: own_k, False: own_v}
        spare_got = lax.switch(level, [branch(x) for x in range(LEVELS)], spare_packed)
        spare_got, packed_values = lax.optimization_barrier((spare_got, packed_values))
        for a, b in packed_values:
            a = send(a, 2)
            b = send(b, 3)
            fixed_got[False].append((a, b))
        spare_got = {True: spare_got[:len(UNITS)], False: spare_got[len(UNITS):]}
        forwarded = {is_key: [(send(b, 1), send(a, 1)) for a, b in spare_got[is_key]] for is_key in (True, False)}

        me1 = me.reshape(1)

        def run(is_key, base, far_parts, qp, prev, cache):
            return assemble(is_key, base, codes, places, mine, me1, far_parts, close_got[is_key][0], own[is_key], new[is_key], qp, prev, cache)

        def spares(is_key, qp, prev, cache):
            for got, at in ((spare_got, FIXED), (forwarded, FIXED + SPARE)):
                for u, base in enumerate(starts_of(UNITS)):
                    cache, prev = run(is_key, at + base, got[is_key][u], qp, prev, cache)
            return cache, prev

        for base, parts_got in zip(starts_of(K_PIECES), fixed_got[True]):
            k_cache, scores = run(True, base, parts_got, q_pad, scores, k_cache)
        k_cache, scores = spares(True, q_pad, scores, k_cache)
        exp_scores = jnp.exp(scores - jnp.max(scores, axis=-1, keepdims=True))
        weights = (exp_scores / jnp.sum(exp_scores, axis=-1, keepdims=True)).astype(jnp.bfloat16)
        sums = jnp.zeros((WAYS, 8, 256), jnp.float32)
        v_cache, sums = spares(False, weights, sums, v_cache)
        for base, parts_got in zip(starts_of(V_PIECES), fixed_got[False]):
            v_cache, sums = run(False, base, parts_got, weights, sums, v_cache)
        attn_out = sums[:, :ROWS * q_group].astype(jnp.bfloat16).reshape(WAYS, ROWS, q_group * 256).transpose(1, 0, 2).reshape(ROWS, WAYS * q_group * 256)
        resid_out = (resid_f32 + jnp.dot(attn_out, w_out, preferred_element_type=jnp.float32)).astype(jnp.bfloat16)
        return resid_out, k_cache, v_cache

    return jax.shard_map(
        step, mesh=mesh, in_specs=(head_spec, head_spec, P('dp'), P(('dp', 'sh'), None), P(None), full_spec, full_spec, full_spec, full_spec),
        out_specs=(P(('dp', 'sh'), None), row_spec, row_spec), check_vma=False)
```

```python
import functools

import jax
import jax.numpy as jnp
from jax import lax
from jax.experimental import pallas as pl
from jax.experimental.pallas import tpu as pltpu
from jax.sharding import PartitionSpec as P


WINDOW = 4096
THETA = 10000.0
EPS = 1e-5
GRAN = 64
WIN_G = WINDOW // GRAN
STEP = 8
FIXED = 128
UNITS = (32, 16, 8, 4, 4)
SPARE = sum(UNITS)
QUANTUM = UNITS[-1]
LEVELS = SPARE // QUANTUM + 1
K_PIECES = (8, 24, 96)
V_PIECES = (64, 32, 16, 8, 4, 4)
WAYS, ROWS = 4, 3
VMEM_LIMIT = 67_043_328
ANYWHERE = pl.BlockSpec(memory_space=pl.ANY)


def starts_of(sizes):
    return [sum(sizes[:i]) for i in range(len(sizes))]


def active_units(level):
    full = level == LEVELS - 1
    return [full | ((level & (size // QUANTUM)) != 0) for size in UNITS[:-1]] + [full]


def rotate(heads, positions):
    head_dim = heads.shape[-1]
    half_dim = head_dim // 2
    inv_freq = THETA ** (-2.0 * jnp.arange(half_dim, dtype=jnp.float32) / head_dim)
    angles = positions.astype(jnp.float32).reshape(positions.shape + (1,) * (heads.ndim - 1)) * inv_freq
    cos_part = jnp.cos(angles)
    sin_part = jnp.sin(angles)
    first_half = heads[..., :half_dim].astype(jnp.float32)
    second_half = heads[..., half_dim:].astype(jnp.float32)
    return jnp.concatenate([first_half * cos_part - second_half * sin_part, second_half * cos_part + first_half * sin_part], axis=-1).astype(jnp.bfloat16)


def blank(shape, dtype):
    return pl.pallas_call(
        lambda o_ref: None,
        out_shape=jax.ShapeDtypeStruct(shape, dtype),
        out_specs=ANYWHERE,
        name="blank",
    )()


def cleared_kernel(n_ref, k_ref, v_ref, zeros, sem):
    zeros[...] = jnp.zeros_like(zeros)

    def each(act):
        for r in range(ROWS):
            def one(g, carry):
                for ref in (k_ref, v_ref):
                    act(pltpu.make_async_copy(zeros, ref.at[r, pl.ds(g * GRAN, GRAN)], sem))
                return carry

            lax.fori_loop(jnp.minimum(n_ref[r] // GRAN + 1, WIN_G), WIN_G, one, 0)

    each(lambda copy: copy.start())
    each(lambda copy: copy.wait())


def cleared(n, shape):
    return pl.pallas_call(
        cleared_kernel,
        grid_spec=pltpu.PrefetchScalarGridSpec(
            num_scalar_prefetch=1, grid=(1,), in_specs=[], out_specs=[ANYWHERE, ANYWHERE],
            scratch_shapes=[pltpu.VMEM((GRAN, WAYS, 256), jnp.bfloat16), pltpu.SemaphoreType.DMA]),
        out_shape=[jax.ShapeDtypeStruct(shape, jnp.bfloat16)] * 2,
        compiler_params=pltpu.CompilerParams(vmem_limit_bytes=VMEM_LIMIT),
        cost_estimate=pl.CostEstimate(flops=10_000_000, bytes_accessed=20_000_000, transcendentals=0),
        name="cleared",
    )(n)


class Lists:
    def __init__(self, n, row0, seq_g):
        self.n, self.row0, self.seq_g = n, row0, seq_g
        self.lap = n // WINDOW
        self.cut = n % WINDOW
        width = jnp.minimum(n // GRAN + 1, WIN_G)
        self.off1 = width[..., 0:1]
        self.off2 = self.off1 + width[..., 1:2]
        self.size = self.off2 + width[..., 2:3]

    def of_row(self, x, r):
        return jnp.where(r == 0, x[..., 0:1], jnp.where(r == 1, x[..., 1:2], x[..., 2:3]))

    def at(self, i):
        r = (i >= self.off1).astype(jnp.int32) + (i >= self.off2).astype(jnp.int32)
        return r, i - jnp.where(r == 0, 0, jnp.where(r == 1, self.off1, self.off2))

    def source(self, i):
        r, g = self.at(i)
        lap, cut = self.of_row(self.lap, r), self.of_row(self.cut, r)
        older = jnp.maximum(lap - 1, 0)
        base = (self.row0 + r) * self.seq_g
        src = base + jnp.minimum(jnp.where(g <= cut // GRAN, lap, older) * WIN_G + g, self.seq_g - 1)
        mixed = jnp.where(lap >= 1, base + older * WIN_G + g, -1)
        return src, jnp.where(g == cut // GRAN, (mixed + 1) * GRAN + cut % GRAN, -1)


def pack_kernel(base, size, steps, src_ref, mix_ref, *refs):
    prefills, outs, (older, sem) = refs[:-4], refs[-4:-2], refs[-2:]
    i = pl.program_id(0)
    first = base + lax.rem(i, steps) * size

    def by_tensor(do):
        for k, ref in enumerate(prefills):
            pl.when((i >= k * steps) & (i < (k + 1) * steps))(functools.partial(do, ref))

    def fetch(ref, act):
        def one(t, carry):
            for a in range(2):
                act(pltpu.make_async_copy(ref.at[src_ref[a, first + t]], outs[a].at[t], sem))
            return carry

        lax.fori_loop(0, size, one, 0)

    by_tensor(lambda ref: fetch(ref, lambda copy: copy.start()))
    fetch(prefills[0], lambda copy: copy.wait())

    for a in range(2):
        def patch(t, carry):
            code = mix_ref[a, first + t]

            @pl.when(code >= 0)
            def _():
                granule = code // GRAN - 1

                @pl.when(granule >= 0)
                def _():
                    by_tensor(lambda ref: pltpu.make_async_copy(ref.at[granule], older, sem).start())
                    pltpu.make_async_copy(prefills[0].at[0], older, sem).wait()

                @pl.when(granule < 0)
                def _():
                    older[...] = jnp.zeros_like(older)

                newer = lax.broadcasted_iota(jnp.int32, (GRAN, 256), 0) < lax.rem(code, GRAN)
                outs[a][t] = jnp.where(newer, outs[a][t].astype(jnp.float32), older[...].astype(jnp.float32)).astype(jnp.bfloat16)

            return carry

        lax.fori_loop(0, size, patch, 0)


def pack(prefills, src, mix, base, count):
    size = next(x for x in (16, 8, 4) if count % x == 0)
    steps = count // size
    total = count * len(prefills)
    return pl.pallas_call(
        functools.partial(pack_kernel, base, size, steps),
        grid_spec=pltpu.PrefetchScalarGridSpec(
            num_scalar_prefetch=2,
            grid=(steps * len(prefills),),
            in_specs=[ANYWHERE] * len(prefills),
            out_specs=[pl.BlockSpec((size, GRAN, 256), lambda i, src_ref, mix_ref: (i, 0, 0))] * 2,
            scratch_shapes=[pltpu.VMEM((GRAN, 256), jnp.bfloat16), pltpu.SemaphoreType.DMA],
        ),
        out_shape=[jax.ShapeDtypeStruct((total, GRAN, 256), jnp.bfloat16)] * 2,
        compiler_params=pltpu.CompilerParams(dimension_semantics=("arbitrary",), vmem_limit_bytes=VMEM_LIMIT),
        cost_estimate=pl.CostEstimate(flops=10_000_000, bytes_accessed=total * 130_000, transcendentals=0),
        name="pack",
    )(src, mix, *prefills)


def assemble_kernel(is_key, base, size, steps, segments, code_ref, idx_ref, n_ref, me_ref, *refs):
    num_far = 2 * (1 + max(s[2] for s in segments))
    far_refs = refs[:num_far]
    near_ref, own_ref, new_ref, qp_ref, prev_ref, _, cache_ref, res_ref, xb, mix, ob, acc, sems = refs[num_far:]
    i = pl.program_id(0)
    me = me_ref[0]
    slot = lax.rem(i, 2)

    def code_at(step, t):
        return code_ref[0, base + step * size + t]

    def active_at(step):
        return functools.reduce(jnp.maximum, [code_at(step, t) for t in range(size)]) >= 0

    def reads(step, buf, act):
        @pl.when(active_at(step))
        def _():
            for begin, end, entry, offset, count, place in segments:
                @pl.when((step >= begin) & (step < end))
                def _():
                    for d in range(2):
                        act(pltpu.make_async_copy(far_refs[2 * entry + d].at[pl.ds(offset + (step - begin) * size, count)], xb.at[buf, me ^ (2 + d), pl.ds(place, count)], sems.at[0, buf]))

            def one(t, carry):
                at = idx_ref[0, base + step * size + t]
                act(pltpu.make_async_copy(near_ref.at[at], xb.at[buf, me ^ 1, t], sems.at[0, buf]))
                act(pltpu.make_async_copy(own_ref.at[at], xb.at[buf, me, t], sems.at[0, buf]))
                return carry

            lax.fori_loop(0, size, one, 0)

    def write(step, t, buf):
        code = code_at(step, t)
        return pltpu.make_async_copy(ob.at[buf, t], cache_ref.at[code // WIN_G, pl.ds(lax.rem(code, WIN_G) * GRAN, GRAN)], sems.at[1, buf])

    def written(step, buf):
        def one(t, carry):
            @pl.when(code_at(step, t) >= 0)
            def _():
                write(step, t, buf).wait()

            return carry

        lax.fori_loop(0, size, one, 0)

    @pl.when(i == 0)
    def _():
        reads(i, slot, lambda copy: copy.start())
        if not is_key:
            acc[...] = prev_ref[...]

    if steps > 1:
        @pl.when(i + 1 < steps)
        def _():
            reads(i + 1, 1 - slot, lambda copy: copy.start())

    if steps > 2:
        @pl.when(i >= 2)
        def _():
            written(i - 2, slot)

    reads(i, slot, lambda copy: copy.wait())
    active = active_at(i)

    @pl.when(active)
    def _():
        def one(t, carry):
            code = code_at(i, t)

            @pl.when(code < 0)
            def _():
                for h in range(WAYS):
                    xb[slot, h, t] = jnp.zeros((GRAN, 256), jnp.bfloat16)

            for r in range(ROWS):
                cut = lax.rem(n_ref[r], WINDOW)

                @pl.when(code == r * WIN_G + cut // GRAN)
                def _():
                    here = lax.broadcasted_iota(jnp.int32, (GRAN, 256), 0) == lax.rem(cut, GRAN)
                    for h in range(WAYS):
                        new = jnp.broadcast_to(new_ref[r * WAYS + h], (GRAN, 256))
                        xb[slot, h, t] = jnp.where(here, new, xb[slot, h, t].astype(jnp.float32)).astype(jnp.bfloat16)

            @pl.when(code >= 0)
            def _():
                for h in range(WAYS):
                    x = xb[slot, h, t].astype(jnp.float32)
                    for half in range(2):
                        mix[half, pl.ds(h, GRAN, stride=WAYS), :] = x[:, half * 128:(half + 1) * 128]
                joined = jnp.concatenate([mix[half].astype(jnp.bfloat16) for half in range(2)], axis=1)
                ob[slot, t] = joined.reshape(GRAN, WAYS, 256)
                write(i, t, slot).start()

            return carry

        lax.fori_loop(0, size, one, 0)

        lanes = size * GRAN
        if is_key:
            lane = lax.broadcasted_iota(jnp.int32, (8, lanes), 1)
            row = lax.broadcasted_iota(jnp.int32, (8, lanes), 0) // 2
            code = jnp.full((8, lanes), -1, jnp.int32)
            for t in range(size):
                code = jnp.where(lane // GRAN == t, code_at(i, t), code)
            length = jnp.where(row == 0, n_ref[0], jnp.where(row == 1, n_ref[1], n_ref[2]))
            place = (code % WIN_G) * GRAN + lane % GRAN
            live = (code >= 0) & (code // WIN_G == row) & ((length >= WINDOW) | (place <= length))
            for h in range(WAYS):
                s = lax.dot_general(qp_ref[h], xb[slot, h].reshape(lanes, 256), (((1,), (1,)), ((), ())), preferred_element_type=jnp.float32)
                res_ref[h] = jnp.where(live, s / 16.0, -jnp.inf)
        else:
            for h in range(WAYS):
                acc[h] += jnp.dot(qp_ref[h], xb[slot, h].reshape(lanes, 256), preferred_element_type=jnp.float32)

    if is_key:
        @pl.when(jnp.logical_not(active))
        def _():
            res_ref[...] = jnp.full_like(res_ref, -jnp.inf)

    @pl.when(i == steps - 1)
    def _():
        if not is_key:
            res_ref[...] = acc[...]
        if steps >= 2:
            written(i - 1, 1 - slot)
        written(i, slot)


def assemble(is_key, base, codes, places, n, me, far, near, own, new, qp, prev, cache):
    total = sum(f[3] for f in far)
    size = min(STEP, total)
    steps = total // size
    segments, at = [], 0
    for entry, (_, _, offset, count) in enumerate(far):
        if count >= size:
            segments.append((at // size, (at + count) // size, entry, offset, size, 0))
        else:
            segments.append((at // size, at // size + 1, entry, offset, count, at % size))
        at += count
    whole = lambda *shape: pl.BlockSpec(shape, lambda i, *_: (0,) * len(shape))
    by_step = pl.BlockSpec((WAYS, 8, size * GRAN), lambda i, *_: (0, 0, base // size + i))
    if is_key:
        qp_spec, prev_spec, res_spec = whole(WAYS, 8, 256), ANYWHERE, by_step
    else:
        qp_spec, prev_spec, res_spec = by_step, whole(WAYS, 8, 256), whole(WAYS, 8, 256)
    after = 4 + 2 * len(far) + 2
    aliases = {after + 3: 0}
    if is_key:
        aliases[after + 2] = 1
    return pl.pallas_call(
        functools.partial(assemble_kernel, is_key, base, size, steps, segments),
        grid_spec=pltpu.PrefetchScalarGridSpec(
            num_scalar_prefetch=4,
            grid=(steps,),
            in_specs=[ANYWHERE] * (2 * len(far) + 2) + [whole(ROWS * WAYS, 1, 256), qp_spec, prev_spec, ANYWHERE],
            out_specs=[ANYWHERE, res_spec],
            scratch_shapes=[
                pltpu.VMEM((2, WAYS, size, GRAN, 256), jnp.bfloat16),
                pltpu.VMEM((2, WAYS * GRAN, 128), jnp.float32),
                pltpu.VMEM((2, size, GRAN, WAYS, 256), jnp.bfloat16),
                pltpu.VMEM((WAYS, 8, 256), jnp.float32),
                pltpu.SemaphoreType.DMA((2, 2)),
            ],
        ),
        out_shape=[jax.ShapeDtypeStruct(cache.shape, cache.dtype), jax.ShapeDtypeStruct(prev.shape, prev.dtype)],
        input_output_aliases=aliases,
        compiler_params=pltpu.CompilerParams(dimension_semantics=("arbitrary",), vmem_limit_bytes=VMEM_LIMIT),
        cost_estimate=pl.CostEstimate(flops=10_000_000, bytes_accessed=steps * 4_000_000, transcendentals=0),
        name="assemble_keys" if is_key else "assemble_values",
    )(codes, places, n, me, *[x for f in far for x in f[:2]], near, own, new, qp, prev, cache)


def solution(mesh):
    head_spec = P('dp', None, 'sh', None)
    row_spec = P(('dp', 'sh'))
    full_spec = P(None, None)

    def send(x, d):
        return lax.ppermute(x, 'sh', [(i, i ^ d) for i in range(WAYS)])

    def step(k_prefill, v_prefill, lengths, residual, norm_gain, w_query, w_key, w_value, w_out):
        seq_g = k_prefill.shape[1] // GRAN
        me = lax.axis_index('sh').astype(jnp.int32)
        peers = me ^ jnp.arange(WAYS, dtype=jnp.int32)
        by_peer = lengths[(peers[:, None] * ROWS + jnp.arange(ROWS, dtype=jnp.int32)).reshape(-1)].reshape(WAYS, ROWS)
        mine = by_peer[0]
        prefill = {True: k_prefill.reshape(-1, GRAN, 256), False: v_prefill.reshape(-1, GRAN, 256)}

        def lists(*ds):
            return Lists(jnp.stack([by_peer[d] for d in ds]), jnp.stack([(me ^ d) * ROWS for d in ds])[:, None], seq_g)

        def span(count):
            return jnp.arange(count, dtype=jnp.int32)[None, :]

        def held(which, i):
            src, mixed = which.source(i)
            valid = i < which.size
            return jnp.where(valid, src, 0), jnp.where(valid, mixed, -1)

        far, far_other, close, self_list = lists(2, 3), lists(3, 2), lists(1, 0), lists(0)
        fixed_src, fixed_mix = held(far, span(FIXED))
        close_src, close_mix = held(close, span(ROWS * WIN_G))

        sizes = jnp.sum(jnp.minimum(lengths // GRAN + 1, WIN_G).reshape(WAYS, ROWS), axis=1)
        excess = jnp.max(jnp.sum(jnp.maximum(sizes - FIXED, 0).reshape(WAYS // 2, 2), axis=1))
        level = lax.pmax((excess + 2 * QUANTUM - 1) // (2 * QUANTUM), 'dp')
        spare = QUANTUM * level
        on = active_units(level)
        column = span(SPARE)
        unit = functools.reduce(jnp.add, [(column >= s).astype(jnp.int32) for s in starts_of(UNITS)[1:]])
        skipped, used, place = 0, jnp.zeros_like(column, dtype=bool), column
        for u, size in enumerate(UNITS):
            used = jnp.where(unit == u, on[u], used)
            place = jnp.where(unit == u, column - skipped, place)
            skipped = skipped + jnp.where(on[u], 0, size)
        own_at, other_at = FIXED + place, FIXED + 2 * spare - 1 - place
        src_a, mix_a = held(far, own_at)
        src_b, mix_b = held(far_other, other_at)
        is_own = used & (own_at < far.size)
        is_other = used & (own_at >= far.size) & (other_at < far_other.size)
        spare_src = jnp.where(is_own, src_a, jnp.where(is_other, src_b, 0))
        spare_mix = jnp.where(is_own, mix_a, jnp.where(is_other, mix_b, -1))

        def belongs(i, valid):
            r, g = self_list.at(i)
            return jnp.where(valid & (i < self_list.size), r * WIN_G + g, -1), jnp.clip(i, 0, ROWS * WIN_G - 1)

        parts = [belongs(span(FIXED), True), belongs(own_at, used), belongs(other_at, used)]
        codes = jnp.concatenate([p[0] for p in parts], axis=1)
        places = jnp.concatenate([p[1] for p in parts], axis=1)

        fixed_got = {True: [], False: []}
        packed_values = []
        for base, count in zip(starts_of(K_PIECES), K_PIECES):
            out = pack([prefill[True]], fixed_src, fixed_mix, base, count)
            a = send(out[0], 2)
            b = send(out[1], 3)
            fixed_got[True].append((a, b))
        close_got = {}
        for is_key in (True, False):
            near, own = pack([prefill[is_key]], close_src, close_mix, 0, ROWS * WIN_G)
            close_got[is_key] = (send(near, 1), own)
        spare_packed = [pack([prefill[True], prefill[False]], spare_src, spare_mix, base, count) for base, count in zip(starts_of(UNITS), UNITS)]
        for base, count in zip(starts_of(V_PIECES), V_PIECES):
            packed_values.append(pack([prefill[False]], fixed_src, fixed_mix, base, count))

        resid_f32 = residual.astype(jnp.float32)
        inv_rms = lax.rsqrt(jnp.mean(resid_f32 * resid_f32, axis=-1, keepdims=True) + EPS)
        normed = (resid_f32 * inv_rms * norm_gain.astype(jnp.float32)).astype(jnp.bfloat16)
        q_group = w_query.shape[1] // (WAYS * 256)
        q_heads = jnp.dot(normed, w_query, preferred_element_type=jnp.float32).astype(jnp.bfloat16).reshape(ROWS, WAYS, q_group, 256)
        k_new = jnp.dot(normed, w_key, preferred_element_type=jnp.float32).astype(jnp.bfloat16).reshape(ROWS, WAYS, 256)
        v_new = jnp.dot(normed, w_value, preferred_element_type=jnp.float32).astype(jnp.bfloat16).reshape(ROWS, WAYS, 256)
        q_heads = rotate(q_heads, mine)
        k_new = rotate(k_new, mine)
        new = {True: k_new.astype(jnp.float32).reshape(-1, 1, 256), False: v_new.astype(jnp.float32).reshape(-1, 1, 256)}
        q_pad = jnp.pad(q_heads.transpose(1, 0, 2, 3).reshape(WAYS, ROWS * q_group, 256), ((0, 0), (0, 8 - ROWS * q_group), (0, 0)))
        k_cache, v_cache = cleared(mine, (ROWS, WINDOW, WAYS, 256))
        scores = blank((WAYS, 8, codes.shape[1] * GRAN), jnp.float32)

        def branch(lvl):
            keep = [bool(x) for x in active_units(lvl)]

            def run(pairs):
                return [(send(a, 2), send(b, 3)) if k else (blank(a.shape, a.dtype), blank(b.shape, b.dtype)) for k, (a, b) in zip(keep, pairs)]

            return run

        spare_packed, packed_values, ready = lax.optimization_barrier((spare_packed, packed_values, (new, q_pad, k_cache, v_cache, scores, close_got[True][1], close_got[False][1])))
        new, q_pad, k_cache, v_cache, scores, own_k, own_v = ready
        own = {True: own_k, False: own_v}
        spare_got = lax.switch(level, [branch(x) for x in range(LEVELS)], spare_packed)
        spare_got, packed_values = lax.optimization_barrier((spare_got, packed_values))
        for a, b in packed_values:
            a = send(a, 2)
            b = send(b, 3)
            fixed_got[False].append((a, b))
        forwarded = [(send(b, 1), send(a, 1)) for a, b in spare_got]

        me1 = me.reshape(1)

        def run(is_key, base, far_parts, qp, prev, cache):
            return assemble(is_key, base, codes, places, mine, me1, far_parts, close_got[is_key][0], own[is_key], new[is_key], qp, prev, cache)

        def fixed(pieces, got):
            return [(a, b, 0, count) for (a, b), count in zip(got, pieces)]

        def spares(is_key):
            return [(a, b, 0 if is_key else count, count) for got in (spare_got, forwarded) for (a, b), count in zip(got, UNITS)]

        k_cache, scores = run(True, 0, fixed(K_PIECES, fixed_got[True]), q_pad, scores, k_cache)
        k_cache, scores = run(True, FIXED, spares(True), q_pad, scores, k_cache)
        exp_scores = jnp.exp(scores - jnp.max(scores, axis=-1, keepdims=True))
        weights = (exp_scores / jnp.sum(exp_scores, axis=-1, keepdims=True)).astype(jnp.bfloat16)
        sums = jnp.zeros((WAYS, 8, 256), jnp.float32)
        v_cache, sums = run(False, FIXED, spares(False), weights, sums, v_cache)
        for base, part in zip(starts_of(V_PIECES), fixed(V_PIECES, fixed_got[False])):
            v_cache, sums = run(False, base, [part], weights, sums, v_cache)
        attn_out = sums[:, :ROWS * q_group].astype(jnp.bfloat16).reshape(WAYS, ROWS, q_group * 256).transpose(1, 0, 2).reshape(ROWS, WAYS * q_group * 256)
        resid_out = (resid_f32 + jnp.dot(attn_out, w_out, preferred_element_type=jnp.float32)).astype(jnp.bfloat16)
        return resid_out, k_cache, v_cache

    return jax.shard_map(
        step, mesh=mesh, in_specs=(head_spec, head_spec, P('dp'), P(('dp', 'sh'), None), P(None), full_spec, full_spec, full_spec, full_spec),
        out_specs=(P(('dp', 'sh'), None), row_spec, row_spec), check_vma=False)
```

```python
import functools

import jax
import jax.numpy as jnp
from jax import lax
from jax.experimental import pallas as pl
from jax.experimental.pallas import tpu as pltpu
from jax.sharding import PartitionSpec as P


WINDOW = 4096
THETA = 10000.0
EPS = 1e-5
GRAN = 64
WIN_G = WINDOW // GRAN
STEP = 8
FIXED = 128
UNITS = (32, 16, 8, 4, 4)
SPARE = sum(UNITS)
QUANTUM = UNITS[-1]
LEVELS = SPARE // QUANTUM + 1
K_PIECES = (8, 24, 96)
V_PIECES = (64, 32, 16, 8, 4, 4)
WAYS, ROWS = 4, 3
VMEM_LIMIT = 67_043_328
ANYWHERE = pl.BlockSpec(memory_space=pl.ANY)


def starts_of(sizes):
    return [sum(sizes[:i]) for i in range(len(sizes))]


def active_units(level):
    full = level == LEVELS - 1
    return [full | ((level & (size // QUANTUM)) != 0) for size in UNITS[:-1]] + [full]


def rotate(heads, positions):
    head_dim = heads.shape[-1]
    half_dim = head_dim // 2
    inv_freq = THETA ** (-2.0 * jnp.arange(half_dim, dtype=jnp.float32) / head_dim)
    angles = positions.astype(jnp.float32).reshape(positions.shape + (1,) * (heads.ndim - 1)) * inv_freq
    cos_part = jnp.cos(angles)
    sin_part = jnp.sin(angles)
    first_half = heads[..., :half_dim].astype(jnp.float32)
    second_half = heads[..., half_dim:].astype(jnp.float32)
    return jnp.concatenate([first_half * cos_part - second_half * sin_part, second_half * cos_part + first_half * sin_part], axis=-1).astype(jnp.bfloat16)


def blank(shape, dtype):
    return pl.pallas_call(
        lambda o_ref: None,
        out_shape=jax.ShapeDtypeStruct(shape, dtype),
        out_specs=ANYWHERE,
        name="blank",
    )()


def cleared_kernel(n_ref, k_ref, v_ref, zeros, sem):
    zeros[...] = jnp.zeros_like(zeros)

    def each(act):
        for r in range(ROWS):
            def one(g, carry):
                for ref in (k_ref, v_ref):
                    act(pltpu.make_async_copy(zeros, ref.at[r, pl.ds(g * GRAN, GRAN)], sem))
                return carry

            lax.fori_loop(jnp.minimum(n_ref[r] // GRAN + 1, WIN_G), WIN_G, one, 0)

    each(lambda copy: copy.start())
    each(lambda copy: copy.wait())


def cleared(n, shape):
    return pl.pallas_call(
        cleared_kernel,
        grid_spec=pltpu.PrefetchScalarGridSpec(
            num_scalar_prefetch=1, grid=(1,), in_specs=[], out_specs=[ANYWHERE, ANYWHERE],
            scratch_shapes=[pltpu.VMEM((GRAN, WAYS, 256), jnp.bfloat16), pltpu.SemaphoreType.DMA]),
        out_shape=[jax.ShapeDtypeStruct(shape, jnp.bfloat16)] * 2,
        compiler_params=pltpu.CompilerParams(vmem_limit_bytes=VMEM_LIMIT),
        cost_estimate=pl.CostEstimate(flops=10_000_000, bytes_accessed=20_000_000, transcendentals=0),
        name="cleared",
    )(n)


class Lists:
    def __init__(self, n, row0, seq_g):
        self.n, self.row0, self.seq_g = n, row0, seq_g
        self.lap = n // WINDOW
        self.cut = n % WINDOW
        width = jnp.minimum(n // GRAN + 1, WIN_G)
        self.off1 = width[..., 0:1]
        self.off2 = self.off1 + width[..., 1:2]
        self.size = self.off2 + width[..., 2:3]

    def of_row(self, x, r):
        return jnp.where(r == 0, x[..., 0:1], jnp.where(r == 1, x[..., 1:2], x[..., 2:3]))

    def at(self, i):
        r = (i >= self.off1).astype(jnp.int32) + (i >= self.off2).astype(jnp.int32)
        return r, i - jnp.where(r == 0, 0, jnp.where(r == 1, self.off1, self.off2))

    def source(self, i):
        r, g = self.at(i)
        lap, cut = self.of_row(self.lap, r), self.of_row(self.cut, r)
        older = jnp.maximum(lap - 1, 0)
        base = (self.row0 + r) * self.seq_g
        src = base + jnp.minimum(jnp.where(g <= cut // GRAN, lap, older) * WIN_G + g, self.seq_g - 1)
        mixed = jnp.where(lap >= 1, base + older * WIN_G + g, -1)
        return src, jnp.where(g == cut // GRAN, (mixed + 1) * GRAN + cut % GRAN, -1)


def pack_kernel(base, size, steps, source, *refs):
    num = source.num_scalars
    scalars, refs = refs[:num], refs[num:]
    prefills, outs, (buf, older, sems) = refs[:-5], refs[-5:-3], refs[-3:]
    at = source.reader(*scalars)
    i = pl.program_id(0)
    total = steps * len(prefills)
    slots = buf.shape[0]
    slot = lax.rem(i, slots)

    def by_tensor(step, do):
        for k, ref in enumerate(prefills):
            pl.when((step >= k * steps) & (step < (k + 1) * steps))(functools.partial(do, ref))

    def fetch(step):
        first = base + lax.rem(step, steps) * size
        to = lax.rem(step, slots)

        def from_ref(ref):
            def one(t, carry):
                for a in range(2):
                    pltpu.make_async_copy(ref.at[at(a, first + t)[0]], buf.at[to, a, t], sems.at[0, to]).start()
                return carry

            lax.fori_loop(0, size, one, 0)

        by_tensor(step, from_ref)

    def stores(step):
        to = lax.rem(step, slots)
        return [pltpu.make_async_copy(buf.at[to, a], outs[a].at[pl.ds(step * size, size)], sems.at[1, to]) for a in range(2)]

    @pl.when(i == 0)
    def _():
        fetch(i)

    if total > 1:
        @pl.when(i + 1 < total)
        def _():
            if total > slots:
                @pl.when(i + 1 >= slots)
                def _():
                    for copy in stores(i + 1 - slots):
                        copy.wait()
            fetch(i + 1)

    pltpu.make_async_copy(buf.at[slot], buf.at[slot], sems.at[0, slot]).wait()
    first = base + lax.rem(i, steps) * size
    for a in range(2):
        def patch(t, carry):
            code = at(a, first + t)[1]

            @pl.when(code >= 0)
            def _():
                granule = code // GRAN - 1

                @pl.when(granule >= 0)
                def _():
                    by_tensor(i, lambda ref: pltpu.make_async_copy(ref.at[granule], older, sems.at[0, slot]).start())
                    pltpu.make_async_copy(older, older, sems.at[0, slot]).wait()

                @pl.when(granule < 0)
                def _():
                    older[...] = jnp.zeros_like(older)

                newer = lax.broadcasted_iota(jnp.int32, (GRAN, 256), 0) < lax.rem(code, GRAN)
                buf[slot, a, t] = jnp.where(newer, buf[slot, a, t].astype(jnp.float32), older[...].astype(jnp.float32)).astype(jnp.bfloat16)

            return carry

        lax.fori_loop(0, size, patch, 0)
    for copy in stores(i):
        copy.start()

    @pl.when(i == total - 1)
    def _():
        for back in range(min(slots, total)):
            for copy in stores(i - back):
                copy.wait()


class FromTable:
    num_scalars = 2

    def __init__(self, src, mix):
        self.scalars = (src, mix)

    def reader(self, src_ref, mix_ref):
        return lambda a, i: (src_ref[a, i], mix_ref[a, i])


class FromLengths:
    num_scalars = 1

    def __init__(self, lengths, seq_g):
        self.scalars = (lengths,)
        self.seq_g = seq_g

    def reader(self, n_ref):
        me = lax.axis_index('sh').astype(jnp.int32)

        def at(a, i):
            row0 = (me ^ (2 + a)) * ROWS
            n = [n_ref[row0 + r] for r in range(ROWS)]
            ends, end = [], 0
            for x in n:
                end = end + jnp.minimum(x // GRAN + 1, WIN_G)
                ends.append(end)
            r = jnp.where(i >= ends[0], 1, 0) + jnp.where(i >= ends[1], 1, 0)
            g = i - jnp.where(r == 0, 0, jnp.where(r == 1, ends[0], ends[1]))
            length = jnp.where(r == 0, n[0], jnp.where(r == 1, n[1], n[2]))
            lap, cut = length // WINDOW, lax.rem(length, WINDOW)
            older = jnp.maximum(lap - 1, 0)
            first = (row0 + r) * self.seq_g
            src = first + jnp.minimum(jnp.where(g <= cut // GRAN, lap, older) * WIN_G + g, self.seq_g - 1)
            mixed = jnp.where(lap >= 1, first + older * WIN_G + g, -1)
            valid = i < ends[2]
            return jnp.where(valid, src, 0), jnp.where(valid & (g == cut // GRAN), (mixed + 1) * GRAN + lax.rem(cut, GRAN), -1)

        return at


def pack(prefills, source, base, count):
    size = next(x for x in (16, 8, 4) if count % x == 0)
    steps = count // size
    total = count * len(prefills)
    return pl.pallas_call(
        functools.partial(pack_kernel, base, size, steps, source),
        grid_spec=pltpu.PrefetchScalarGridSpec(
            num_scalar_prefetch=source.num_scalars,
            grid=(steps * len(prefills),),
            in_specs=[ANYWHERE] * len(prefills),
            out_specs=[ANYWHERE] * 2,
            scratch_shapes=[pltpu.VMEM((3, 2, size, GRAN, 256), jnp.bfloat16), pltpu.VMEM((GRAN, 256), jnp.bfloat16), pltpu.SemaphoreType.DMA((2, 3))],
        ),
        out_shape=[jax.ShapeDtypeStruct((total, GRAN, 256), jnp.bfloat16)] * 2,
        compiler_params=pltpu.CompilerParams(dimension_semantics=("arbitrary",), vmem_limit_bytes=VMEM_LIMIT),
        cost_estimate=pl.CostEstimate(flops=10_000_000, bytes_accessed=total * 130_000, transcendentals=0),
        name="pack",
    )(*source.scalars, *prefills)


def assemble_kernel(is_key, base, size, steps, segments, code_ref, idx_ref, n_ref, me_ref, *refs):
    num_far = 2 * (1 + max(s[2] for s in segments))
    far_refs = refs[:num_far]
    near_ref, own_ref, new_ref, qp_ref, prev_ref, _, cache_ref, res_ref, xb, mix, ob, acc, sems = refs[num_far:]
    i = pl.program_id(0)
    me = me_ref[0]
    slot = lax.rem(i, 2)

    def code_at(step, t):
        return code_ref[0, base + step * size + t]

    def active_at(step):
        return functools.reduce(jnp.maximum, [code_at(step, t) for t in range(size)]) >= 0

    def read(step, buf):
        @pl.when(active_at(step))
        def _():
            for begin, end, entry, offset, count, place in segments:
                @pl.when((step >= begin) & (step < end))
                def _():
                    for d in range(2):
                        pltpu.make_async_copy(far_refs[2 * entry + d].at[pl.ds(offset + (step - begin) * size, count)], xb.at[buf, me ^ (2 + d), pl.ds(place, count)], sems.at[0, buf]).start()

            def one(t, carry):
                at = idx_ref[0, base + step * size + t]
                pltpu.make_async_copy(near_ref.at[at], xb.at[buf, me ^ 1, t], sems.at[0, buf]).start()
                pltpu.make_async_copy(own_ref.at[at], xb.at[buf, me, t], sems.at[0, buf]).start()
                return carry

            lax.fori_loop(0, size, one, 0)

    def write(step, t, buf):
        code = code_at(step, t)
        return pltpu.make_async_copy(ob.at[buf, t], cache_ref.at[code // WIN_G, pl.ds(lax.rem(code, WIN_G) * GRAN, GRAN)], sems.at[1, buf])

    def written(step, buf):
        def one(t, carry):
            @pl.when(code_at(step, t) >= 0)
            def _():
                write(step, t, buf).wait()

            return carry

        lax.fori_loop(0, size, one, 0)

    @pl.when(i == 0)
    def _():
        read(i, slot)
        if not is_key:
            acc[...] = prev_ref[...]

    if steps > 1:
        @pl.when(i + 1 < steps)
        def _():
            read(i + 1, 1 - slot)

    if steps > 2:
        @pl.when(i >= 2)
        def _():
            written(i - 2, slot)

    active = active_at(i)

    @pl.when(active)
    def _():
        pltpu.make_async_copy(xb.at[slot], xb.at[slot], sems.at[0, slot]).wait()

        def one(t, carry):
            code = code_at(i, t)

            @pl.when(code < 0)
            def _():
                for h in range(WAYS):
                    xb[slot, h, t] = jnp.zeros((GRAN, 256), jnp.bfloat16)

            for r in range(ROWS):
                cut = lax.rem(n_ref[r], WINDOW)

                @pl.when(code == r * WIN_G + cut // GRAN)
                def _():
                    here = lax.broadcasted_iota(jnp.int32, (GRAN, 256), 0) == lax.rem(cut, GRAN)
                    for h in range(WAYS):
                        new = jnp.broadcast_to(new_ref[r * WAYS + h], (GRAN, 256))
                        xb[slot, h, t] = jnp.where(here, new, xb[slot, h, t].astype(jnp.float32)).astype(jnp.bfloat16)

            @pl.when(code >= 0)
            def _():
                for h in range(WAYS):
                    x = xb[slot, h, t].astype(jnp.float32)
                    for half in range(2):
                        mix[half, pl.ds(h, GRAN, stride=WAYS), :] = x[:, half * 128:(half + 1) * 128]
                joined = jnp.concatenate([mix[half].astype(jnp.bfloat16) for half in range(2)], axis=1)
                ob[slot, t] = joined.reshape(GRAN, WAYS, 256)
                write(i, t, slot).start()

            return carry

        lax.fori_loop(0, size, one, 0)

        lanes = size * GRAN
        if is_key:
            lane = lax.broadcasted_iota(jnp.int32, (8, lanes), 1)
            row = lax.broadcasted_iota(jnp.int32, (8, lanes), 0) // 2
            code = jnp.full((8, lanes), -1, jnp.int32)
            for t in range(size):
                code = jnp.where(lane // GRAN == t, code_at(i, t), code)
            length = jnp.where(row == 0, n_ref[0], jnp.where(row == 1, n_ref[1], n_ref[2]))
            place = (code % WIN_G) * GRAN + lane % GRAN
            live = (code >= 0) & (code // WIN_G == row) & ((length >= WINDOW) | (place <= length))
            for h in range(WAYS):
                s = lax.dot_general(qp_ref[h], xb[slot, h].reshape(lanes, 256), (((1,), (1,)), ((), ())), preferred_element_type=jnp.float32)
                res_ref[h] = jnp.where(live, s / 16.0, -jnp.inf)
        else:
            for h in range(WAYS):
                acc[h] += jnp.dot(qp_ref[h], xb[slot, h].reshape(lanes, 256), preferred_element_type=jnp.float32)

    if is_key:
        @pl.when(jnp.logical_not(active))
        def _():
            res_ref[...] = jnp.full_like(res_ref, -jnp.inf)

    @pl.when(i == steps - 1)
    def _():
        if not is_key:
            res_ref[...] = acc[...]
        if steps >= 2:
            written(i - 1, 1 - slot)
        written(i, slot)


def assemble(is_key, base, codes, places, n, me, far, near, own, new, qp, prev, cache):
    total = sum(f[3] for f in far)
    size = min(STEP, total)
    steps = total // size
    segments, at = [], 0
    for entry, (_, _, offset, count) in enumerate(far):
        if count >= size:
            segments.append((at // size, (at + count) // size, entry, offset, size, 0))
        else:
            segments.append((at // size, at // size + 1, entry, offset, count, at % size))
        at += count
    whole = lambda *shape: pl.BlockSpec(shape, lambda i, *_: (0,) * len(shape))
    by_step = pl.BlockSpec((WAYS, 8, size * GRAN), lambda i, *_: (0, 0, base // size + i))
    if is_key:
        qp_spec, prev_spec, res_spec = whole(WAYS, 8, 256), ANYWHERE, by_step
    else:
        qp_spec, prev_spec, res_spec = by_step, whole(WAYS, 8, 256), whole(WAYS, 8, 256)
    after = 4 + 2 * len(far) + 2
    aliases = {after + 3: 0}
    if is_key:
        aliases[after + 2] = 1
    return pl.pallas_call(
        functools.partial(assemble_kernel, is_key, base, size, steps, segments),
        grid_spec=pltpu.PrefetchScalarGridSpec(
            num_scalar_prefetch=4,
            grid=(steps,),
            in_specs=[ANYWHERE] * (2 * len(far) + 2) + [whole(ROWS * WAYS, 1, 256), qp_spec, prev_spec, ANYWHERE],
            out_specs=[ANYWHERE, res_spec],
            scratch_shapes=[
                pltpu.VMEM((2, WAYS, size, GRAN, 256), jnp.bfloat16),
                pltpu.VMEM((2, WAYS * GRAN, 128), jnp.float32),
                pltpu.VMEM((2, size, GRAN, WAYS, 256), jnp.bfloat16),
                pltpu.VMEM((WAYS, 8, 256), jnp.float32),
                pltpu.SemaphoreType.DMA((2, 2)),
            ],
        ),
        out_shape=[jax.ShapeDtypeStruct(cache.shape, cache.dtype), jax.ShapeDtypeStruct(prev.shape, prev.dtype)],
        input_output_aliases=aliases,
        compiler_params=pltpu.CompilerParams(dimension_semantics=("arbitrary",), vmem_limit_bytes=VMEM_LIMIT),
        cost_estimate=pl.CostEstimate(flops=10_000_000, bytes_accessed=steps * 4_000_000, transcendentals=0),
        name="assemble_keys" if is_key else "assemble_values",
    )(codes, places, n, me, *[x for f in far for x in f[:2]], near, own, new, qp, prev, cache)


def solution(mesh):
    head_spec = P('dp', None, 'sh', None)
    row_spec = P(('dp', 'sh'))
    full_spec = P(None, None)

    def send(x, d):
        return lax.ppermute(x, 'sh', [(i, i ^ d) for i in range(WAYS)])

    def step(k_prefill, v_prefill, lengths, residual, norm_gain, w_query, w_key, w_value, w_out):
        seq_g = k_prefill.shape[1] // GRAN
        me = lax.axis_index('sh').astype(jnp.int32)
        peers = me ^ jnp.arange(WAYS, dtype=jnp.int32)
        by_peer = lengths[(peers[:, None] * ROWS + jnp.arange(ROWS, dtype=jnp.int32)).reshape(-1)].reshape(WAYS, ROWS)
        mine = by_peer[0]
        prefill = {True: k_prefill.reshape(-1, GRAN, 256), False: v_prefill.reshape(-1, GRAN, 256)}

        def lists(*ds):
            return Lists(jnp.stack([by_peer[d] for d in ds]), jnp.stack([(me ^ d) * ROWS for d in ds])[:, None], seq_g)

        def span(count):
            return jnp.arange(count, dtype=jnp.int32)[None, :]

        def held(which, i):
            src, mixed = which.source(i)
            valid = i < which.size
            return jnp.where(valid, src, 0), jnp.where(valid, mixed, -1)

        far, far_other, close, self_list = lists(2, 3), lists(3, 2), lists(1, 0), lists(0)
        fixed_src, fixed_mix = held(far, span(FIXED))
        close_src, close_mix = held(close, span(ROWS * WIN_G))

        sizes = jnp.sum(jnp.minimum(lengths // GRAN + 1, WIN_G).reshape(WAYS, ROWS), axis=1)
        excess = jnp.max(jnp.sum(jnp.maximum(sizes - FIXED, 0).reshape(WAYS // 2, 2), axis=1))
        level = lax.pmax((excess + 2 * QUANTUM - 1) // (2 * QUANTUM), 'dp')
        spare = QUANTUM * level
        on = active_units(level)
        column = span(SPARE)
        unit = functools.reduce(jnp.add, [(column >= s).astype(jnp.int32) for s in starts_of(UNITS)[1:]])
        skipped, used, place = 0, jnp.zeros_like(column, dtype=bool), column
        for u, size in enumerate(UNITS):
            used = jnp.where(unit == u, on[u], used)
            place = jnp.where(unit == u, column - skipped, place)
            skipped = skipped + jnp.where(on[u], 0, size)
        own_at, other_at = FIXED + place, FIXED + 2 * spare - 1 - place
        src_a, mix_a = held(far, own_at)
        src_b, mix_b = held(far_other, other_at)
        is_own = used & (own_at < far.size)
        is_other = used & (own_at >= far.size) & (other_at < far_other.size)
        spare_src = jnp.where(is_own, src_a, jnp.where(is_other, src_b, 0))
        spare_mix = jnp.where(is_own, mix_a, jnp.where(is_other, mix_b, -1))

        def belongs(i, valid):
            r, g = self_list.at(i)
            return jnp.where(valid & (i < self_list.size), r * WIN_G + g, -1), jnp.clip(i, 0, ROWS * WIN_G - 1)

        parts = [belongs(span(FIXED), True), belongs(own_at, used), belongs(other_at, used)]
        codes = jnp.concatenate([p[0] for p in parts], axis=1)
        places = jnp.concatenate([p[1] for p in parts], axis=1)

        fixed_from, close_from, spare_from = FromTable(fixed_src, fixed_mix), FromTable(close_src, close_mix), FromTable(spare_src, spare_mix)
        fixed_got = {True: [], False: []}
        packed_values = []
        for i, (base, count) in enumerate(zip(starts_of(K_PIECES), K_PIECES)):
            out = pack([prefill[True]], FromLengths(lengths, seq_g) if i == 0 else fixed_from, base, count)
            a = send(out[0], 2)
            b = send(out[1], 3)
            fixed_got[True].append((a, b))
        close_got = {}
        for is_key in (True, False):
            near, own = pack([prefill[is_key]], close_from, 0, ROWS * WIN_G)
            close_got[is_key] = (send(near, 1), own)
        spare_packed = [pack([prefill[True], prefill[False]], spare_from, base, count) for base, count in zip(starts_of(UNITS), UNITS)]
        for base, count in zip(starts_of(V_PIECES), V_PIECES):
            packed_values.append(pack([prefill[False]], fixed_from, base, count))

        resid_f32 = residual.astype(jnp.float32)
        inv_rms = lax.rsqrt(jnp.mean(resid_f32 * resid_f32, axis=-1, keepdims=True) + EPS)
        normed = (resid_f32 * inv_rms * norm_gain.astype(jnp.float32)).astype(jnp.bfloat16)
        q_group = w_query.shape[1] // (WAYS * 256)
        q_heads = jnp.dot(normed, w_query, preferred_element_type=jnp.float32).astype(jnp.bfloat16).reshape(ROWS, WAYS, q_group, 256)
        k_new = jnp.dot(normed, w_key, preferred_element_type=jnp.float32).astype(jnp.bfloat16).reshape(ROWS, WAYS, 256)
        v_new = jnp.dot(normed, w_value, preferred_element_type=jnp.float32).astype(jnp.bfloat16).reshape(ROWS, WAYS, 256)
        q_heads = rotate(q_heads, mine)
        k_new = rotate(k_new, mine)
        new = {True: k_new.astype(jnp.float32).reshape(-1, 1, 256), False: v_new.astype(jnp.float32).reshape(-1, 1, 256)}
        q_pad = jnp.pad(q_heads.transpose(1, 0, 2, 3).reshape(WAYS, ROWS * q_group, 256), ((0, 0), (0, 8 - ROWS * q_group), (0, 0)))
        k_cache, v_cache = cleared(mine, (ROWS, WINDOW, WAYS, 256))
        scores = blank((WAYS, 8, codes.shape[1] * GRAN), jnp.float32)

        def branch(lvl):
            keep = [bool(x) for x in active_units(lvl)]

            def run(pairs):
                return [(send(a, 2), send(b, 3)) if k else (blank(a.shape, a.dtype), blank(b.shape, b.dtype)) for k, (a, b) in zip(keep, pairs)]

            return run

        spare_packed, packed_values, ready = lax.optimization_barrier((spare_packed, packed_values, (new, q_pad, k_cache, v_cache, scores, close_got[True][1], close_got[False][1])))
        new, q_pad, k_cache, v_cache, scores, own_k, own_v = ready
        own = {True: own_k, False: own_v}
        spare_got = lax.switch(level, [branch(x) for x in range(LEVELS)], spare_packed)
        spare_got, packed_values = lax.optimization_barrier((spare_got, packed_values))
        for a, b in packed_values:
            a = send(a, 2)
            b = send(b, 3)
            fixed_got[False].append((a, b))
        forwarded = [(send(b, 1), send(a, 1)) for a, b in spare_got]

        me1 = me.reshape(1)

        def run(is_key, base, far_parts, qp, prev, cache):
            return assemble(is_key, base, codes, places, mine, me1, far_parts, close_got[is_key][0], own[is_key], new[is_key], qp, prev, cache)

        def fixed(pieces, got):
            return [(a, b, 0, count) for (a, b), count in zip(got, pieces)]

        def spares(is_key):
            return [(a, b, 0 if is_key else count, count) for got in (spare_got, forwarded) for (a, b), count in zip(got, UNITS)]

        k_cache, scores = run(True, 0, fixed(K_PIECES, fixed_got[True]), q_pad, scores, k_cache)
        k_cache, scores = run(True, FIXED, spares(True), q_pad, scores, k_cache)
        exp_scores = jnp.exp(scores - jnp.max(scores, axis=-1, keepdims=True))
        weights = (exp_scores / jnp.sum(exp_scores, axis=-1, keepdims=True)).astype(jnp.bfloat16)
        sums = jnp.zeros((WAYS, 8, 256), jnp.float32)
        v_cache, sums = run(False, FIXED, spares(False), weights, sums, v_cache)
        for base, part in zip(starts_of(V_PIECES), fixed(V_PIECES, fixed_got[False])):
            v_cache, sums = run(False, base, [part], weights, sums, v_cache)
        attn_out = sums[:, :ROWS * q_group].astype(jnp.bfloat16).reshape(WAYS, ROWS, q_group * 256).transpose(1, 0, 2).reshape(ROWS, WAYS * q_group * 256)
        resid_out = (resid_f32 + jnp.dot(attn_out, w_out, preferred_element_type=jnp.float32)).astype(jnp.bfloat16)
        return resid_out, k_cache, v_cache

    return jax.shard_map(
        step, mesh=mesh, in_specs=(head_spec, head_spec, P('dp'), P(('dp', 'sh'), None), P(None), full_spec, full_spec, full_spec, full_spec),
        out_specs=(P(('dp', 'sh'), None), row_spec, row_spec), check_vma=False)
```

```python
import functools

import jax
import jax.numpy as jnp
from jax import lax
from jax.experimental import pallas as pl
from jax.experimental.pallas import tpu as pltpu
from jax.sharding import PartitionSpec as P


WINDOW = 4096
THETA = 10000.0
EPS = 1e-5
GRAN = 64
WIN_G = WINDOW // GRAN
STEP = 8
FIXED = 128
UNITS = (32, 16, 8, 4, 4)
SPARE = sum(UNITS)
QUANTUM = UNITS[-1]
LEVELS = SPARE // QUANTUM + 1
K_PIECES = (8, 24, 96)
V_PIECES = (96, 24, 8)
WAYS, ROWS = 4, 3
VMEM_LIMIT = 67_043_328
ANYWHERE = pl.BlockSpec(memory_space=pl.ANY)


def starts_of(sizes):
    return [sum(sizes[:i]) for i in range(len(sizes))]


def active_units(level):
    full = level == LEVELS - 1
    return [full | ((level & (size // QUANTUM)) != 0) for size in UNITS[:-1]] + [full]


def rotate(heads, positions):
    head_dim = heads.shape[-1]
    half_dim = head_dim // 2
    inv_freq = THETA ** (-2.0 * jnp.arange(half_dim, dtype=jnp.float32) / head_dim)
    angles = positions.astype(jnp.float32).reshape(positions.shape + (1,) * (heads.ndim - 1)) * inv_freq
    cos_part = jnp.cos(angles)
    sin_part = jnp.sin(angles)
    first_half = heads[..., :half_dim].astype(jnp.float32)
    second_half = heads[..., half_dim:].astype(jnp.float32)
    return jnp.concatenate([first_half * cos_part - second_half * sin_part, second_half * cos_part + first_half * sin_part], axis=-1).astype(jnp.bfloat16)


def blank(shape, dtype):
    return pl.pallas_call(
        lambda o_ref: None,
        out_shape=jax.ShapeDtypeStruct(shape, dtype),
        out_specs=ANYWHERE,
        name="blank",
    )()


def cleared_kernel(n_ref, k_ref, v_ref, zeros, sem):
    zeros[...] = jnp.zeros_like(zeros)

    def each(act):
        for r in range(ROWS):
            def one(g, carry):
                for ref in (k_ref, v_ref):
                    act(pltpu.make_async_copy(zeros, ref.at[r, pl.ds(g * GRAN, GRAN)], sem))
                return carry

            lax.fori_loop(jnp.minimum(n_ref[r] // GRAN + 1, WIN_G), WIN_G, one, 0)

    each(lambda copy: copy.start())
    each(lambda copy: copy.wait())


def cleared(n, shape):
    return pl.pallas_call(
        cleared_kernel,
        grid_spec=pltpu.PrefetchScalarGridSpec(
            num_scalar_prefetch=1, grid=(1,), in_specs=[], out_specs=[ANYWHERE, ANYWHERE],
            scratch_shapes=[pltpu.VMEM((GRAN, WAYS, 256), jnp.bfloat16), pltpu.SemaphoreType.DMA]),
        out_shape=[jax.ShapeDtypeStruct(shape, jnp.bfloat16)] * 2,
        compiler_params=pltpu.CompilerParams(vmem_limit_bytes=VMEM_LIMIT),
        cost_estimate=pl.CostEstimate(flops=10_000_000, bytes_accessed=20_000_000, transcendentals=0),
        name="cleared",
    )(n)


class Lists:
    def __init__(self, n, row0, seq_g):
        self.n, self.row0, self.seq_g = n, row0, seq_g
        self.lap = n // WINDOW
        self.cut = n % WINDOW
        width = jnp.minimum(n // GRAN + 1, WIN_G)
        self.off1 = width[..., 0:1]
        self.off2 = self.off1 + width[..., 1:2]
        self.size = self.off2 + width[..., 2:3]

    def of_row(self, x, r):
        return jnp.where(r == 0, x[..., 0:1], jnp.where(r == 1, x[..., 1:2], x[..., 2:3]))

    def at(self, i):
        r = (i >= self.off1).astype(jnp.int32) + (i >= self.off2).astype(jnp.int32)
        return r, i - jnp.where(r == 0, 0, jnp.where(r == 1, self.off1, self.off2))

    def source(self, i):
        r, g = self.at(i)
        lap, cut = self.of_row(self.lap, r), self.of_row(self.cut, r)
        older = jnp.maximum(lap - 1, 0)
        base = (self.row0 + r) * self.seq_g
        src = base + jnp.minimum(jnp.where(g <= cut // GRAN, lap, older) * WIN_G + g, self.seq_g - 1)
        mixed = jnp.where(lap >= 1, base + older * WIN_G + g, -1)
        return src, jnp.where(g == cut // GRAN, (mixed + 1) * GRAN + cut % GRAN, -1)


def pack_kernel(base, size, steps, source, *refs):
    num = source.num_scalars
    scalars, refs = refs[:num], refs[num:]
    prefills, outs, (buf, older, sems) = refs[:-5], refs[-5:-3], refs[-3:]
    at = source.reader(*scalars)
    i = pl.program_id(0)
    total = steps * len(prefills)
    slots = buf.shape[0]
    slot = lax.rem(i, slots)

    def by_tensor(step, do):
        for k, ref in enumerate(prefills):
            pl.when((step >= k * steps) & (step < (k + 1) * steps))(functools.partial(do, ref))

    def fetch(step):
        first = base + lax.rem(step, steps) * size
        to = lax.rem(step, slots)

        def from_ref(ref):
            for a in range(2):
                def one(t, found):
                    src, code = at(a, first + t)
                    pltpu.make_async_copy(ref.at[src], buf.at[to, a, t], sems.at[0, to]).start()
                    mixed = code >= GRAN

                    @pl.when(mixed)
                    def _():
                        pltpu.make_async_copy(ref.at[code // GRAN - 1], older.at[to, a, found], sems.at[2, to]).start()

                    return found + mixed.astype(jnp.int32)

                lax.fori_loop(0, size, one, jnp.int32(0))

        by_tensor(step, from_ref)

    def stores(step):
        to = lax.rem(step, slots)
        return [pltpu.make_async_copy(buf.at[to, a], outs[a].at[pl.ds(step * size, size)], sems.at[1, to]) for a in range(2)]

    @pl.when(i == 0)
    def _():
        fetch(i)

    if total > 1:
        @pl.when(i + 1 < total)
        def _():
            if total > slots:
                @pl.when(i + 1 >= slots)
                def _():
                    for copy in stores(i + 1 - slots):
                        copy.wait()
            fetch(i + 1)

    pltpu.make_async_copy(buf.at[slot], buf.at[slot], sems.at[0, slot]).wait()
    first = base + lax.rem(i, steps) * size
    for a in range(2):
        def patch(t, found):
            code = at(a, first + t)[1]
            mixed = code >= GRAN

            @pl.when(code >= 0)
            def _():
                @pl.when(mixed)
                def _():
                    pltpu.make_async_copy(older.at[slot, a, found], older.at[slot, a, found], sems.at[2, slot]).wait()

                newer = lax.broadcasted_iota(jnp.int32, (GRAN, 256), 0) < lax.rem(code, GRAN)
                rest = jnp.where(mixed, older[slot, a, found].astype(jnp.float32), 0.0)
                buf[slot, a, t] = jnp.where(newer, buf[slot, a, t].astype(jnp.float32), rest).astype(jnp.bfloat16)

            return found + mixed.astype(jnp.int32)

        lax.fori_loop(0, size, patch, jnp.int32(0))
    for copy in stores(i):
        copy.start()

    @pl.when(i == total - 1)
    def _():
        for back in range(min(slots, total)):
            for copy in stores(i - back):
                copy.wait()


class FromTable:
    num_scalars = 2

    def __init__(self, src, mix):
        self.scalars = (src, mix)

    def reader(self, src_ref, mix_ref):
        return lambda a, i: (src_ref[a, i], mix_ref[a, i])


class FromLengths:
    num_scalars = 1

    def __init__(self, lengths, seq_g):
        self.scalars = (lengths,)
        self.seq_g = seq_g

    def reader(self, n_ref):
        me = lax.axis_index('sh').astype(jnp.int32)

        def at(a, i):
            row0 = (me ^ (2 + a)) * ROWS
            n = [n_ref[row0 + r] for r in range(ROWS)]
            ends, end = [], 0
            for x in n:
                end = end + jnp.minimum(x // GRAN + 1, WIN_G)
                ends.append(end)
            r = jnp.where(i >= ends[0], 1, 0) + jnp.where(i >= ends[1], 1, 0)
            g = i - jnp.where(r == 0, 0, jnp.where(r == 1, ends[0], ends[1]))
            length = jnp.where(r == 0, n[0], jnp.where(r == 1, n[1], n[2]))
            lap, cut = length // WINDOW, lax.rem(length, WINDOW)
            older = jnp.maximum(lap - 1, 0)
            first = (row0 + r) * self.seq_g
            src = first + jnp.minimum(jnp.where(g <= cut // GRAN, lap, older) * WIN_G + g, self.seq_g - 1)
            mixed = jnp.where(lap >= 1, first + older * WIN_G + g, -1)
            valid = i < ends[2]
            return jnp.where(valid, src, 0), jnp.where(valid & (g == cut // GRAN), (mixed + 1) * GRAN + lax.rem(cut, GRAN), -1)

        return at


def pack(prefills, source, base, count):
    size = next(x for x in (16, 8, 4) if count % x == 0)
    steps = count // size
    total = count * len(prefills)
    return pl.pallas_call(
        functools.partial(pack_kernel, base, size, steps, source),
        grid_spec=pltpu.PrefetchScalarGridSpec(
            num_scalar_prefetch=source.num_scalars,
            grid=(steps * len(prefills),),
            in_specs=[ANYWHERE] * len(prefills),
            out_specs=[ANYWHERE] * 2,
            scratch_shapes=[pltpu.VMEM((3, 2, size, GRAN, 256), jnp.bfloat16), pltpu.VMEM((3, 2, 2 * ROWS + 1, GRAN, 256), jnp.bfloat16), pltpu.SemaphoreType.DMA((3, 3))],
        ),
        out_shape=[jax.ShapeDtypeStruct((total, GRAN, 256), jnp.bfloat16)] * 2,
        compiler_params=pltpu.CompilerParams(dimension_semantics=("arbitrary",), vmem_limit_bytes=VMEM_LIMIT),
        cost_estimate=pl.CostEstimate(flops=10_000_000, bytes_accessed=total * 130_000, transcendentals=0),
        name="pack",
    )(*source.scalars, *prefills)


def assemble_kernel(is_key, base, size, steps, segments, code_ref, idx_ref, n_ref, me_ref, *refs):
    num_far = 2 * (1 + max(s[2] for s in segments))
    far_refs = refs[:num_far]
    near_ref, own_ref, new_ref, qp_ref, prev_ref, _, cache_ref, res_ref, xb, mix, ob, acc, sems = refs[num_far:]
    i = pl.program_id(0)
    me = me_ref[0]
    slot = lax.rem(i, 2)

    def code_at(step, t):
        return code_ref[0, base + step * size + t]

    def active_at(step):
        return functools.reduce(jnp.maximum, [code_at(step, t) for t in range(size)]) >= 0

    def read(step, buf):
        @pl.when(active_at(step))
        def _():
            for begin, end, entry, offset, count, place in segments:
                @pl.when((step >= begin) & (step < end))
                def _():
                    for d in range(2):
                        pltpu.make_async_copy(far_refs[2 * entry + d].at[pl.ds(offset + (step - begin) * size, count)], xb.at[buf, me ^ (2 + d), pl.ds(place, count)], sems.at[0, buf]).start()

            def one(t, carry):
                at = idx_ref[0, base + step * size + t]
                pltpu.make_async_copy(near_ref.at[at], xb.at[buf, me ^ 1, t], sems.at[0, buf]).start()
                pltpu.make_async_copy(own_ref.at[at], xb.at[buf, me, t], sems.at[0, buf]).start()
                return carry

            lax.fori_loop(0, size, one, 0)

    def write(step, t, buf):
        code = code_at(step, t)
        return pltpu.make_async_copy(ob.at[buf, t], cache_ref.at[code // WIN_G, pl.ds(lax.rem(code, WIN_G) * GRAN, GRAN)], sems.at[1, buf])

    def written(step, buf):
        def one(t, carry):
            @pl.when(code_at(step, t) >= 0)
            def _():
                write(step, t, buf).wait()

            return carry

        lax.fori_loop(0, size, one, 0)

    @pl.when(i == 0)
    def _():
        read(i, slot)
        if not is_key:
            acc[...] = prev_ref[...]

    if steps > 1:
        @pl.when(i + 1 < steps)
        def _():
            read(i + 1, 1 - slot)

    if steps > 2:
        @pl.when(i >= 2)
        def _():
            written(i - 2, slot)

    active = active_at(i)

    @pl.when(active)
    def _():
        pltpu.make_async_copy(xb.at[slot], xb.at[slot], sems.at[0, slot]).wait()

        def one(t, carry):
            code = code_at(i, t)

            @pl.when(code < 0)
            def _():
                for h in range(WAYS):
                    xb[slot, h, t] = jnp.zeros((GRAN, 256), jnp.bfloat16)

            for r in range(ROWS):
                cut = lax.rem(n_ref[r], WINDOW)

                @pl.when(code == r * WIN_G + cut // GRAN)
                def _():
                    here = lax.broadcasted_iota(jnp.int32, (GRAN, 256), 0) == lax.rem(cut, GRAN)
                    for h in range(WAYS):
                        new = jnp.broadcast_to(new_ref[r * WAYS + h], (GRAN, 256))
                        xb[slot, h, t] = jnp.where(here, new, xb[slot, h, t].astype(jnp.float32)).astype(jnp.bfloat16)

            @pl.when(code >= 0)
            def _():
                for h in range(WAYS):
                    x = xb[slot, h, t].astype(jnp.float32)
                    for half in range(2):
                        mix[half, pl.ds(h, GRAN, stride=WAYS), :] = x[:, half * 128:(half + 1) * 128]
                joined = jnp.concatenate([mix[half].astype(jnp.bfloat16) for half in range(2)], axis=1)
                ob[slot, t] = joined.reshape(GRAN, WAYS, 256)
                write(i, t, slot).start()

            return carry

        lax.fori_loop(0, size, one, 0)

        lanes = size * GRAN
        if is_key:
            lane = lax.broadcasted_iota(jnp.int32, (8, lanes), 1)
            row = lax.broadcasted_iota(jnp.int32, (8, lanes), 0) // 2
            code = jnp.full((8, lanes), -1, jnp.int32)
            for t in range(size):
                code = jnp.where(lane // GRAN == t, code_at(i, t), code)
            length = jnp.where(row == 0, n_ref[0], jnp.where(row == 1, n_ref[1], n_ref[2]))
            place = (code % WIN_G) * GRAN + lane % GRAN
            live = (code >= 0) & (code // WIN_G == row) & ((length >= WINDOW) | (place <= length))
            for h in range(WAYS):
                s = lax.dot_general(qp_ref[h], xb[slot, h].reshape(lanes, 256), (((1,), (1,)), ((), ())), preferred_element_type=jnp.float32)
                res_ref[h] = jnp.where(live, s / 16.0, -jnp.inf)
        else:
            for h in range(WAYS):
                acc[h] += jnp.dot(qp_ref[h], xb[slot, h].reshape(lanes, 256), preferred_element_type=jnp.float32)

    if is_key:
        @pl.when(jnp.logical_not(active))
        def _():
            res_ref[...] = jnp.full_like(res_ref, -jnp.inf)

    @pl.when(i == steps - 1)
    def _():
        if not is_key:
            res_ref[...] = acc[...]
        if steps >= 2:
            written(i - 1, 1 - slot)
        written(i, slot)


def assemble(is_key, base, codes, places, n, me, far, near, own, new, qp, prev, cache):
    total = sum(f[3] for f in far)
    size = min(STEP, total)
    steps = total // size
    segments, at = [], 0
    for entry, (_, _, offset, count) in enumerate(far):
        if count >= size:
            segments.append((at // size, (at + count) // size, entry, offset, size, 0))
        else:
            segments.append((at // size, at // size + 1, entry, offset, count, at % size))
        at += count
    whole = lambda *shape: pl.BlockSpec(shape, lambda i, *_: (0,) * len(shape))
    by_step = pl.BlockSpec((WAYS, 8, size * GRAN), lambda i, *_: (0, 0, base // size + i))
    if is_key:
        qp_spec, prev_spec, res_spec = whole(WAYS, 8, 256), ANYWHERE, by_step
    else:
        qp_spec, prev_spec, res_spec = by_step, whole(WAYS, 8, 256), whole(WAYS, 8, 256)
    after = 4 + 2 * len(far) + 2
    aliases = {after + 3: 0}
    if is_key:
        aliases[after + 2] = 1
    return pl.pallas_call(
        functools.partial(assemble_kernel, is_key, base, size, steps, segments),
        grid_spec=pltpu.PrefetchScalarGridSpec(
            num_scalar_prefetch=4,
            grid=(steps,),
            in_specs=[ANYWHERE] * (2 * len(far) + 2) + [whole(ROWS * WAYS, 1, 256), qp_spec, prev_spec, ANYWHERE],
            out_specs=[ANYWHERE, res_spec],
            scratch_shapes=[
                pltpu.VMEM((2, WAYS, size, GRAN, 256), jnp.bfloat16),
                pltpu.VMEM((2, WAYS * GRAN, 128), jnp.float32),
                pltpu.VMEM((2, size, GRAN, WAYS, 256), jnp.bfloat16),
                pltpu.VMEM((WAYS, 8, 256), jnp.float32),
                pltpu.SemaphoreType.DMA((2, 2)),
            ],
        ),
        out_shape=[jax.ShapeDtypeStruct(cache.shape, cache.dtype), jax.ShapeDtypeStruct(prev.shape, prev.dtype)],
        input_output_aliases=aliases,
        compiler_params=pltpu.CompilerParams(dimension_semantics=("arbitrary",), vmem_limit_bytes=VMEM_LIMIT),
        cost_estimate=pl.CostEstimate(flops=10_000_000, bytes_accessed=steps * 4_000_000, transcendentals=0),
        name="assemble_keys" if is_key else "assemble_values",
    )(codes, places, n, me, *[x for f in far for x in f[:2]], near, own, new, qp, prev, cache)


def solution(mesh):
    head_spec = P('dp', None, 'sh', None)
    row_spec = P(('dp', 'sh'))
    full_spec = P(None, None)

    def send(x, d):
        return lax.ppermute(x, 'sh', [(i, i ^ d) for i in range(WAYS)])

    def step(k_prefill, v_prefill, lengths, residual, norm_gain, w_query, w_key, w_value, w_out):
        seq_g = k_prefill.shape[1] // GRAN
        me = lax.axis_index('sh').astype(jnp.int32)
        peers = me ^ jnp.arange(WAYS, dtype=jnp.int32)
        by_peer = lengths[(peers[:, None] * ROWS + jnp.arange(ROWS, dtype=jnp.int32)).reshape(-1)].reshape(WAYS, ROWS)
        mine = by_peer[0]
        prefill = {True: k_prefill.reshape(-1, GRAN, 256), False: v_prefill.reshape(-1, GRAN, 256)}

        def lists(*ds):
            return Lists(jnp.stack([by_peer[d] for d in ds]), jnp.stack([(me ^ d) * ROWS for d in ds])[:, None], seq_g)

        def span(count):
            return jnp.arange(count, dtype=jnp.int32)[None, :]

        def held(which, i):
            src, mixed = which.source(i)
            valid = i < which.size
            return jnp.where(valid, src, 0), jnp.where(valid, mixed, -1)

        far, far_other, close, self_list = lists(2, 3), lists(3, 2), lists(1, 0), lists(0)
        fixed_src, fixed_mix = held(far, span(FIXED))
        close_src, close_mix = held(close, span(ROWS * WIN_G))

        sizes = jnp.sum(jnp.minimum(lengths // GRAN + 1, WIN_G).reshape(WAYS, ROWS), axis=1)
        excess = jnp.max(jnp.sum(jnp.maximum(sizes - FIXED, 0).reshape(WAYS // 2, 2), axis=1))
        level = lax.pmax((excess + 2 * QUANTUM - 1) // (2 * QUANTUM), 'dp')
        spare = QUANTUM * level
        on = active_units(level)
        column = span(SPARE)
        unit = functools.reduce(jnp.add, [(column >= s).astype(jnp.int32) for s in starts_of(UNITS)[1:]])
        skipped, used, place = 0, jnp.zeros_like(column, dtype=bool), column
        for u, size in enumerate(UNITS):
            used = jnp.where(unit == u, on[u], used)
            place = jnp.where(unit == u, column - skipped, place)
            skipped = skipped + jnp.where(on[u], 0, size)
        own_at, other_at = FIXED + place, FIXED + 2 * spare - 1 - place
        src_a, mix_a = held(far, own_at)
        src_b, mix_b = held(far_other, other_at)
        is_own = used & (own_at < far.size)
        is_other = used & (own_at >= far.size) & (other_at < far_other.size)
        spare_src = jnp.where(is_own, src_a, jnp.where(is_other, src_b, 0))
        spare_mix = jnp.where(is_own, mix_a, jnp.where(is_other, mix_b, -1))

        def belongs(i, valid):
            r, g = self_list.at(i)
            return jnp.where(valid & (i < self_list.size), r * WIN_G + g, -1), jnp.clip(i, 0, ROWS * WIN_G - 1)

        parts = [belongs(span(FIXED), True), belongs(own_at, used), belongs(other_at, used)]
        codes = jnp.concatenate([p[0] for p in parts], axis=1)
        places = jnp.concatenate([p[1] for p in parts], axis=1)

        fixed_from, close_from, spare_from = FromTable(fixed_src, fixed_mix), FromTable(close_src, close_mix), FromTable(spare_src, spare_mix)
        fixed_got = {True: [], False: []}
        packed_values = []
        for i, (base, count) in enumerate(zip(starts_of(K_PIECES), K_PIECES)):
            out = pack([prefill[True]], FromLengths(lengths, seq_g) if i == 0 else fixed_from, base, count)
            a = send(out[0], 2)
            b = send(out[1], 3)
            fixed_got[True].append((a, b))
        close_got = {}
        for is_key in (True, False):
            near, own = pack([prefill[is_key]], close_from, 0, ROWS * WIN_G)
            close_got[is_key] = (send(near, 1), own)
        spare_packed = [pack([prefill[True], prefill[False]], spare_from, base, count) for base, count in zip(starts_of(UNITS), UNITS)]
        for base, count in zip(starts_of(V_PIECES), V_PIECES):
            packed_values.append(pack([prefill[False]], fixed_from, base, count))

        resid_f32 = residual.astype(jnp.float32)
        inv_rms = lax.rsqrt(jnp.mean(resid_f32 * resid_f32, axis=-1, keepdims=True) + EPS)
        normed = (resid_f32 * inv_rms * norm_gain.astype(jnp.float32)).astype(jnp.bfloat16)
        q_group = w_query.shape[1] // (WAYS * 256)
        q_heads = jnp.dot(normed, w_query, preferred_element_type=jnp.float32).astype(jnp.bfloat16).reshape(ROWS, WAYS, q_group, 256)
        k_new = jnp.dot(normed, w_key, preferred_element_type=jnp.float32).astype(jnp.bfloat16).reshape(ROWS, WAYS, 256)
        v_new = jnp.dot(normed, w_value, preferred_element_type=jnp.float32).astype(jnp.bfloat16).reshape(ROWS, WAYS, 256)
        q_heads = rotate(q_heads, mine)
        k_new = rotate(k_new, mine)
        new = {True: k_new.astype(jnp.float32).reshape(-1, 1, 256), False: v_new.astype(jnp.float32).reshape(-1, 1, 256)}
        q_pad = jnp.pad(q_heads.transpose(1, 0, 2, 3).reshape(WAYS, ROWS * q_group, 256), ((0, 0), (0, 8 - ROWS * q_group), (0, 0)))
        k_cache, v_cache = cleared(mine, (ROWS, WINDOW, WAYS, 256))
        scores = blank((WAYS, 8, codes.shape[1] * GRAN), jnp.float32)

        def branch(lvl):
            keep = [bool(x) for x in active_units(lvl)]

            def run(pairs):
                return [(send(a, 2), send(b, 3)) if k else (blank(a.shape, a.dtype), blank(b.shape, b.dtype)) for k, (a, b) in zip(keep, pairs)]

            return run

        spare_packed, packed_values, ready = lax.optimization_barrier((spare_packed, packed_values, (new, q_pad, k_cache, v_cache, scores, close_got[True][1], close_got[False][1])))
        new, q_pad, k_cache, v_cache, scores, own_k, own_v = ready
        own = {True: own_k, False: own_v}
        spare_got = lax.switch(level, [branch(x) for x in range(LEVELS)], spare_packed)
        spare_got, packed_values = lax.optimization_barrier((spare_got, packed_values))
        for a, b in packed_values:
            a = send(a, 2)
            b = send(b, 3)
            fixed_got[False].append((a, b))
        forwarded = [(send(b, 1), send(a, 1)) for a, b in spare_got]

        me1 = me.reshape(1)

        def run(is_key, base, far_parts, qp, prev, cache):
            return assemble(is_key, base, codes, places, mine, me1, far_parts, close_got[is_key][0], own[is_key], new[is_key], qp, prev, cache)

        def fixed(pieces, got):
            return [(a, b, 0, count) for (a, b), count in zip(got, pieces)]

        def spares(is_key):
            return [(a, b, 0 if is_key else count, count) for got in (spare_got, forwarded) for (a, b), count in zip(got, UNITS)]

        k_cache, scores = run(True, 0, fixed(K_PIECES, fixed_got[True]), q_pad, scores, k_cache)
        k_cache, scores = run(True, FIXED, spares(True), q_pad, scores, k_cache)
        exp_scores = jnp.exp(scores - jnp.max(scores, axis=-1, keepdims=True))
        weights = (exp_scores / jnp.sum(exp_scores, axis=-1, keepdims=True)).astype(jnp.bfloat16)
        sums = jnp.zeros((WAYS, 8, 256), jnp.float32)
        v_cache, sums = run(False, FIXED, spares(False), weights, sums, v_cache)
        for base, part in zip(starts_of(V_PIECES), fixed(V_PIECES, fixed_got[False])):
            v_cache, sums = run(False, base, [part], weights, sums, v_cache)
        attn_out = sums[:, :ROWS * q_group].astype(jnp.bfloat16).reshape(WAYS, ROWS, q_group * 256).transpose(1, 0, 2).reshape(ROWS, WAYS * q_group * 256)
        resid_out = (resid_f32 + jnp.dot(attn_out, w_out, preferred_element_type=jnp.float32)).astype(jnp.bfloat16)
        return resid_out, k_cache, v_cache

    return jax.shard_map(
        step, mesh=mesh, in_specs=(head_spec, head_spec, P('dp'), P(('dp', 'sh'), None), P(None), full_spec, full_spec, full_spec, full_spec),
        out_specs=(P(('dp', 'sh'), None), row_spec, row_spec), check_vma=False)
```

```python
import functools

import jax
import jax.numpy as jnp
from jax import lax
from jax.experimental import pallas as pl
from jax.experimental.pallas import tpu as pltpu
from jax.sharding import PartitionSpec as P


WINDOW = 4096
THETA = 10000.0
EPS = 1e-5
GRAN = 64
WIN_G = WINDOW // GRAN
STEP = 8
FIXED = 128
UNITS = (32, 16, 8, 4, 4)
SPARE = sum(UNITS)
QUANTUM = UNITS[-1]
LEVELS = SPARE // QUANTUM + 1
K_PIECES = (8, 24, 96)
V_PIECES = (96, 24, 8)
CROSS = 32
ELSEWHERE = 1 << 20
WAYS, ROWS = 4, 3
VMEM_LIMIT = 67_043_328
HALF = CROSS // 2
KV = (True, False)
BOTH = range(2)
SERIAL = pltpu.CompilerParams(dimension_semantics=("arbitrary",), vmem_limit_bytes=VMEM_LIMIT)
ANYWHERE = pl.BlockSpec(memory_space=pl.ANY)


beside = functools.partial(jnp.concatenate, axis=1)


def cost(moved):
    return pl.CostEstimate(flops=10_000_000, bytes_accessed=moved, transcendentals=0)


def starts_of(sizes):
    return [sum(sizes[:i]) for i in range(len(sizes))]


def active_units(level):
    full = level == LEVELS - 1
    return [full | ((level & (size // QUANTUM)) != 0) for size in UNITS[:-1]] + [full]


def rotate(heads, positions):
    head_dim = heads.shape[-1]
    half_dim = head_dim // 2
    inv_freq = THETA ** (-2.0 * jnp.arange(half_dim, dtype=jnp.float32) / head_dim)
    angles = positions.astype(jnp.float32).reshape(positions.shape + (1,) * (heads.ndim - 1)) * inv_freq
    cos_part = jnp.cos(angles)
    sin_part = jnp.sin(angles)
    first_half = heads[..., :half_dim].astype(jnp.float32)
    second_half = heads[..., half_dim:].astype(jnp.float32)
    return jnp.concatenate([first_half * cos_part - second_half * sin_part, second_half * cos_part + first_half * sin_part], axis=-1).astype(jnp.bfloat16)


def blank(shape, dtype):
    return pl.pallas_call(
        lambda o_ref: None,
        out_shape=jax.ShapeDtypeStruct(shape, dtype),
        out_specs=ANYWHERE,
        name="blank",
    )()


def cleared_kernel(n_ref, k_ref, v_ref, zeros, sem):
    zeros[...] = jnp.zeros_like(zeros)

    def each(act):
        for r in range(ROWS):
            def one(g, carry):
                for ref in (k_ref, v_ref):
                    act(pltpu.make_async_copy(zeros, ref.at[r, pl.ds(g * GRAN, GRAN)], sem))
                return carry

            lax.fori_loop(jnp.minimum(n_ref[r] // GRAN + 1, WIN_G), WIN_G, one, 0)

    each(lambda copy: copy.start())
    each(lambda copy: copy.wait())


def cleared(n, shape):
    return pl.pallas_call(
        cleared_kernel,
        grid_spec=pltpu.PrefetchScalarGridSpec(
            num_scalar_prefetch=1, grid=(1,), in_specs=[], out_specs=[ANYWHERE, ANYWHERE],
            scratch_shapes=[pltpu.VMEM((GRAN, WAYS, 256), jnp.bfloat16), pltpu.SemaphoreType.DMA]),
        out_shape=[jax.ShapeDtypeStruct(shape, jnp.bfloat16)] * 2,
        compiler_params=pltpu.CompilerParams(vmem_limit_bytes=VMEM_LIMIT),
        cost_estimate=cost(20_000_000),
        name="cleared",
    )(n)


class Lists:
    def __init__(self, n, row0, seq_g):
        self.n, self.row0, self.seq_g = n, row0, seq_g
        self.lap = n // WINDOW
        self.cut = n % WINDOW
        width = jnp.minimum(n // GRAN + 1, WIN_G)
        self.off1 = width[..., 0:1]
        self.off2 = self.off1 + width[..., 1:2]
        self.size = self.off2 + width[..., 2:3]

    def of_row(self, x, r):
        return jnp.where(r == 0, x[..., 0:1], jnp.where(r == 1, x[..., 1:2], x[..., 2:3]))

    def at(self, i):
        r = (i >= self.off1).astype(jnp.int32) + (i >= self.off2).astype(jnp.int32)
        return r, i - jnp.where(r == 0, 0, jnp.where(r == 1, self.off1, self.off2))

    def source(self, i):
        r, g = self.at(i)
        lap, cut = self.of_row(self.lap, r), self.of_row(self.cut, r)
        older = jnp.maximum(lap - 1, 0)
        base = (self.row0 + r) * self.seq_g
        src = base + jnp.minimum(jnp.where(g <= cut // GRAN, lap, older) * WIN_G + g, self.seq_g - 1)
        mixed = jnp.where(lap >= 1, base + older * WIN_G + g, -1)
        return src, jnp.where(g == cut // GRAN, (mixed + 1) * GRAN + cut % GRAN, -1)


def pack_kernel(base, size, steps, source, extra, *refs):
    num = source.num_scalars
    scalars, refs = refs[:num], refs[num:]
    prefills, extras, outs, (buf, older, sems) = refs[:-5 - extra], refs[-5 - extra:-5], refs[-5:-3], refs[-3:]
    at = source.reader(*scalars)
    i = pl.program_id(0)
    total = steps * len(prefills)
    slots = buf.shape[0]
    slot = lax.rem(i, slots)

    def by_tensor(step, do):
        for k, ref in enumerate(prefills):
            pl.when((step >= k * steps) & (step < (k + 1) * steps))(functools.partial(do, k, ref))

    def fetch(step):
        first = base + lax.rem(step, steps) * size
        to = lax.rem(step, slots)

        def from_ref(k, ref):
            for a in BOTH:
                def one(t, found):
                    src, code = at(a, first + t)
                    if not extras:
                        pltpu.make_async_copy(ref.at[src], buf.at[to, a, t], sems.at[0, to]).start()
                    else:
                        @pl.when(src < ELSEWHERE)
                        def _():
                            pltpu.make_async_copy(ref.at[src], buf.at[to, a, t], sems.at[0, to]).start()

                        for e, other in enumerate(extras):

                            @pl.when((src >= ELSEWHERE + e * HALF) & (src < ELSEWHERE + (e + 1) * HALF))
                            def _():
                                pltpu.make_async_copy(other.at[src - ELSEWHERE + (k - e) * HALF], buf.at[to, a, t], sems.at[0, to]).start()
                    mixed = code >= GRAN

                    @pl.when(mixed)
                    def _():
                        pltpu.make_async_copy(ref.at[code // GRAN - 1], older.at[to, a, found], sems.at[2, to]).start()

                    return found + mixed.astype(jnp.int32)

                lax.fori_loop(0, size, one, jnp.int32(0))

        by_tensor(step, from_ref)

    def stores(step):
        to = lax.rem(step, slots)
        return [pltpu.make_async_copy(buf.at[to, a], outs[a].at[pl.ds(step * size, size)], sems.at[1, to]) for a in BOTH]

    @pl.when(i == 0)
    def _():
        fetch(i)

    if total > 1:
        @pl.when(i + 1 < total)
        def _():
            if total > slots:
                @pl.when(i + 1 >= slots)
                def _():
                    for copy in stores(i + 1 - slots):
                        copy.wait()
            fetch(i + 1)

    pltpu.make_async_copy(buf.at[slot], buf.at[slot], sems.at[0, slot]).wait()
    first = base + lax.rem(i, steps) * size
    for a in BOTH:
        def patch(t, found):
            code = at(a, first + t)[1]
            mixed = code >= GRAN

            @pl.when(code >= 0)
            def _():
                @pl.when(mixed)
                def _():
                    pltpu.make_async_copy(older.at[slot, a, found], older.at[slot, a, found], sems.at[2, slot]).wait()

                newer = lax.broadcasted_iota(jnp.int32, (GRAN, 256), 0) < lax.rem(code, GRAN)
                rest = jnp.where(mixed, older[slot, a, found].astype(jnp.float32), 0.0)
                buf[slot, a, t] = jnp.where(newer, buf[slot, a, t].astype(jnp.float32), rest).astype(jnp.bfloat16)

            return found + mixed.astype(jnp.int32)

        lax.fori_loop(0, size, patch, jnp.int32(0))
    for copy in stores(i):
        copy.start()

    @pl.when(i == total - 1)
    def _():
        for back in range(min(slots, total)):
            for copy in stores(i - back):
                copy.wait()


class FromTable:
    num_scalars = 2

    def __init__(self, src, mix):
        self.scalars = (src, mix)

    def reader(self, src_ref, mix_ref):
        return lambda a, i: (src_ref[a, i], mix_ref[a, i])


class FromLengths:
    num_scalars = 1

    def __init__(self, lengths, seq_g):
        self.scalars = (lengths,)
        self.seq_g = seq_g

    def reader(self, n_ref):
        me = lax.axis_index('sh').astype(jnp.int32)

        def at(a, i):
            row0 = (me ^ (2 + a)) * ROWS
            n = [n_ref[row0 + r] for r in range(ROWS)]
            ends, end = [], 0
            for x in n:
                end = end + jnp.minimum(x // GRAN + 1, WIN_G)
                ends.append(end)
            r = jnp.where(i >= ends[0], 1, 0) + jnp.where(i >= ends[1], 1, 0)
            g = i - jnp.where(r == 0, 0, jnp.where(r == 1, ends[0], ends[1]))
            length = jnp.where(r == 0, n[0], jnp.where(r == 1, n[1], n[2]))
            lap, cut = length // WINDOW, lax.rem(length, WINDOW)
            older = jnp.maximum(lap - 1, 0)
            first = (row0 + r) * self.seq_g
            src = first + jnp.minimum(jnp.where(g <= cut // GRAN, lap, older) * WIN_G + g, self.seq_g - 1)
            mixed = jnp.where(lap >= 1, first + older * WIN_G + g, -1)
            valid = i < ends[2]
            return jnp.where(valid, src, 0), jnp.where(valid & (g == cut // GRAN), (mixed + 1) * GRAN + lax.rem(cut, GRAN), -1)

        return at


def pack(prefills, source, base, count, extras=()):
    size = next(x for x in (16, 8, 4) if count % x == 0)
    steps = count // size
    total = count * len(prefills)
    return pl.pallas_call(
        functools.partial(pack_kernel, base, size, steps, source, len(extras)),
        grid_spec=pltpu.PrefetchScalarGridSpec(
            num_scalar_prefetch=source.num_scalars,
            grid=(steps * len(prefills),),
            in_specs=[ANYWHERE] * (len(prefills) + len(extras)),
            out_specs=[ANYWHERE] * 2,
            scratch_shapes=[pltpu.VMEM((3, 2, size, GRAN, 256), jnp.bfloat16), pltpu.VMEM((3, 2, 2 * ROWS + 1, GRAN, 256), jnp.bfloat16), pltpu.SemaphoreType.DMA((3, 3))],
        ),
        out_shape=[jax.ShapeDtypeStruct((total, GRAN, 256), jnp.bfloat16)] * 2,
        compiler_params=SERIAL,
        cost_estimate=cost(total * 130_000),
        name="pack",
    )(*source.scalars, *prefills, *extras)


def assemble_kernel(is_key, base, size, steps, segments, code_ref, idx_ref, n_ref, me_ref, *refs):
    num_far = 2 * (1 + max(s[2] for s in segments))
    far_refs = refs[:num_far]
    near_ref, own_ref, new_ref, qp_ref, prev_ref, _, cache_ref, res_ref, xb, mix, ob, acc, sems = refs[num_far:]
    i = pl.program_id(0)
    me = me_ref[0]
    slot = lax.rem(i, 2)

    def code_at(step, t):
        return code_ref[0, base + step * size + t]

    def active_at(step):
        return functools.reduce(jnp.maximum, [code_at(step, t) for t in range(size)]) >= 0

    def read(step, buf):
        @pl.when(active_at(step))
        def _():
            for begin, end, entry, offsets, count, place in segments:
                @pl.when((step >= begin) & (step < end))
                def _():
                    for d in BOTH:
                        pltpu.make_async_copy(far_refs[2 * entry + d].at[pl.ds(offsets[d] + (step - begin) * size, count)], xb.at[buf, me ^ (2 + d), pl.ds(place, count)], sems.at[0, buf]).start()

            def one(t, carry):
                at = idx_ref[0, base + step * size + t]
                pltpu.make_async_copy(near_ref.at[at], xb.at[buf, me ^ 1, t], sems.at[0, buf]).start()
                pltpu.make_async_copy(own_ref.at[at], xb.at[buf, me, t], sems.at[0, buf]).start()
                return carry

            lax.fori_loop(0, size, one, 0)

    def write(step, t, buf):
        code = code_at(step, t)
        return pltpu.make_async_copy(ob.at[buf, t], cache_ref.at[code // WIN_G, pl.ds(lax.rem(code, WIN_G) * GRAN, GRAN)], sems.at[1, buf])

    def written(step, buf):
        def one(t, carry):
            @pl.when(code_at(step, t) >= 0)
            def _():
                write(step, t, buf).wait()

            return carry

        lax.fori_loop(0, size, one, 0)

    @pl.when(i == 0)
    def _():
        read(i, slot)
        if not is_key:
            acc[...] = prev_ref[...]

    if steps > 1:
        @pl.when(i + 1 < steps)
        def _():
            read(i + 1, 1 - slot)

    if steps > 2:
        @pl.when(i >= 2)
        def _():
            written(i - 2, slot)

    active = active_at(i)

    @pl.when(active)
    def _():
        pltpu.make_async_copy(xb.at[slot], xb.at[slot], sems.at[0, slot]).wait()

        def one(t, carry):
            code = code_at(i, t)

            @pl.when(code < 0)
            def _():
                for h in range(WAYS):
                    xb[slot, h, t] = jnp.zeros((GRAN, 256), jnp.bfloat16)

            for r in range(ROWS):
                cut = lax.rem(n_ref[r], WINDOW)

                @pl.when(code == r * WIN_G + cut // GRAN)
                def _():
                    here = lax.broadcasted_iota(jnp.int32, (GRAN, 256), 0) == lax.rem(cut, GRAN)
                    for h in range(WAYS):
                        new = jnp.broadcast_to(new_ref[r * WAYS + h], (GRAN, 256))
                        xb[slot, h, t] = jnp.where(here, new, xb[slot, h, t].astype(jnp.float32)).astype(jnp.bfloat16)

            @pl.when(code >= 0)
            def _():
                for h in range(WAYS):
                    x = xb[slot, h, t].astype(jnp.float32)
                    for half in BOTH:
                        mix[half, pl.ds(h, GRAN, stride=WAYS), :] = x[:, half * 128:(half + 1) * 128]
                joined = beside([mix[half].astype(jnp.bfloat16) for half in BOTH])
                ob[slot, t] = joined.reshape(GRAN, WAYS, 256)
                write(i, t, slot).start()

            return carry

        lax.fori_loop(0, size, one, 0)

        lanes = size * GRAN
        if is_key:
            lane = lax.broadcasted_iota(jnp.int32, (8, lanes), 1)
            row = lax.broadcasted_iota(jnp.int32, (8, lanes), 0) // 2
            code = jnp.full((8, lanes), -1, jnp.int32)
            for t in range(size):
                code = jnp.where(lane // GRAN == t, code_at(i, t), code)
            length = jnp.where(row == 0, n_ref[0], jnp.where(row == 1, n_ref[1], n_ref[2]))
            place = (code % WIN_G) * GRAN + lane % GRAN
            live = (code >= 0) & (code // WIN_G == row) & ((length >= WINDOW) | (place <= length))
            for h in range(WAYS):
                s = lax.dot_general(qp_ref[h], xb[slot, h].reshape(lanes, 256), (((1,), (1,)), ((), ())), preferred_element_type=jnp.float32)
                res_ref[h] = jnp.where(live, s / 16.0, -jnp.inf)
        else:
            for h in range(WAYS):
                acc[h] += jnp.dot(qp_ref[h], xb[slot, h].reshape(lanes, 256), preferred_element_type=jnp.float32)

    if is_key:
        @pl.when(jnp.logical_not(active))
        def _():
            res_ref[...] = jnp.full_like(res_ref, -jnp.inf)

    @pl.when(i == steps - 1)
    def _():
        if not is_key:
            res_ref[...] = acc[...]
        if steps >= 2:
            written(i - 1, 1 - slot)
        written(i, slot)


def assemble(is_key, base, codes, places, n, me, far, near, own, new, qp, prev, cache):
    total = sum(f[3] for f in far)
    size = min(STEP, total)
    steps = total // size
    segments, at = [], 0
    for entry, (_, _, offsets, count) in enumerate(far):
        if count >= size:
            segments.append((at // size, (at + count) // size, entry, offsets, size, 0))
        else:
            segments.append((at // size, at // size + 1, entry, offsets, count, at % size))
        at += count
    whole = lambda *shape: pl.BlockSpec(shape, lambda i, *_: (0,) * len(shape))
    by_step = pl.BlockSpec((WAYS, 8, size * GRAN), lambda i, *_: (0, 0, base // size + i))
    if is_key:
        qp_spec, prev_spec, res_spec = whole(WAYS, 8, 256), ANYWHERE, by_step
    else:
        qp_spec, prev_spec, res_spec = by_step, whole(WAYS, 8, 256), whole(WAYS, 8, 256)
    after = 4 + 2 * len(far) + 2
    aliases = {after + 3: 0}
    if is_key:
        aliases[after + 2] = 1
    return pl.pallas_call(
        functools.partial(assemble_kernel, is_key, base, size, steps, segments),
        grid_spec=pltpu.PrefetchScalarGridSpec(
            num_scalar_prefetch=4,
            grid=(steps,),
            in_specs=[ANYWHERE] * (2 * len(far) + 2) + [whole(ROWS * WAYS, 1, 256), qp_spec, prev_spec, ANYWHERE],
            out_specs=[ANYWHERE, res_spec],
            scratch_shapes=[
                pltpu.VMEM((2, WAYS, size, GRAN, 256), jnp.bfloat16),
                pltpu.VMEM((2, WAYS * GRAN, 128), jnp.float32),
                pltpu.VMEM((2, size, GRAN, WAYS, 256), jnp.bfloat16),
                pltpu.VMEM((WAYS, 8, 256), jnp.float32),
                pltpu.SemaphoreType.DMA((2, 2)),
            ],
        ),
        out_shape=[jax.ShapeDtypeStruct(cache.shape, cache.dtype), jax.ShapeDtypeStruct(prev.shape, prev.dtype)],
        input_output_aliases=aliases,
        compiler_params=SERIAL,
        cost_estimate=cost(steps * 4_000_000),
        name="assemble_keys" if is_key else "assemble_values",
    )(codes, places, n, me, *[x for f in far for x in f[:2]], near, own, new, qp, prev, cache)


def hand_back_kernel(table_ref, *refs):
    outs, sem = refs[-3:-1], refs[-1]
    arrays = refs[:-3]
    units = len(arrays) // 2

    def one(t, carry):
        for u in range(units):
            size = UNITS[u % len(UNITS)]

            @pl.when(table_ref[0, t] == u)
            def _():
                for k in BOTH:
                    for d in BOTH:
                        pltpu.make_async_copy(arrays[2 * u + d].at[table_ref[1, t] + k * size], outs[k].at[d * HALF + t], sem).start()
        return carry

    def wait(t, carry):
        @pl.when(table_ref[0, t] >= 0)
        def _():
            for k in BOTH:
                for d in BOTH:
                    pltpu.make_async_copy(outs[k].at[d * HALF + t], outs[k].at[d * HALF + t], sem).wait()

        return carry

    lax.fori_loop(0, HALF, one, 0)
    lax.fori_loop(0, HALF, wait, 0)


def hand_back(table, pairs):
    arrays = [x for pair in pairs for x in pair]
    return pl.pallas_call(
        hand_back_kernel,
        grid_spec=pltpu.PrefetchScalarGridSpec(
            num_scalar_prefetch=1, grid=(1,), in_specs=[ANYWHERE] * len(arrays),
            out_specs=[pl.BlockSpec((CROSS, GRAN, 256), lambda i, t_ref: (0, 0, 0))] * 2, scratch_shapes=[pltpu.SemaphoreType.DMA]),
        out_shape=[jax.ShapeDtypeStruct((CROSS, GRAN, 256), jnp.bfloat16)] * 2,
        compiler_params=pltpu.CompilerParams(vmem_limit_bytes=VMEM_LIMIT),
        cost_estimate=cost(8_000_000),
        name="hand_back",
    )(table, *arrays)


def solution(mesh):
    head_spec = P('dp', None, 'sh', None)
    row_spec = P(('dp', 'sh'))
    full_spec = P(None, None)

    def send(x, d):
        return lax.ppermute(x, 'sh', [(i, i ^ d) for i in range(WAYS)])

    def across(x):
        return lax.ppermute(x, 'dp', [(0, 1), (1, 0)])

    def step(k_prefill, v_prefill, lengths, residual, norm_gain, w_query, w_key, w_value, w_out):
        seq_g = k_prefill.shape[1] // GRAN
        me = lax.axis_index('sh').astype(jnp.int32)
        peers = me ^ jnp.arange(WAYS, dtype=jnp.int32)
        by_peer = lengths[(peers[:, None] * ROWS + jnp.arange(ROWS, dtype=jnp.int32)).reshape(-1)].reshape(WAYS, ROWS)
        mine = by_peer[0]
        prefill = {True: k_prefill.reshape(-1, GRAN, 256), False: v_prefill.reshape(-1, GRAN, 256)}

        def lists(*ds):
            return Lists(jnp.stack([by_peer[d] for d in ds]), jnp.stack([(me ^ d) * ROWS for d in ds])[:, None], seq_g)

        def span(count):
            return lax.broadcasted_iota(jnp.int32, (1, count), 1)

        def held(which, i):
            src, mixed = which.source(i)
            valid = i < which.size
            return jnp.where(valid, src, 0), jnp.where(valid, mixed, -1)

        far, close, self_list = lists(2, 3), lists(1, 0), lists(0)
        fixed_src, fixed_mix = held(far, span(FIXED))
        close_src, close_mix = held(close, span(ROWS * WIN_G))

        chip, core = me // 2, me % 2

        def rests(lens):
            sizes = jnp.sum(jnp.minimum(lens // GRAN + 1, WIN_G).reshape(WAYS, ROWS), axis=1)
            return jnp.maximum(sizes - FIXED, 0).reshape(WAYS // 2, 2)

        def of_chip(x, c):
            return jnp.where(c == 0, x[0], x[1])

        other_lengths = across(lengths)
        rest, other_rest = rests(lengths), rests(other_lengths)
        need, other_need = jnp.sum(rest, axis=1), jnp.sum(other_rest, axis=1)
        level = jnp.max(jnp.maximum((need + other_need + 4 * QUANTUM - 1) // (4 * QUANTUM), (jnp.maximum(need, other_need) - CROSS + 2 * QUANTUM - 1) // (2 * QUANTUM)))
        spare = QUANTUM * level
        on = active_units(level)
        column = span(SPARE)
        unit = functools.reduce(jnp.add, [(column >= s).astype(jnp.int32) for s in starts_of(UNITS)[1:]])
        skipped, used, place = 0, jnp.zeros_like(column, dtype=bool), column
        for u, size in enumerate(UNITS):
            used = jnp.where(unit == u, on[u], used)
            place = jnp.where(unit == u, column - skipped, place)
            skipped = skipped + jnp.where(on[u], 0, size)
        far_n = lax.dynamic_slice_in_dim(lengths, (1 - chip) * 2 * ROWS, 2 * ROWS).reshape(2, ROWS)
        far_lists = Lists(far_n, ((1 - chip) * 2 + jnp.arange(2, dtype=jnp.int32))[:, None] * ROWS, seq_g)
        far_first, far_need = of_chip(rest, 1 - chip)[0], of_chip(need, 1 - chip)
        far_guests = jnp.maximum(of_chip(other_need, 1 - chip) - 2 * spare, 0)

        def from_rest(c):
            second = c >= far_first
            src, mixed = far_lists.source(FIXED + c - jnp.where(second, far_first, 0))
            return tuple(jnp.where(second[0], x[1], x[0]) for x in (src, mixed))

        both_used = beside([used, used])[0]
        z = beside([place + (core ^ a) * spare for a in BOTH])
        src, mixed = from_rest(z)
        order = z[0] - far_need
        hosted, guest = both_used & (order < 0), both_used & (order >= 0) & (order < far_guests)
        spare_src = jnp.where(hosted, src, jnp.where(guest, ELSEWHERE + order, 0)).reshape(2, SPARE)
        spare_mix = jnp.where(hosted, mixed, -1).reshape(2, SPARE)
        z = 2 * spare + span(CROSS)
        src, mixed = from_rest(z)
        hosted = z[0] < far_need
        cross_src, cross_mix = jnp.where(hosted, src, 0).reshape(2, HALF), jnp.where(hosted, mixed, -1).reshape(2, HALF)

        own_first, own_need = of_chip(rest, chip)[0], of_chip(need, chip)

        def belongs(i, valid):
            r, g = self_list.at(i)
            return jnp.where(valid & (i < self_list.size), r * WIN_G + g, -1), jnp.clip(i, 0, ROWS * WIN_G - 1)

        def rest_belongs(c, valid):
            second = c >= own_first
            return belongs(FIXED + c - jnp.where(second, own_first, 0), valid & (c < own_need) & (second == (core == 1)))

        half_span = span(HALF)
        parts = [belongs(span(FIXED), True), rest_belongs(place + core * spare, used), rest_belongs(place + (1 - core) * spare, used)]
        parts += [rest_belongs(2 * spare + x * (HALF) + half_span, True) for x in (core, 1 - core)]
        codes = beside([p[0] for p in parts])
        places = beside([p[1] for p in parts])

        w = core * (HALF) + half_span
        z = own_need + w
        high = (z >= spare).astype(jnp.int32)
        u = z - high * spare
        back_unit, back_at, begin = jnp.full_like(u, -1), jnp.zeros_like(u), 0
        for k, size in enumerate(UNITS):
            inside = (u >= begin) & (u < begin + jnp.where(on[k], size, 0))
            back_unit = jnp.where(inside, k, back_unit)
            back_at = jnp.where(inside, u - begin, back_at)
            begin = begin + jnp.where(on[k], size, 0)
        back_unit = jnp.where(w < jnp.maximum(of_chip(other_need, chip) - 2 * spare, 0), back_unit + len(UNITS) * (high != core).astype(jnp.int32), -1)
        back_table = jnp.concatenate([back_unit, back_at], axis=0)

        fixed_from, close_from = FromTable(fixed_src, fixed_mix), FromTable(close_src, close_mix)
        spare_from, cross_from = FromTable(spare_src, spare_mix), FromTable(cross_src, cross_mix)
        fixed_got = {True: [], False: []}
        packed_values = []
        for i, (base, count) in enumerate(zip(starts_of(K_PIECES), K_PIECES)):
            out = pack([prefill[True]], FromLengths(lengths, seq_g) if i == 0 else fixed_from, base, count)
            a = send(out[0], 2)
            b = send(out[1], 3)
            fixed_got[True].append((a, b))
        cross = pack([prefill[True], prefill[False]], cross_from, 0, HALF)
        guests = []
        for e in BOTH:
            guests.append(across(cross[e]))
        close_got = {}
        for is_key in KV:
            near, own = pack([prefill[is_key]], close_from, 0, ROWS * WIN_G)
            close_got[is_key] = (send(near, 1), own)
        spare_packed = [pack([prefill[True], prefill[False]], spare_from, base, count, guests) for base, count in zip(starts_of(UNITS), UNITS)]
        for base, count in zip(starts_of(V_PIECES), V_PIECES):
            packed_values.append(pack([prefill[False]], fixed_from, base, count))

        resid_f32 = residual.astype(jnp.float32)
        inv_rms = lax.rsqrt(jnp.mean(resid_f32 * resid_f32, axis=-1, keepdims=True) + EPS)
        normed = (resid_f32 * inv_rms * norm_gain.astype(jnp.float32)).astype(jnp.bfloat16)
        q_group = w_query.shape[1] // (WAYS * 256)
        q_heads = jnp.dot(normed, w_query, preferred_element_type=jnp.float32).astype(jnp.bfloat16).reshape(ROWS, WAYS, q_group, 256)
        k_new = jnp.dot(normed, w_key, preferred_element_type=jnp.float32).astype(jnp.bfloat16).reshape(ROWS, WAYS, 256)
        v_new = jnp.dot(normed, w_value, preferred_element_type=jnp.float32).astype(jnp.bfloat16).reshape(ROWS, WAYS, 256)
        q_heads = rotate(q_heads, mine)
        k_new = rotate(k_new, mine)
        new = {True: k_new.astype(jnp.float32).reshape(-1, 1, 256), False: v_new.astype(jnp.float32).reshape(-1, 1, 256)}
        q_pad = jnp.pad(q_heads.transpose(1, 0, 2, 3).reshape(WAYS, ROWS * q_group, 256), ((0, 0), (0, 8 - ROWS * q_group), (0, 0)))
        k_cache, v_cache = cleared(mine, (ROWS, WINDOW, WAYS, 256))
        scores = blank((WAYS, 8, codes.shape[1] * GRAN), jnp.float32)

        def branch(lvl):
            keep = [bool(x) for x in active_units(lvl)]

            def run(pairs):
                return [(send(a, 2), send(b, 3)) if k else (blank(a.shape, a.dtype), blank(b.shape, b.dtype)) for k, (a, b) in zip(keep, pairs)]

            return run

        spare_packed, packed_values, ready = lax.optimization_barrier((spare_packed, packed_values, (new, q_pad, k_cache, v_cache, scores, close_got[True][1], close_got[False][1])))
        new, q_pad, k_cache, v_cache, scores, own_k, own_v = ready
        own = {True: own_k, False: own_v}
        spare_got = lax.switch(level, [branch(x) for x in range(LEVELS)], spare_packed)
        spare_got, packed_values = lax.optimization_barrier((spare_got, packed_values))
        for a, b in packed_values:
            a = send(a, 2)
            b = send(b, 3)
            fixed_got[False].append((a, b))
        forwarded = [(send(b, 1), send(a, 1)) for a, b in spare_got]
        found = hand_back(back_table, spare_got + forwarded)
        handed, handed_on = [], []
        for k in BOTH:
            handed.append(across(found[k]))
            handed_on.append(send(handed[k], 1))

        me1 = me.reshape(1)

        def run(is_key, base, far_parts, qp, prev, cache):
            return assemble(is_key, base, codes, places, mine, me1, far_parts, close_got[is_key][0], own[is_key], new[is_key], qp, prev, cache)

        def fixed(pieces, got):
            return [(a, b, (0, 0), count) for (a, b), count in zip(got, pieces)]

        def spares(is_key):
            return [(a, b, (0, 0) if is_key else (count, count), count) for got in (spare_got, forwarded) for (a, b), count in zip(got, UNITS)]

        def returned(is_key):
            own_half, other_half = handed[0 if is_key else 1], handed_on[0 if is_key else 1]
            return [(own_half, own_half, (0, HALF), HALF), (other_half, other_half, (HALF, 0), HALF)]


        k_cache, scores = run(True, 0, fixed(K_PIECES, fixed_got[True]), q_pad, scores, k_cache)
        k_cache, scores = run(True, FIXED, spares(True), q_pad, scores, k_cache)
        k_cache, scores = run(True, FIXED + 2 * SPARE, returned(True), q_pad, scores, k_cache)
        exp_scores = jnp.exp(scores - jnp.max(scores, axis=-1, keepdims=True))
        weights = (exp_scores / jnp.sum(exp_scores, axis=-1, keepdims=True)).astype(jnp.bfloat16)
        sums = jnp.zeros((WAYS, 8, 256), jnp.float32)
        v_cache, sums = run(False, FIXED, spares(False), weights, sums, v_cache)
        v_cache, sums = run(False, FIXED + 2 * SPARE, returned(False), weights, sums, v_cache)
        for base, part in zip(starts_of(V_PIECES), fixed(V_PIECES, fixed_got[False])):
            v_cache, sums = run(False, base, [part], weights, sums, v_cache)
        attn_out = sums[:, :ROWS * q_group].astype(jnp.bfloat16).reshape(WAYS, ROWS, q_group * 256).transpose(1, 0, 2).reshape(ROWS, WAYS * q_group * 256)
        resid_out = (resid_f32 + jnp.dot(attn_out, w_out, preferred_element_type=jnp.float32)).astype(jnp.bfloat16)
        return resid_out, k_cache, v_cache

    return jax.shard_map(
        step, mesh=mesh, in_specs=(head_spec, head_spec, P('dp'), P(('dp', 'sh'), None), P(None), full_spec, full_spec, full_spec, full_spec),
        out_specs=(P(('dp', 'sh'), None), row_spec, row_spec), check_vma=False)
```

```python
import functools

import jax
import jax.numpy as jnp
from jax import lax
from jax.experimental import pallas as pl
from jax.experimental.pallas import tpu as pltpu
from jax.sharding import PartitionSpec as P


WINDOW = 4096
THETA = 10000.0
EPS = 1e-5
GRAN = 64
WIN_G = WINDOW // GRAN
STEP = 8
FIXED = 112
UNITS = (64, 32, 16, 8, 4)
QUANTUM = UNITS[-1]
SPARE = sum(UNITS) + QUANTUM
K_PIECES = (8, 24, 80)
V_PIECES = (80, 24, 8)
CROSS = 48
ELSEWHERE = 1 << 20
WAYS, ROWS = 4, 3
LEVELS = (ROWS * WIN_G - FIXED) // QUANTUM + 1
VMEM_LIMIT = 67_043_328
HALF = CROSS // 2
KV = (True, False)
BOTH = range(2)
SERIAL = pltpu.CompilerParams(dimension_semantics=("arbitrary",), vmem_limit_bytes=VMEM_LIMIT)
ANYWHERE = pl.BlockSpec(memory_space=pl.ANY)


beside = functools.partial(jnp.concatenate, axis=1)


def cost(moved):
    return pl.CostEstimate(flops=10_000_000, bytes_accessed=moved, transcendentals=0)


def starts_of(sizes):
    return [sum(sizes[:i]) for i in range(len(sizes))]


def active_units(level):
    return [(level & (size // QUANTUM)) != 0 for size in UNITS]


def rotate(heads, positions):
    head_dim = heads.shape[-1]
    half_dim = head_dim // 2
    inv_freq = THETA ** (-2.0 * jnp.arange(half_dim, dtype=jnp.float32) / head_dim)
    angles = positions.astype(jnp.float32).reshape(positions.shape + (1,) * (heads.ndim - 1)) * inv_freq
    cos_part = jnp.cos(angles)
    sin_part = jnp.sin(angles)
    first_half = heads[..., :half_dim].astype(jnp.float32)
    second_half = heads[..., half_dim:].astype(jnp.float32)
    return jnp.concatenate([first_half * cos_part - second_half * sin_part, second_half * cos_part + first_half * sin_part], axis=-1).astype(jnp.bfloat16)


def blank(shape, dtype):
    return pl.pallas_call(
        lambda o_ref: None,
        out_shape=jax.ShapeDtypeStruct(shape, dtype),
        out_specs=ANYWHERE,
        name="blank",
    )()


def cleared_kernel(n_ref, k_ref, v_ref, zeros, sem):
    zeros[...] = jnp.zeros_like(zeros)

    def each(act):
        for r in range(ROWS):
            def one(g, carry):
                for ref in (k_ref, v_ref):
                    act(pltpu.make_async_copy(zeros, ref.at[r, pl.ds(g * GRAN, GRAN)], sem))
                return carry

            lax.fori_loop(jnp.minimum(n_ref[r] // GRAN + 1, WIN_G), WIN_G, one, 0)

    each(lambda copy: copy.start())
    each(lambda copy: copy.wait())


def cleared(n, shape):
    return pl.pallas_call(
        cleared_kernel,
        grid_spec=pltpu.PrefetchScalarGridSpec(
            num_scalar_prefetch=1, grid=(1,), in_specs=[], out_specs=[ANYWHERE, ANYWHERE],
            scratch_shapes=[pltpu.VMEM((GRAN, WAYS, 256), jnp.bfloat16), pltpu.SemaphoreType.DMA]),
        out_shape=[jax.ShapeDtypeStruct(shape, jnp.bfloat16)] * 2,
        compiler_params=pltpu.CompilerParams(vmem_limit_bytes=VMEM_LIMIT),
        cost_estimate=cost(20_000_000),
        name="cleared",
    )(n)


class Lists:
    def __init__(self, n, row0, seq_g):
        self.n, self.row0, self.seq_g = n, row0, seq_g
        self.lap = n // WINDOW
        self.cut = n % WINDOW
        width = jnp.minimum(n // GRAN + 1, WIN_G)
        self.off1 = width[..., 0:1]
        self.off2 = self.off1 + width[..., 1:2]
        self.size = self.off2 + width[..., 2:3]

    def of_row(self, x, r):
        return jnp.where(r == 0, x[..., 0:1], jnp.where(r == 1, x[..., 1:2], x[..., 2:3]))

    def at(self, i):
        r = (i >= self.off1).astype(jnp.int32) + (i >= self.off2).astype(jnp.int32)
        return r, i - jnp.where(r == 0, 0, jnp.where(r == 1, self.off1, self.off2))

    def source(self, i):
        r, g = self.at(i)
        lap, cut = self.of_row(self.lap, r), self.of_row(self.cut, r)
        older = jnp.maximum(lap - 1, 0)
        base = (self.row0 + r) * self.seq_g
        src = base + jnp.minimum(jnp.where(g <= cut // GRAN, lap, older) * WIN_G + g, self.seq_g - 1)
        mixed = jnp.where(lap >= 1, base + older * WIN_G + g, -1)
        return src, jnp.where(g == cut // GRAN, (mixed + 1) * GRAN + cut % GRAN, -1)


def pack_kernel(base, size, steps, source, extra, *refs):
    num = source.num_scalars
    scalars, refs = refs[:num], refs[num:]
    prefills, extras, outs, (buf, older, sems) = refs[:-5 - extra], refs[-5 - extra:-5], refs[-5:-3], refs[-3:]
    at = source.reader(*scalars)
    i = pl.program_id(0)
    total = steps * len(prefills)
    slots = buf.shape[0]
    slot = lax.rem(i, slots)

    def by_tensor(step, do):
        for k, ref in enumerate(prefills):
            pl.when((step >= k * steps) & (step < (k + 1) * steps))(functools.partial(do, k, ref))

    def fetch(step):
        first = base + lax.rem(step, steps) * size
        to = lax.rem(step, slots)

        def from_ref(k, ref):
            for a in BOTH:
                def one(t, found):
                    src, code = at(a, first + t)
                    if not extras:
                        pltpu.make_async_copy(ref.at[src], buf.at[to, a, t], sems.at[0, to]).start()
                    else:
                        @pl.when(src < ELSEWHERE)
                        def _():
                            pltpu.make_async_copy(ref.at[src], buf.at[to, a, t], sems.at[0, to]).start()

                        for e, other in enumerate(extras):

                            @pl.when((src >= ELSEWHERE + e * HALF) & (src < ELSEWHERE + (e + 1) * HALF))
                            def _():
                                pltpu.make_async_copy(other.at[src - ELSEWHERE + (k - e) * HALF], buf.at[to, a, t], sems.at[0, to]).start()
                    mixed = code >= GRAN

                    @pl.when(mixed)
                    def _():
                        pltpu.make_async_copy(ref.at[code // GRAN - 1], older.at[to, a, found], sems.at[2, to]).start()

                    return found + mixed.astype(jnp.int32)

                lax.fori_loop(0, size, one, jnp.int32(0))

        by_tensor(step, from_ref)

    def stores(step):
        to = lax.rem(step, slots)
        return [pltpu.make_async_copy(buf.at[to, a], outs[a].at[pl.ds(step * size, size)], sems.at[1, to]) for a in BOTH]

    @pl.when(i == 0)
    def _():
        fetch(i)

    if total > 1:
        @pl.when(i + 1 < total)
        def _():
            if total > slots:
                @pl.when(i + 1 >= slots)
                def _():
                    for copy in stores(i + 1 - slots):
                        copy.wait()
            fetch(i + 1)

    pltpu.make_async_copy(buf.at[slot], buf.at[slot], sems.at[0, slot]).wait()
    first = base + lax.rem(i, steps) * size
    for a in BOTH:
        def patch(t, found):
            code = at(a, first + t)[1]
            mixed = code >= GRAN

            @pl.when(code >= 0)
            def _():
                @pl.when(mixed)
                def _():
                    pltpu.make_async_copy(older.at[slot, a, found], older.at[slot, a, found], sems.at[2, slot]).wait()

                newer = lax.broadcasted_iota(jnp.int32, (GRAN, 256), 0) < lax.rem(code, GRAN)
                rest = jnp.where(mixed, older[slot, a, found].astype(jnp.float32), 0.0)
                buf[slot, a, t] = jnp.where(newer, buf[slot, a, t].astype(jnp.float32), rest).astype(jnp.bfloat16)

            return found + mixed.astype(jnp.int32)

        lax.fori_loop(0, size, patch, jnp.int32(0))
    for copy in stores(i):
        copy.start()

    @pl.when(i == total - 1)
    def _():
        for back in range(min(slots, total)):
            for copy in stores(i - back):
                copy.wait()


class FromTable:
    num_scalars = 2

    def __init__(self, src, mix):
        self.scalars = (src, mix)

    def reader(self, src_ref, mix_ref):
        return lambda a, i: (src_ref[a, i], mix_ref[a, i])


class FromLengths:
    num_scalars = 1

    def __init__(self, lengths, seq_g):
        self.scalars = (lengths,)
        self.seq_g = seq_g

    def reader(self, n_ref):
        me = lax.axis_index('sh').astype(jnp.int32)

        def at(a, i):
            row0 = (me ^ (2 + a)) * ROWS
            n = [n_ref[row0 + r] for r in range(ROWS)]
            ends, end = [], 0
            for x in n:
                end = end + jnp.minimum(x // GRAN + 1, WIN_G)
                ends.append(end)
            r = jnp.where(i >= ends[0], 1, 0) + jnp.where(i >= ends[1], 1, 0)
            g = i - jnp.where(r == 0, 0, jnp.where(r == 1, ends[0], ends[1]))
            length = jnp.where(r == 0, n[0], jnp.where(r == 1, n[1], n[2]))
            lap, cut = length // WINDOW, lax.rem(length, WINDOW)
            older = jnp.maximum(lap - 1, 0)
            first = (row0 + r) * self.seq_g
            src = first + jnp.minimum(jnp.where(g <= cut // GRAN, lap, older) * WIN_G + g, self.seq_g - 1)
            mixed = jnp.where(lap >= 1, first + older * WIN_G + g, -1)
            valid = i < ends[2]
            return jnp.where(valid, src, 0), jnp.where(valid & (g == cut // GRAN), (mixed + 1) * GRAN + lax.rem(cut, GRAN), -1)

        return at


def pack(prefills, source, base, count, extras=()):
    size = next(x for x in (16, 8, 4) if count % x == 0)
    steps = count // size
    total = count * len(prefills)
    return pl.pallas_call(
        functools.partial(pack_kernel, base, size, steps, source, len(extras)),
        grid_spec=pltpu.PrefetchScalarGridSpec(
            num_scalar_prefetch=source.num_scalars,
            grid=(steps * len(prefills),),
            in_specs=[ANYWHERE] * (len(prefills) + len(extras)),
            out_specs=[ANYWHERE] * 2,
            scratch_shapes=[pltpu.VMEM((3, 2, size, GRAN, 256), jnp.bfloat16), pltpu.VMEM((3, 2, 2 * ROWS + 1, GRAN, 256), jnp.bfloat16), pltpu.SemaphoreType.DMA((3, 3))],
        ),
        out_shape=[jax.ShapeDtypeStruct((total, GRAN, 256), jnp.bfloat16)] * 2,
        compiler_params=SERIAL,
        cost_estimate=cost(total * 130_000),
        name="pack",
    )(*source.scalars, *prefills, *extras)


def assemble_kernel(is_key, base, size, steps, segments, code_ref, idx_ref, n_ref, me_ref, *refs):
    num_far = 2 * (1 + max(s[2] for s in segments))
    far_refs = refs[:num_far]
    near_ref, own_ref, new_ref, qp_ref, prev_ref, _, cache_ref, res_ref, xb, mix, ob, acc, sems = refs[num_far:]
    i = pl.program_id(0)
    me = me_ref[0]
    slot = lax.rem(i, 2)

    def code_at(step, t):
        return code_ref[0, base + step * size + t]

    def active_at(step):
        return functools.reduce(jnp.maximum, [code_at(step, t) for t in range(size)]) >= 0

    def read(step, buf):
        @pl.when(active_at(step))
        def _():
            for begin, end, entry, offsets, count, place in segments:
                @pl.when((step >= begin) & (step < end))
                def _():
                    for d in BOTH:
                        pltpu.make_async_copy(far_refs[2 * entry + d].at[pl.ds(offsets[d] + (step - begin) * size, count)], xb.at[buf, me ^ (2 + d), pl.ds(place, count)], sems.at[0, buf]).start()

            def one(t, carry):
                at = idx_ref[0, base + step * size + t]
                pltpu.make_async_copy(near_ref.at[at], xb.at[buf, me ^ 1, t], sems.at[0, buf]).start()
                pltpu.make_async_copy(own_ref.at[at], xb.at[buf, me, t], sems.at[0, buf]).start()
                return carry

            lax.fori_loop(0, size, one, 0)

    def write(step, t, buf):
        code = code_at(step, t)
        return pltpu.make_async_copy(ob.at[buf, t], cache_ref.at[code // WIN_G, pl.ds(lax.rem(code, WIN_G) * GRAN, GRAN)], sems.at[1, buf])

    def written(step, buf):
        def one(t, carry):
            @pl.when(code_at(step, t) >= 0)
            def _():
                write(step, t, buf).wait()

            return carry

        lax.fori_loop(0, size, one, 0)

    @pl.when(i == 0)
    def _():
        read(i, slot)
        if not is_key:
            acc[...] = prev_ref[...]

    if steps > 1:
        @pl.when(i + 1 < steps)
        def _():
            read(i + 1, 1 - slot)

    if steps > 2:
        @pl.when(i >= 2)
        def _():
            written(i - 2, slot)

    active = active_at(i)

    @pl.when(active)
    def _():
        pltpu.make_async_copy(xb.at[slot], xb.at[slot], sems.at[0, slot]).wait()

        def one(t, carry):
            code = code_at(i, t)

            @pl.when(code < 0)
            def _():
                for h in range(WAYS):
                    xb[slot, h, t] = jnp.zeros((GRAN, 256), jnp.bfloat16)

            for r in range(ROWS):
                cut = lax.rem(n_ref[r], WINDOW)

                @pl.when(code == r * WIN_G + cut // GRAN)
                def _():
                    here = lax.broadcasted_iota(jnp.int32, (GRAN, 256), 0) == lax.rem(cut, GRAN)
                    for h in range(WAYS):
                        new = jnp.broadcast_to(new_ref[r * WAYS + h], (GRAN, 256))
                        xb[slot, h, t] = jnp.where(here, new, xb[slot, h, t].astype(jnp.float32)).astype(jnp.bfloat16)

            @pl.when(code >= 0)
            def _():
                for h in range(WAYS):
                    x = xb[slot, h, t].astype(jnp.float32)
                    for half in BOTH:
                        mix[half, pl.ds(h, GRAN, stride=WAYS), :] = x[:, half * 128:(half + 1) * 128]
                joined = beside([mix[half].astype(jnp.bfloat16) for half in BOTH])
                ob[slot, t] = joined.reshape(GRAN, WAYS, 256)
                write(i, t, slot).start()

            return carry

        lax.fori_loop(0, size, one, 0)

        lanes = size * GRAN
        if is_key:
            lane = lax.broadcasted_iota(jnp.int32, (8, lanes), 1)
            row = lax.broadcasted_iota(jnp.int32, (8, lanes), 0) // 2
            code = jnp.full((8, lanes), -1, jnp.int32)
            for t in range(size):
                code = jnp.where(lane // GRAN == t, code_at(i, t), code)
            length = jnp.where(row == 0, n_ref[0], jnp.where(row == 1, n_ref[1], n_ref[2]))
            place = (code % WIN_G) * GRAN + lane % GRAN
            live = (code >= 0) & (code // WIN_G == row) & ((length >= WINDOW) | (place <= length))
            for h in range(WAYS):
                s = lax.dot_general(qp_ref[h], xb[slot, h].reshape(lanes, 256), (((1,), (1,)), ((), ())), preferred_element_type=jnp.float32)
                res_ref[h] = jnp.where(live, s / 16.0, -jnp.inf)
        else:
            for h in range(WAYS):
                acc[h] += jnp.dot(qp_ref[h], xb[slot, h].reshape(lanes, 256), preferred_element_type=jnp.float32)

    if is_key:
        @pl.when(jnp.logical_not(active))
        def _():
            res_ref[...] = jnp.full_like(res_ref, -jnp.inf)

    @pl.when(i == steps - 1)
    def _():
        if not is_key:
            res_ref[...] = acc[...]
        if steps >= 2:
            written(i - 1, 1 - slot)
        written(i, slot)


def assemble(is_key, base, codes, places, n, me, far, near, own, new, qp, prev, cache):
    total = sum(f[3] for f in far)
    size = min(STEP, total)
    steps = total // size
    segments, at = [], 0
    for entry, (_, _, offsets, count) in enumerate(far):
        if count >= size:
            segments.append((at // size, (at + count) // size, entry, offsets, size, 0))
        else:
            segments.append((at // size, at // size + 1, entry, offsets, count, at % size))
        at += count
    whole = lambda *shape: pl.BlockSpec(shape, lambda i, *_: (0,) * len(shape))
    by_step = pl.BlockSpec((WAYS, 8, size * GRAN), lambda i, *_: (0, 0, base // size + i))
    if is_key:
        qp_spec, prev_spec, res_spec = whole(WAYS, 8, 256), ANYWHERE, by_step
    else:
        qp_spec, prev_spec, res_spec = by_step, whole(WAYS, 8, 256), whole(WAYS, 8, 256)
    after = 4 + 2 * len(far) + 2
    aliases = {after + 3: 0}
    if is_key:
        aliases[after + 2] = 1
    return pl.pallas_call(
        functools.partial(assemble_kernel, is_key, base, size, steps, segments),
        grid_spec=pltpu.PrefetchScalarGridSpec(
            num_scalar_prefetch=4,
            grid=(steps,),
            in_specs=[ANYWHERE] * (2 * len(far) + 2) + [whole(ROWS * WAYS, 1, 256), qp_spec, prev_spec, ANYWHERE],
            out_specs=[ANYWHERE, res_spec],
            scratch_shapes=[
                pltpu.VMEM((2, WAYS, size, GRAN, 256), jnp.bfloat16),
                pltpu.VMEM((2, WAYS * GRAN, 128), jnp.float32),
                pltpu.VMEM((2, size, GRAN, WAYS, 256), jnp.bfloat16),
                pltpu.VMEM((WAYS, 8, 256), jnp.float32),
                pltpu.SemaphoreType.DMA((2, 2)),
            ],
        ),
        out_shape=[jax.ShapeDtypeStruct(cache.shape, cache.dtype), jax.ShapeDtypeStruct(prev.shape, prev.dtype)],
        input_output_aliases=aliases,
        compiler_params=SERIAL,
        cost_estimate=cost(steps * 4_000_000),
        name="assemble_keys" if is_key else "assemble_values",
    )(codes, places, n, me, *[x for f in far for x in f[:2]], near, own, new, qp, prev, cache)


def hand_back_kernel(table_ref, *refs):
    outs, sem = refs[-3:-1], refs[-1]
    arrays = refs[:-3]
    units = len(arrays) // 2

    def one(t, carry):
        for u in range(units):
            size = UNITS[u % len(UNITS)]

            @pl.when(table_ref[0, t] == u)
            def _():
                for k in BOTH:
                    for d in BOTH:
                        pltpu.make_async_copy(arrays[2 * u + d].at[table_ref[1, t] + k * size], outs[k].at[d * HALF + t], sem).start()
        return carry

    def wait(t, carry):
        @pl.when(table_ref[0, t] >= 0)
        def _():
            for k in BOTH:
                for d in BOTH:
                    pltpu.make_async_copy(outs[k].at[d * HALF + t], outs[k].at[d * HALF + t], sem).wait()

        return carry

    lax.fori_loop(0, HALF, one, 0)
    lax.fori_loop(0, HALF, wait, 0)


def hand_back(table, pairs):
    arrays = [x for pair in pairs for x in pair]
    return pl.pallas_call(
        hand_back_kernel,
        grid_spec=pltpu.PrefetchScalarGridSpec(
            num_scalar_prefetch=1, grid=(1,), in_specs=[ANYWHERE] * len(arrays),
            out_specs=[pl.BlockSpec((CROSS, GRAN, 256), lambda i, t_ref: (0, 0, 0))] * 2, scratch_shapes=[pltpu.SemaphoreType.DMA]),
        out_shape=[jax.ShapeDtypeStruct((CROSS, GRAN, 256), jnp.bfloat16)] * 2,
        compiler_params=pltpu.CompilerParams(vmem_limit_bytes=VMEM_LIMIT),
        cost_estimate=cost(8_000_000),
        name="hand_back",
    )(table, *arrays)


def solution(mesh):
    head_spec = P('dp', None, 'sh', None)
    row_spec = P(('dp', 'sh'))
    full_spec = P(None, None)

    def send(x, d):
        return lax.ppermute(x, 'sh', [(i, i ^ d) for i in range(WAYS)])

    def across(x):
        return lax.ppermute(x, 'dp', [(0, 1), (1, 0)])

    def step(k_prefill, v_prefill, lengths, residual, norm_gain, w_query, w_key, w_value, w_out):
        seq_g = k_prefill.shape[1] // GRAN
        me = lax.axis_index('sh').astype(jnp.int32)
        peers = me ^ jnp.arange(WAYS, dtype=jnp.int32)
        by_peer = lengths[(peers[:, None] * ROWS + jnp.arange(ROWS, dtype=jnp.int32)).reshape(-1)].reshape(WAYS, ROWS)
        mine = by_peer[0]
        prefill = {True: k_prefill.reshape(-1, GRAN, 256), False: v_prefill.reshape(-1, GRAN, 256)}

        def lists(*ds):
            return Lists(jnp.stack([by_peer[d] for d in ds]), jnp.stack([(me ^ d) * ROWS for d in ds])[:, None], seq_g)

        def span(count):
            return lax.broadcasted_iota(jnp.int32, (1, count), 1)

        def held(which, i):
            src, mixed = which.source(i)
            valid = i < which.size
            return jnp.where(valid, src, 0), jnp.where(valid, mixed, -1)

        far, close, self_list = lists(2, 3), lists(1, 0), lists(0)
        fixed_src, fixed_mix = held(far, span(FIXED))
        close_src, close_mix = held(close, span(ROWS * WIN_G))

        chip, core = me // 2, me % 2

        def rests(lens):
            sizes = jnp.sum(jnp.minimum(lens // GRAN + 1, WIN_G).reshape(WAYS, ROWS), axis=1)
            return jnp.maximum(sizes - FIXED, 0).reshape(WAYS // 2, 2)

        def of_chip(x, c):
            return jnp.where(c == 0, x[0], x[1])

        other_lengths = across(lengths)
        rest, other_rest = rests(lengths), rests(other_lengths)
        need, other_need = jnp.sum(rest, axis=1), jnp.sum(other_rest, axis=1)
        level = jnp.max(jnp.maximum((need + other_need + 4 * QUANTUM - 1) // (4 * QUANTUM), (jnp.maximum(need, other_need) - CROSS + 2 * QUANTUM - 1) // (2 * QUANTUM)))
        spare = QUANTUM * level
        on = active_units(level)
        column = span(SPARE)
        unit = functools.reduce(jnp.add, [(column >= s).astype(jnp.int32) for s in starts_of(UNITS)[1:]])
        skipped, used, place = 0, jnp.zeros_like(column, dtype=bool), column
        for u, size in enumerate(UNITS):
            used = jnp.where(unit == u, on[u], used)
            place = jnp.where(unit == u, column - skipped, place)
            skipped = skipped + jnp.where(on[u], 0, size)
        used = used & (column < sum(UNITS))
        far_n = lax.dynamic_slice_in_dim(lengths, (1 - chip) * 2 * ROWS, 2 * ROWS).reshape(2, ROWS)
        far_lists = Lists(far_n, ((1 - chip) * 2 + jnp.arange(2, dtype=jnp.int32))[:, None] * ROWS, seq_g)
        far_first, far_need = of_chip(rest, 1 - chip)[0], of_chip(need, 1 - chip)
        far_guests = jnp.maximum(of_chip(other_need, 1 - chip) - 2 * spare, 0)

        def from_rest(c):
            second = c >= far_first
            src, mixed = far_lists.source(FIXED + c - jnp.where(second, far_first, 0))
            return tuple(jnp.where(second[0], x[1], x[0]) for x in (src, mixed))

        both_used = beside([used, used])[0]
        z = beside([place + (core ^ a) * spare for a in BOTH])
        src, mixed = from_rest(z)
        order = z[0] - far_need
        hosted, guest = both_used & (order < 0), both_used & (order >= 0) & (order < far_guests)
        spare_src = jnp.where(hosted, src, jnp.where(guest, ELSEWHERE + order, 0)).reshape(2, SPARE)
        spare_mix = jnp.where(hosted, mixed, -1).reshape(2, SPARE)
        z = 2 * spare + span(CROSS)
        src, mixed = from_rest(z)
        hosted = z[0] < far_need
        cross_src, cross_mix = jnp.where(hosted, src, 0).reshape(2, HALF), jnp.where(hosted, mixed, -1).reshape(2, HALF)

        own_first, own_need = of_chip(rest, chip)[0], of_chip(need, chip)

        def belongs(i, valid):
            r, g = self_list.at(i)
            return jnp.where(valid & (i < self_list.size), r * WIN_G + g, -1), jnp.clip(i, 0, ROWS * WIN_G - 1)

        def rest_belongs(c, valid):
            second = c >= own_first
            return belongs(FIXED + c - jnp.where(second, own_first, 0), valid & (c < own_need) & (second == (core == 1)))

        half_span = span(HALF)
        parts = [belongs(span(FIXED), True), rest_belongs(place + core * spare, used), rest_belongs(place + (1 - core) * spare, used)]
        parts += [rest_belongs(2 * spare + x * (HALF) + half_span, True) for x in (core, 1 - core)]
        codes = beside([p[0] for p in parts])
        places = beside([p[1] for p in parts])

        w = core * (HALF) + half_span
        z = own_need + w
        high = (z >= spare).astype(jnp.int32)
        u = z - high * spare
        back_unit, back_at, begin = jnp.full_like(u, -1), jnp.zeros_like(u), 0
        for k, size in enumerate(UNITS):
            inside = (u >= begin) & (u < begin + jnp.where(on[k], size, 0))
            back_unit = jnp.where(inside, k, back_unit)
            back_at = jnp.where(inside, u - begin, back_at)
            begin = begin + jnp.where(on[k], size, 0)
        back_unit = jnp.where(w < jnp.maximum(of_chip(other_need, chip) - 2 * spare, 0), back_unit + len(UNITS) * (high != core).astype(jnp.int32), -1)
        back_table = jnp.concatenate([back_unit, back_at], axis=0)

        fixed_from, close_from = FromTable(fixed_src, fixed_mix), FromTable(close_src, close_mix)
        spare_from, cross_from = FromTable(spare_src, spare_mix), FromTable(cross_src, cross_mix)
        fixed_got = {True: [], False: []}
        packed_values = []
        for i, (base, count) in enumerate(zip(starts_of(K_PIECES), K_PIECES)):
            out = pack([prefill[True]], FromLengths(lengths, seq_g) if i == 0 else fixed_from, base, count)
            a = send(out[0], 2)
            b = send(out[1], 3)
            fixed_got[True].append((a, b))
        cross = pack([prefill[True], prefill[False]], cross_from, 0, HALF)
        guests = []
        for e in BOTH:
            guests.append(across(cross[e]))
        close_got = {}
        for is_key in KV:
            near, own = pack([prefill[is_key]], close_from, 0, ROWS * WIN_G)
            close_got[is_key] = (send(near, 1), own)
        spare_packed = [pack([prefill[True], prefill[False]], spare_from, base, count, guests) for base, count in zip(starts_of(UNITS), UNITS)]
        for base, count in zip(starts_of(V_PIECES), V_PIECES):
            packed_values.append(pack([prefill[False]], fixed_from, base, count))

        resid_f32 = residual.astype(jnp.float32)
        inv_rms = lax.rsqrt(jnp.mean(resid_f32 * resid_f32, axis=-1, keepdims=True) + EPS)
        normed = (resid_f32 * inv_rms * norm_gain.astype(jnp.float32)).astype(jnp.bfloat16)
        q_group = w_query.shape[1] // (WAYS * 256)
        q_heads = jnp.dot(normed, w_query, preferred_element_type=jnp.float32).astype(jnp.bfloat16).reshape(ROWS, WAYS, q_group, 256)
        k_new = jnp.dot(normed, w_key, preferred_element_type=jnp.float32).astype(jnp.bfloat16).reshape(ROWS, WAYS, 256)
        v_new = jnp.dot(normed, w_value, preferred_element_type=jnp.float32).astype(jnp.bfloat16).reshape(ROWS, WAYS, 256)
        q_heads = rotate(q_heads, mine)
        k_new = rotate(k_new, mine)
        new = {True: k_new.astype(jnp.float32).reshape(-1, 1, 256), False: v_new.astype(jnp.float32).reshape(-1, 1, 256)}
        q_pad = jnp.pad(q_heads.transpose(1, 0, 2, 3).reshape(WAYS, ROWS * q_group, 256), ((0, 0), (0, 8 - ROWS * q_group), (0, 0)))
        k_cache, v_cache = cleared(mine, (ROWS, WINDOW, WAYS, 256))
        scores = blank((WAYS, 8, codes.shape[1] * GRAN), jnp.float32)

        def branch(lvl):
            keep = [bool(x) for x in active_units(lvl)]

            def run(pairs):
                return [(send(a, 2), send(b, 3)) if k else (blank(a.shape, a.dtype), blank(b.shape, b.dtype)) for k, (a, b) in zip(keep, pairs)]

            return run

        spare_packed, packed_values, ready = lax.optimization_barrier((spare_packed, packed_values, (new, q_pad, scores, close_got[True][1], close_got[False][1])))
        new, q_pad, scores, own_k, own_v = ready
        own = {True: own_k, False: own_v}
        spare_got = lax.switch(level, [branch(x) for x in range(LEVELS)], spare_packed)
        spare_got, packed_values = lax.optimization_barrier((spare_got, packed_values))
        for a, b in packed_values:
            a = send(a, 2)
            b = send(b, 3)
            fixed_got[False].append((a, b))
        forwarded = [(send(b, 1), send(a, 1)) for a, b in spare_got]
        found = hand_back(back_table, spare_got + forwarded)
        handed, handed_on = [], []
        for k in BOTH:
            handed.append(across(found[k]))
            handed_on.append(send(handed[k], 1))

        me1 = me.reshape(1)

        def run(is_key, base, far_parts, qp, prev, cache):
            return assemble(is_key, base, codes, places, mine, me1, far_parts, close_got[is_key][0], own[is_key], new[is_key], qp, prev, cache)

        def fixed(pieces, got):
            return [(a, b, (0, 0), count) for (a, b), count in zip(got, pieces)]

        def spares(is_key):
            runs = []
            for got in (spare_got, forwarded):
                runs += [(a, b, (0, 0) if is_key else (count, count), count) for (a, b), count in zip(got, UNITS)]
                runs.append(runs[-1])
            return runs

        def returned(is_key):
            own_half, other_half = handed[0 if is_key else 1], handed_on[0 if is_key else 1]
            return [(own_half, own_half, (0, HALF), HALF), (other_half, other_half, (HALF, 0), HALF)]


        k_cache, scores = run(True, 0, fixed(K_PIECES, fixed_got[True]), q_pad, scores, k_cache)
        k_cache, scores = run(True, FIXED, spares(True), q_pad, scores, k_cache)
        k_cache, scores = run(True, FIXED + 2 * SPARE, returned(True), q_pad, scores, k_cache)
        exp_scores = jnp.exp(scores - jnp.max(scores, axis=-1, keepdims=True))
        weights = (exp_scores / jnp.sum(exp_scores, axis=-1, keepdims=True)).astype(jnp.bfloat16)
        sums = jnp.zeros((WAYS, 8, 256), jnp.float32)
        v_cache, sums = run(False, FIXED, spares(False), weights, sums, v_cache)
        v_cache, sums = run(False, FIXED + 2 * SPARE, returned(False), weights, sums, v_cache)
        for base, part in zip(starts_of(V_PIECES), fixed(V_PIECES, fixed_got[False])):
            v_cache, sums = run(False, base, [part], weights, sums, v_cache)
        attn_out = sums[:, :ROWS * q_group].astype(jnp.bfloat16).reshape(WAYS, ROWS, q_group * 256).transpose(1, 0, 2).reshape(ROWS, WAYS * q_group * 256)
        resid_out = (resid_f32 + jnp.dot(attn_out, w_out, preferred_element_type=jnp.float32)).astype(jnp.bfloat16)
        return resid_out, k_cache, v_cache

    return jax.shard_map(
        step, mesh=mesh, in_specs=(head_spec, head_spec, P('dp'), P(('dp', 'sh'), None), P(None), full_spec, full_spec, full_spec, full_spec),
        out_specs=(P(('dp', 'sh'), None), row_spec, row_spec), check_vma=False)
```

```python
import functools

import jax
import jax.numpy as jnp
from jax import lax
from jax.experimental import pallas as pl
from jax.experimental.pallas import tpu as pltpu
from jax.sharding import PartitionSpec as P


WINDOW = 4096
THETA = 10000.0
EPS = 1e-5
GRAN = 64
WIN_G = WINDOW // GRAN
STEP = 8
FIXED = 112
UNITS = (64, 32, 16, 8, 4)
QUANTUM = UNITS[-1]
SPARE = sum(UNITS) + QUANTUM
K_PIECES = (8, 24, 80)
V_PIECES = (80, 24, 8)
CROSS = 48
ELSEWHERE = 1 << 20
WAYS, ROWS = 4, 3
LEVELS = (ROWS * WIN_G - FIXED) // QUANTUM + 1
VMEM_LIMIT = 67_043_328
HALF = CROSS // 2
KV = (True, False)
BOTH = range(2)
SERIAL = pltpu.CompilerParams(dimension_semantics=("arbitrary",), vmem_limit_bytes=VMEM_LIMIT)
ANYWHERE = pl.BlockSpec(memory_space=pl.ANY)


beside = functools.partial(jnp.concatenate, axis=1)


def cost(moved):
    return pl.CostEstimate(flops=10_000_000, bytes_accessed=moved, transcendentals=0)


def starts_of(sizes):
    return [sum(sizes[:i]) for i in range(len(sizes))]


def active_units(level):
    return [(level & (size // QUANTUM)) != 0 for size in UNITS]


def rotate(heads, positions):
    head_dim = heads.shape[-1]
    half_dim = head_dim // 2
    inv_freq = THETA ** (-2.0 * jnp.arange(half_dim, dtype=jnp.float32) / head_dim)
    angles = positions.astype(jnp.float32).reshape(positions.shape + (1,) * (heads.ndim - 1)) * inv_freq
    cos_part = jnp.cos(angles)
    sin_part = jnp.sin(angles)
    first_half = heads[..., :half_dim].astype(jnp.float32)
    second_half = heads[..., half_dim:].astype(jnp.float32)
    return jnp.concatenate([first_half * cos_part - second_half * sin_part, second_half * cos_part + first_half * sin_part], axis=-1).astype(jnp.bfloat16)


def blank(shape, dtype):
    return pl.pallas_call(
        lambda o_ref: None,
        out_shape=jax.ShapeDtypeStruct(shape, dtype),
        out_specs=ANYWHERE,
        name="blank",
    )()


def cleared_kernel(n_ref, k_ref, v_ref, zeros, sem):
    zeros[...] = jnp.zeros_like(zeros)

    def each(act):
        for r in range(ROWS):
            def one(g, carry):
                for ref in (k_ref, v_ref):
                    act(pltpu.make_async_copy(zeros, ref.at[r, pl.ds(g * GRAN, GRAN)], sem))
                return carry

            lax.fori_loop(jnp.minimum(n_ref[r] // GRAN + 1, WIN_G), WIN_G, one, 0)

    each(lambda copy: copy.start())
    each(lambda copy: copy.wait())


def cleared(n, shape):
    return pl.pallas_call(
        cleared_kernel,
        grid_spec=pltpu.PrefetchScalarGridSpec(
            num_scalar_prefetch=1, grid=(1,), in_specs=[], out_specs=[ANYWHERE, ANYWHERE],
            scratch_shapes=[pltpu.VMEM((GRAN, WAYS, 256), jnp.bfloat16), pltpu.SemaphoreType.DMA]),
        out_shape=[jax.ShapeDtypeStruct(shape, jnp.bfloat16)] * 2,
        compiler_params=pltpu.CompilerParams(vmem_limit_bytes=VMEM_LIMIT),
        cost_estimate=cost(20_000_000),
        name="cleared",
    )(n)


class Lists:
    def __init__(self, n, row0, seq_g):
        self.n, self.row0, self.seq_g = n, row0, seq_g
        self.lap = n // WINDOW
        self.cut = n % WINDOW
        width = jnp.minimum(n // GRAN + 1, WIN_G)
        self.off1 = width[..., 0:1]
        self.off2 = self.off1 + width[..., 1:2]
        self.size = self.off2 + width[..., 2:3]

    def of_row(self, x, r):
        return jnp.where(r == 0, x[..., 0:1], jnp.where(r == 1, x[..., 1:2], x[..., 2:3]))

    def at(self, i):
        r = (i >= self.off1).astype(jnp.int32) + (i >= self.off2).astype(jnp.int32)
        return r, i - jnp.where(r == 0, 0, jnp.where(r == 1, self.off1, self.off2))

    def source(self, i):
        r, g = self.at(i)
        lap, cut = self.of_row(self.lap, r), self.of_row(self.cut, r)
        older = jnp.maximum(lap - 1, 0)
        base = (self.row0 + r) * self.seq_g
        src = base + jnp.minimum(jnp.where(g <= cut // GRAN, lap, older) * WIN_G + g, self.seq_g - 1)
        mixed = jnp.where(lap >= 1, base + older * WIN_G + g, -1)
        return src, jnp.where(g == cut // GRAN, (mixed + 1) * GRAN + cut % GRAN, -1)


def pack_kernel(base, size, steps, source, extra, *refs):
    num = source.num_scalars
    scalars, refs = refs[:num], refs[num:]
    prefills, extras, outs, (buf, older, sems) = refs[:-5 - extra], refs[-5 - extra:-5], refs[-5:-3], refs[-3:]
    at = source.reader(*scalars)
    i = pl.program_id(0)
    total = steps * len(prefills)
    slots = buf.shape[0]
    slot = lax.rem(i, slots)

    def by_tensor(step, do):
        for k, ref in enumerate(prefills):
            pl.when((step >= k * steps) & (step < (k + 1) * steps))(functools.partial(do, k, ref))

    def fetch(step):
        first = base + lax.rem(step, steps) * size
        to = lax.rem(step, slots)

        def from_ref(k, ref):
            for a in BOTH:
                def one(t, found):
                    src, code = at(a, first + t)
                    if not extras:
                        pltpu.make_async_copy(ref.at[src], buf.at[to, a, t], sems.at[0, to]).start()
                    else:
                        @pl.when(src < ELSEWHERE)
                        def _():
                            pltpu.make_async_copy(ref.at[src], buf.at[to, a, t], sems.at[0, to]).start()

                        for e, other in enumerate(extras):

                            @pl.when((src >= ELSEWHERE + e * HALF) & (src < ELSEWHERE + (e + 1) * HALF))
                            def _():
                                pltpu.make_async_copy(other.at[src - ELSEWHERE + (k - e) * HALF], buf.at[to, a, t], sems.at[0, to]).start()
                    mixed = code >= GRAN

                    @pl.when(mixed)
                    def _():
                        pltpu.make_async_copy(ref.at[code // GRAN - 1], older.at[to, a, found], sems.at[2, to]).start()

                    return found + mixed.astype(jnp.int32)

                lax.fori_loop(0, size, one, jnp.int32(0))

        by_tensor(step, from_ref)

    def stores(step):
        to = lax.rem(step, slots)
        return [pltpu.make_async_copy(buf.at[to, a], outs[a].at[pl.ds(step * size, size)], sems.at[1, to]) for a in BOTH]

    @pl.when(i == 0)
    def _():
        fetch(i)

    if total > 1:
        @pl.when(i + 1 < total)
        def _():
            if total > slots:
                @pl.when(i + 1 >= slots)
                def _():
                    for copy in stores(i + 1 - slots):
                        copy.wait()
            fetch(i + 1)

    pltpu.make_async_copy(buf.at[slot], buf.at[slot], sems.at[0, slot]).wait()
    first = base + lax.rem(i, steps) * size
    for a in BOTH:
        def patch(t, found):
            code = at(a, first + t)[1]
            mixed = code >= GRAN

            @pl.when(code >= 0)
            def _():
                @pl.when(mixed)
                def _():
                    pltpu.make_async_copy(older.at[slot, a, found], older.at[slot, a, found], sems.at[2, slot]).wait()

                newer = lax.broadcasted_iota(jnp.int32, (GRAN, 256), 0) < lax.rem(code, GRAN)
                rest = jnp.where(mixed, older[slot, a, found].astype(jnp.float32), 0.0)
                buf[slot, a, t] = jnp.where(newer, buf[slot, a, t].astype(jnp.float32), rest).astype(jnp.bfloat16)

            return found + mixed.astype(jnp.int32)

        lax.fori_loop(0, size, patch, jnp.int32(0))
    for copy in stores(i):
        copy.start()

    @pl.when(i == total - 1)
    def _():
        for back in range(min(slots, total)):
            for copy in stores(i - back):
                copy.wait()


class FromTable:
    num_scalars = 2

    def __init__(self, src, mix):
        self.scalars = (src, mix)

    def reader(self, src_ref, mix_ref):
        return lambda a, i: (src_ref[a, i], mix_ref[a, i])


class FromLengths:
    num_scalars = 1

    def __init__(self, lengths, seq_g):
        self.scalars = (lengths,)
        self.seq_g = seq_g

    def reader(self, n_ref):
        me = lax.axis_index('sh').astype(jnp.int32)

        def at(a, i):
            row0 = (me ^ (2 + a)) * ROWS
            n = [n_ref[row0 + r] for r in range(ROWS)]
            ends, end = [], 0
            for x in n:
                end = end + jnp.minimum(x // GRAN + 1, WIN_G)
                ends.append(end)
            r = jnp.where(i >= ends[0], 1, 0) + jnp.where(i >= ends[1], 1, 0)
            g = i - jnp.where(r == 0, 0, jnp.where(r == 1, ends[0], ends[1]))
            length = jnp.where(r == 0, n[0], jnp.where(r == 1, n[1], n[2]))
            lap, cut = length // WINDOW, lax.rem(length, WINDOW)
            older = jnp.maximum(lap - 1, 0)
            first = (row0 + r) * self.seq_g
            src = first + jnp.minimum(jnp.where(g <= cut // GRAN, lap, older) * WIN_G + g, self.seq_g - 1)
            mixed = jnp.where(lap >= 1, first + older * WIN_G + g, -1)
            valid = i < ends[2]
            return jnp.where(valid, src, 0), jnp.where(valid & (g == cut // GRAN), (mixed + 1) * GRAN + lax.rem(cut, GRAN), -1)

        return at


def pack(prefills, source, base, count, extras=()):
    size = next(x for x in (16, 8, 4) if count % x == 0)
    steps = count // size
    total = count * len(prefills)
    return pl.pallas_call(
        functools.partial(pack_kernel, base, size, steps, source, len(extras)),
        grid_spec=pltpu.PrefetchScalarGridSpec(
            num_scalar_prefetch=source.num_scalars,
            grid=(steps * len(prefills),),
            in_specs=[ANYWHERE] * (len(prefills) + len(extras)),
            out_specs=[ANYWHERE] * 2,
            scratch_shapes=[pltpu.VMEM((3, 2, size, GRAN, 256), jnp.bfloat16), pltpu.VMEM((3, 2, 2 * ROWS + 1, GRAN, 256), jnp.bfloat16), pltpu.SemaphoreType.DMA((3, 3))],
        ),
        out_shape=[jax.ShapeDtypeStruct((total, GRAN, 256), jnp.bfloat16)] * 2,
        compiler_params=SERIAL,
        cost_estimate=cost(total * 130_000),
        name="pack",
    )(*source.scalars, *prefills, *extras)


def assemble_kernel(is_key, base, size, steps, segments, code_ref, idx_ref, n_ref, me_ref, *refs):
    num_far = 2 * (1 + max(s[2] for s in segments))
    far_refs = refs[:num_far]
    near_ref, own_ref, new_ref, qp_ref, prev_ref, _, cache_ref, res_ref, xb, mix, ob, acc, sems = refs[num_far:]
    i = pl.program_id(0)
    me = me_ref[0]
    slot = lax.rem(i, 2)

    def code_at(step, t):
        return code_ref[0, base + step * size + t]

    def active_at(step):
        return functools.reduce(jnp.maximum, [code_at(step, t) for t in range(size)]) >= 0

    def read(step, buf):
        @pl.when(active_at(step))
        def _():
            for begin, end, entry, offsets, count, place in segments:
                @pl.when((step >= begin) & (step < end))
                def _():
                    for d in BOTH:
                        pltpu.make_async_copy(far_refs[2 * entry + d].at[pl.ds(offsets[d] + (step - begin) * size, count)], xb.at[buf, me ^ (2 + d), pl.ds(place, count)], sems.at[0, buf]).start()

            def one(t, carry):
                at = idx_ref[0, base + step * size + t]
                pltpu.make_async_copy(near_ref.at[at], xb.at[buf, me ^ 1, t], sems.at[0, buf]).start()
                pltpu.make_async_copy(own_ref.at[at], xb.at[buf, me, t], sems.at[0, buf]).start()
                return carry

            lax.fori_loop(0, size, one, 0)

    def write(step, t, buf):
        code = code_at(step, t)
        return pltpu.make_async_copy(ob.at[buf, t], cache_ref.at[code // WIN_G, pl.ds(lax.rem(code, WIN_G) * GRAN, GRAN)], sems.at[1, buf])

    def written(step, buf):
        def one(t, carry):
            @pl.when(code_at(step, t) >= 0)
            def _():
                write(step, t, buf).wait()

            return carry

        lax.fori_loop(0, size, one, 0)

    @pl.when(i == 0)
    def _():
        read(i, slot)
        if not is_key:
            acc[...] = prev_ref[...]

    if steps > 1:
        @pl.when(i + 1 < steps)
        def _():
            read(i + 1, 1 - slot)

    if steps > 2:
        @pl.when(i >= 2)
        def _():
            written(i - 2, slot)

    active = active_at(i)

    @pl.when(active)
    def _():
        pltpu.make_async_copy(xb.at[slot], xb.at[slot], sems.at[0, slot]).wait()

        def one(t, carry):
            code = code_at(i, t)

            @pl.when(code < 0)
            def _():
                for h in range(WAYS):
                    xb[slot, h, t] = jnp.zeros((GRAN, 256), jnp.bfloat16)

            for r in range(ROWS):
                cut = lax.rem(n_ref[r], WINDOW)

                @pl.when(code == r * WIN_G + cut // GRAN)
                def _():
                    here = lax.broadcasted_iota(jnp.int32, (GRAN, 256), 0) == lax.rem(cut, GRAN)
                    for h in range(WAYS):
                        new = jnp.broadcast_to(new_ref[r * WAYS + h], (GRAN, 256))
                        xb[slot, h, t] = jnp.where(here, new, xb[slot, h, t].astype(jnp.float32)).astype(jnp.bfloat16)

            @pl.when(code >= 0)
            def _():
                for h in range(WAYS):
                    x = xb[slot, h, t].astype(jnp.float32)
                    for half in BOTH:
                        mix[half, pl.ds(h, GRAN, stride=WAYS), :] = x[:, half * 128:(half + 1) * 128]
                joined = beside([mix[half].astype(jnp.bfloat16) for half in BOTH])
                ob[slot, t] = joined.reshape(GRAN, WAYS, 256)
                write(i, t, slot).start()

            return carry

        lax.fori_loop(0, size, one, 0)

        lanes = size * GRAN
        if is_key:
            lane = lax.broadcasted_iota(jnp.int32, (8, lanes), 1)
            row = lax.broadcasted_iota(jnp.int32, (8, lanes), 0) // 2
            code = jnp.full((8, lanes), -1, jnp.int32)
            for t in range(size):
                code = jnp.where(lane // GRAN == t, code_at(i, t), code)
            length = jnp.where(row == 0, n_ref[0], jnp.where(row == 1, n_ref[1], n_ref[2]))
            place = (code % WIN_G) * GRAN + lane % GRAN
            live = (code >= 0) & (code // WIN_G == row) & ((length >= WINDOW) | (place <= length))
            for h in range(WAYS):
                s = lax.dot_general(qp_ref[h], xb[slot, h].reshape(lanes, 256), (((1,), (1,)), ((), ())), preferred_element_type=jnp.float32)
                res_ref[h] = jnp.where(live, s / 16.0, -jnp.inf)
        else:
            for h in range(WAYS):
                acc[h] += jnp.dot(qp_ref[h], xb[slot, h].reshape(lanes, 256), preferred_element_type=jnp.float32)

    if is_key:
        @pl.when(jnp.logical_not(active))
        def _():
            res_ref[...] = jnp.full_like(res_ref, -jnp.inf)

    @pl.when(i == steps - 1)
    def _():
        if not is_key:
            res_ref[...] = acc[...]
        if steps >= 2:
            written(i - 1, 1 - slot)
        written(i, slot)


def assemble(is_key, base, codes, places, n, me, far, near, own, new, qp, prev, cache):
    total = sum(f[3] for f in far)
    size = min(STEP, total)
    steps = total // size
    segments, at = [], 0
    for entry, (_, _, offsets, count) in enumerate(far):
        if count >= size:
            segments.append((at // size, (at + count) // size, entry, offsets, size, 0))
        else:
            segments.append((at // size, at // size + 1, entry, offsets, count, at % size))
        at += count
    whole = lambda *shape: pl.BlockSpec(shape, lambda i, *_: (0,) * len(shape))
    by_step = pl.BlockSpec((WAYS, 8, size * GRAN), lambda i, *_: (0, 0, base // size + i))
    if is_key:
        qp_spec, prev_spec, res_spec = whole(WAYS, 8, 256), ANYWHERE, by_step
    else:
        qp_spec, prev_spec, res_spec = by_step, whole(WAYS, 8, 256), whole(WAYS, 8, 256)
    after = 4 + 2 * len(far) + 2
    aliases = {after + 3: 0}
    if is_key:
        aliases[after + 2] = 1
    return pl.pallas_call(
        functools.partial(assemble_kernel, is_key, base, size, steps, segments),
        grid_spec=pltpu.PrefetchScalarGridSpec(
            num_scalar_prefetch=4,
            grid=(steps,),
            in_specs=[ANYWHERE] * (2 * len(far) + 2) + [whole(ROWS * WAYS, 1, 256), qp_spec, prev_spec, ANYWHERE],
            out_specs=[ANYWHERE, res_spec],
            scratch_shapes=[
                pltpu.VMEM((2, WAYS, size, GRAN, 256), jnp.bfloat16),
                pltpu.VMEM((2, WAYS * GRAN, 128), jnp.float32),
                pltpu.VMEM((2, size, GRAN, WAYS, 256), jnp.bfloat16),
                pltpu.VMEM((WAYS, 8, 256), jnp.float32),
                pltpu.SemaphoreType.DMA((2, 2)),
            ],
        ),
        out_shape=[jax.ShapeDtypeStruct(cache.shape, cache.dtype), jax.ShapeDtypeStruct(prev.shape, prev.dtype)],
        input_output_aliases=aliases,
        compiler_params=SERIAL,
        cost_estimate=cost(steps * 4_000_000),
        name="assemble_keys" if is_key else "assemble_values",
    )(codes, places, n, me, *[x for f in far for x in f[:2]], near, own, new, qp, prev, cache)


def hand_back_kernel(table_ref, *refs):
    outs, sem = refs[-3:-1], refs[-1]
    arrays = refs[:-3]
    units = len(arrays) // 2

    def one(t, carry):
        for u in range(units):
            size = UNITS[u % len(UNITS)]

            @pl.when(table_ref[0, t] == u)
            def _():
                for k in BOTH:
                    for d in BOTH:
                        pltpu.make_async_copy(arrays[2 * u + d].at[table_ref[1, t] + k * size], outs[k].at[d * HALF + t], sem).start()
        return carry

    def wait(t, carry):
        @pl.when(table_ref[0, t] >= 0)
        def _():
            for k in BOTH:
                for d in BOTH:
                    pltpu.make_async_copy(outs[k].at[d * HALF + t], outs[k].at[d * HALF + t], sem).wait()

        return carry

    lax.fori_loop(0, HALF, one, 0)
    lax.fori_loop(0, HALF, wait, 0)


def hand_back(table, pairs):
    arrays = [x for pair in pairs for x in pair]
    return pl.pallas_call(
        hand_back_kernel,
        grid_spec=pltpu.PrefetchScalarGridSpec(
            num_scalar_prefetch=1, grid=(1,), in_specs=[ANYWHERE] * len(arrays),
            out_specs=[pl.BlockSpec((CROSS, GRAN, 256), lambda i, t_ref: (0, 0, 0))] * 2, scratch_shapes=[pltpu.SemaphoreType.DMA]),
        out_shape=[jax.ShapeDtypeStruct((CROSS, GRAN, 256), jnp.bfloat16)] * 2,
        compiler_params=pltpu.CompilerParams(vmem_limit_bytes=VMEM_LIMIT),
        cost_estimate=cost(8_000_000),
        name="hand_back",
    )(table, *arrays)


def solution(mesh):
    head_spec = P('dp', None, 'sh', None)
    row_spec = P(('dp', 'sh'))
    full_spec = P(None, None)

    def send(x, d):
        return lax.ppermute(x, 'sh', [(i, i ^ d) for i in range(WAYS)])

    def across(x):
        return lax.ppermute(x, 'dp', [(0, 1), (1, 0)])

    def step(k_prefill, v_prefill, lengths, residual, norm_gain, w_query, w_key, w_value, w_out):
        seq_g = k_prefill.shape[1] // GRAN
        me = lax.axis_index('sh').astype(jnp.int32)
        peers = me ^ jnp.arange(WAYS, dtype=jnp.int32)
        by_peer = lengths[(peers[:, None] * ROWS + jnp.arange(ROWS, dtype=jnp.int32)).reshape(-1)].reshape(WAYS, ROWS)
        mine = by_peer[0]
        prefill = {True: k_prefill.reshape(-1, GRAN, 256), False: v_prefill.reshape(-1, GRAN, 256)}

        def lists(*ds):
            return Lists(jnp.stack([by_peer[d] for d in ds]), jnp.stack([(me ^ d) * ROWS for d in ds])[:, None], seq_g)

        def span(count):
            return lax.broadcasted_iota(jnp.int32, (1, count), 1)

        def held(which, i):
            src, mixed = which.source(i)
            valid = i < which.size
            return jnp.where(valid, src, 0), jnp.where(valid, mixed, -1)

        far, close, self_list = lists(2, 3), lists(1, 0), lists(0)
        fixed_src, fixed_mix = held(far, span(FIXED))
        close_src, close_mix = held(close, span(ROWS * WIN_G))

        chip, core = me // 2, me % 2

        def rests(lens):
            sizes = jnp.sum(jnp.minimum(lens // GRAN + 1, WIN_G).reshape(WAYS, ROWS), axis=1)
            return jnp.maximum(sizes - FIXED, 0).reshape(WAYS // 2, 2)

        def of_chip(x, c):
            return jnp.where(c == 0, x[0], x[1])

        other_lengths = across(lengths)
        rest, other_rest = rests(lengths), rests(other_lengths)
        need, other_need = jnp.sum(rest, axis=1), jnp.sum(other_rest, axis=1)
        level = jnp.max(jnp.maximum((need + other_need + 4 * QUANTUM - 1) // (4 * QUANTUM), (jnp.maximum(need, other_need) - CROSS + 2 * QUANTUM - 1) // (2 * QUANTUM)))
        spare = QUANTUM * level
        on = active_units(level)
        column = span(SPARE)
        unit = functools.reduce(jnp.add, [(column >= s).astype(jnp.int32) for s in starts_of(UNITS)[1:]])
        skipped, used, place = 0, jnp.zeros_like(column, dtype=bool), column
        for u, size in enumerate(UNITS):
            used = jnp.where(unit == u, on[u], used)
            place = jnp.where(unit == u, column - skipped, place)
            skipped = skipped + jnp.where(on[u], 0, size)
        used = used & (column < sum(UNITS))
        far_n = lax.dynamic_slice_in_dim(lengths, (1 - chip) * 2 * ROWS, 2 * ROWS).reshape(2, ROWS)
        far_lists = Lists(far_n, ((1 - chip) * 2 + jnp.arange(2, dtype=jnp.int32))[:, None] * ROWS, seq_g)
        far_first, far_need = of_chip(rest, 1 - chip)[0], of_chip(need, 1 - chip)
        far_guests = jnp.maximum(of_chip(other_need, 1 - chip) - 2 * spare, 0)

        def from_rest(c):
            second = c >= far_first
            src, mixed = far_lists.source(FIXED + c - jnp.where(second, far_first, 0))
            return tuple(jnp.where(second[0], x[1], x[0]) for x in (src, mixed))

        both_used = beside([used, used])[0]
        z = beside([place + (core ^ a) * spare for a in BOTH])
        src, mixed = from_rest(z)
        order = z[0] - far_need
        hosted, guest = both_used & (order < 0), both_used & (order >= 0) & (order < far_guests)
        spare_src = jnp.where(hosted, src, jnp.where(guest, ELSEWHERE + order, 0)).reshape(2, SPARE)
        spare_mix = jnp.where(hosted, mixed, -1).reshape(2, SPARE)
        z = 2 * spare + span(CROSS)
        src, mixed = from_rest(z)
        hosted = z[0] < far_need
        cross_src, cross_mix = jnp.where(hosted, src, 0).reshape(2, HALF), jnp.where(hosted, mixed, -1).reshape(2, HALF)

        own_first, own_need = of_chip(rest, chip)[0], of_chip(need, chip)

        def belongs(i, valid):
            r, g = self_list.at(i)
            return jnp.where(valid & (i < self_list.size), r * WIN_G + g, -1), jnp.clip(i, 0, ROWS * WIN_G - 1)

        def rest_belongs(c, valid):
            second = c >= own_first
            return belongs(FIXED + c - jnp.where(second, own_first, 0), valid & (c < own_need) & (second == (core == 1)))

        half_span = span(HALF)
        parts = [belongs(span(FIXED), True), rest_belongs(place + core * spare, used), rest_belongs(place + (1 - core) * spare, used)]
        parts += [rest_belongs(2 * spare + x * (HALF) + half_span, True) for x in (core, 1 - core)]
        codes = beside([p[0] for p in parts])
        places = beside([p[1] for p in parts])

        w = core * (HALF) + half_span
        z = own_need + w
        high = (z >= spare).astype(jnp.int32)
        u = z - high * spare
        back_unit, back_at, begin = jnp.full_like(u, -1), jnp.zeros_like(u), 0
        for k, size in enumerate(UNITS):
            inside = (u >= begin) & (u < begin + jnp.where(on[k], size, 0))
            back_unit = jnp.where(inside, k, back_unit)
            back_at = jnp.where(inside, u - begin, back_at)
            begin = begin + jnp.where(on[k], size, 0)
        back_unit = jnp.where(w < jnp.maximum(of_chip(other_need, chip) - 2 * spare, 0), back_unit + len(UNITS) * (high != core).astype(jnp.int32), -1)
        back_table = jnp.concatenate([back_unit, back_at], axis=0)

        fixed_from, close_from = FromTable(fixed_src, fixed_mix), FromTable(close_src, close_mix)
        spare_from, cross_from = FromTable(spare_src, spare_mix), FromTable(cross_src, cross_mix)
        fixed_got = {True: [], False: []}
        packed_values = []
        for i, (base, count) in enumerate(zip(starts_of(K_PIECES), K_PIECES)):
            out = pack([prefill[True]], FromLengths(lengths, seq_g) if i == 0 else fixed_from, base, count)
            a = send(out[0], 2)
            b = send(out[1], 3)
            fixed_got[True].append((a, b))
        cross = pack([prefill[True], prefill[False]], cross_from, 0, HALF)
        guests = []
        for e in BOTH:
            guests.append(across(cross[e]))
        close_got = {}
        for is_key in KV:
            near, own = pack([prefill[is_key]], close_from, 0, ROWS * WIN_G)
            close_got[is_key] = (send(near, 1), own)
        spare_packed = [pack([prefill[True], prefill[False]], spare_from, base, count, guests) for base, count in zip(starts_of(UNITS), UNITS)]
        for base, count in zip(starts_of(V_PIECES), V_PIECES):
            packed_values.append(pack([prefill[False]], fixed_from, base, count))

        residual, cross = lax.optimization_barrier((residual, cross))
        resid_f32 = residual.astype(jnp.float32)
        inv_rms = lax.rsqrt(jnp.mean(resid_f32 * resid_f32, axis=-1, keepdims=True) + EPS)
        normed = (resid_f32 * inv_rms * norm_gain.astype(jnp.float32)).astype(jnp.bfloat16)
        q_group = w_query.shape[1] // (WAYS * 256)
        q_heads = jnp.dot(normed, w_query, preferred_element_type=jnp.float32).astype(jnp.bfloat16).reshape(ROWS, WAYS, q_group, 256)
        k_new = jnp.dot(normed, w_key, preferred_element_type=jnp.float32).astype(jnp.bfloat16).reshape(ROWS, WAYS, 256)
        v_new = jnp.dot(normed, w_value, preferred_element_type=jnp.float32).astype(jnp.bfloat16).reshape(ROWS, WAYS, 256)
        q_heads = rotate(q_heads, mine)
        k_new = rotate(k_new, mine)
        new = {True: k_new.astype(jnp.float32).reshape(-1, 1, 256), False: v_new.astype(jnp.float32).reshape(-1, 1, 256)}
        q_pad = jnp.pad(q_heads.transpose(1, 0, 2, 3).reshape(WAYS, ROWS * q_group, 256), ((0, 0), (0, 8 - ROWS * q_group), (0, 0)))
        caches = cleared(mine, (ROWS, WINDOW, WAYS, 256))
        scores = blank((WAYS, 8, codes.shape[1] * GRAN), jnp.float32)

        def branch(lvl):
            keep = [bool(x) for x in active_units(lvl)]

            def run(pairs):
                return [(send(a, 2), send(b, 3)) if k else (blank(a.shape, a.dtype), blank(b.shape, b.dtype)) for k, (a, b) in zip(keep, pairs)]

            return run

        spare_packed, packed_values, ready = lax.optimization_barrier((spare_packed, packed_values, (new, q_pad, scores, caches, close_got[True][1], close_got[False][1])))
        new, q_pad, scores, (k_cache, v_cache), own_k, own_v = ready
        own = {True: own_k, False: own_v}
        spare_got = lax.switch(level, [branch(x) for x in range(LEVELS)], spare_packed)
        spare_got, packed_values = lax.optimization_barrier((spare_got, packed_values))
        for a, b in packed_values:
            a = send(a, 2)
            b = send(b, 3)
            fixed_got[False].append((a, b))
        forwarded = [(send(b, 1), send(a, 1)) for a, b in spare_got]
        found = hand_back(back_table, spare_got + forwarded)
        handed, handed_on = [], []
        for k in BOTH:
            handed.append(across(found[k]))
            handed_on.append(send(handed[k], 1))

        me1 = me.reshape(1)

        def run(is_key, base, far_parts, qp, prev, cache):
            return assemble(is_key, base, codes, places, mine, me1, far_parts, close_got[is_key][0], own[is_key], new[is_key], qp, prev, cache)

        def fixed(pieces, got):
            return [(a, b, (0, 0), count) for (a, b), count in zip(got, pieces)]

        def spares(is_key):
            runs = []
            for got in (spare_got, forwarded):
                runs += [(a, b, (0, 0) if is_key else (count, count), count) for (a, b), count in zip(got, UNITS)]
                runs.append(runs[-1])
            return runs

        def returned(is_key):
            own_half, other_half = handed[0 if is_key else 1], handed_on[0 if is_key else 1]
            return [(own_half, own_half, (0, HALF), HALF), (other_half, other_half, (HALF, 0), HALF)]


        k_cache, scores = run(True, 0, fixed(K_PIECES, fixed_got[True]), q_pad, scores, k_cache)
        k_cache, scores = run(True, FIXED, spares(True), q_pad, scores, k_cache)
        k_cache, scores = run(True, FIXED + 2 * SPARE, returned(True), q_pad, scores, k_cache)
        exp_scores = jnp.exp(scores - jnp.max(scores, axis=-1, keepdims=True))
        weights = (exp_scores / jnp.sum(exp_scores, axis=-1, keepdims=True)).astype(jnp.bfloat16)
        sums = jnp.zeros((WAYS, 8, 256), jnp.float32)
        v_cache, sums = run(False, FIXED, spares(False), weights, sums, v_cache)
        v_cache, sums = run(False, FIXED + 2 * SPARE, returned(False), weights, sums, v_cache)
        for base, part in zip(starts_of(V_PIECES), fixed(V_PIECES, fixed_got[False])):
            v_cache, sums = run(False, base, [part], weights, sums, v_cache)
        attn_out = sums[:, :ROWS * q_group].astype(jnp.bfloat16).reshape(WAYS, ROWS, q_group * 256).transpose(1, 0, 2).reshape(ROWS, WAYS * q_group * 256)
        resid_out = (resid_f32 + jnp.dot(attn_out, w_out, preferred_element_type=jnp.float32)).astype(jnp.bfloat16)
        return resid_out, k_cache, v_cache

    return jax.shard_map(
        step, mesh=mesh, in_specs=(head_spec, head_spec, P('dp'), P(('dp', 'sh'), None), P(None), full_spec, full_spec, full_spec, full_spec),
        out_specs=(P(('dp', 'sh'), None), row_spec, row_spec), check_vma=False)
```

```python
import functools

import jax
import jax.numpy as jnp
from jax import lax
from jax.experimental import pallas as pl
from jax.experimental.pallas import tpu as pltpu
from jax.sharding import PartitionSpec as P


WINDOW = 4096
THETA = 10000.0
EPS = 1e-5
GRAN = 64
WIN_G = WINDOW // GRAN
STEP = 8
FIXED = 112
UNITS = (64, 32, 16, 8, 4, 2)
QUANTUM = UNITS[-1]
SPARE = sum(UNITS) + QUANTUM
K_PIECES = (8, 24, 80)
V_PIECES = (80, 24, 8)
CROSS = 48
ELSEWHERE = 1 << 20
WAYS, ROWS = 4, 3
HEAD, GROUP = 256, 2
LEVELS = (ROWS * WIN_G - FIXED) // QUANTUM + 1
VMEM_LIMIT = 67_043_328
HALF = CROSS // 2
KV = (True, False)
BOTH = range(2)
SERIAL = pltpu.CompilerParams(dimension_semantics=("arbitrary",), vmem_limit_bytes=VMEM_LIMIT)
ANYWHERE = pl.BlockSpec(memory_space=pl.ANY)


beside = functools.partial(jnp.concatenate, axis=1)


def cost(moved):
    return pl.CostEstimate(flops=10_000_000, bytes_accessed=moved, transcendentals=0)


def starts_of(sizes):
    return [sum(sizes[:i]) for i in range(len(sizes))]


def active_units(level):
    return [(level & (size // QUANTUM)) != 0 for size in UNITS]


def rotate(heads, positions):
    head_dim = heads.shape[-1]
    half_dim = head_dim // 2
    inv_freq = THETA ** (-2.0 * jnp.arange(half_dim, dtype=jnp.float32) / head_dim)
    angles = positions.astype(jnp.float32).reshape(positions.shape + (1,) * (heads.ndim - 1)) * inv_freq
    cos_part = jnp.cos(angles)
    sin_part = jnp.sin(angles)
    first_half = heads[..., :half_dim].astype(jnp.float32)
    second_half = heads[..., half_dim:].astype(jnp.float32)
    return jnp.concatenate([first_half * cos_part - second_half * sin_part, second_half * cos_part + first_half * sin_part], axis=-1).astype(jnp.bfloat16)


def blank(shape, dtype):
    return pl.pallas_call(
        lambda o_ref: None,
        out_shape=jax.ShapeDtypeStruct(shape, dtype),
        out_specs=ANYWHERE,
        name="blank",
    )()


def cleared_kernel(n_ref, k_ref, v_ref, zeros, sem):
    zeros[...] = jnp.zeros_like(zeros)

    def each(act):
        for r in range(ROWS):
            def one(g, carry):
                for ref in (k_ref, v_ref):
                    act(pltpu.make_async_copy(zeros, ref.at[r, pl.ds(g * GRAN, GRAN)], sem))
                return carry

            lax.fori_loop(jnp.minimum(n_ref[r] // GRAN + 1, WIN_G), WIN_G, one, 0)

    each(lambda copy: copy.start())
    each(lambda copy: copy.wait())


def cleared(n, shape):
    return pl.pallas_call(
        cleared_kernel,
        grid_spec=pltpu.PrefetchScalarGridSpec(
            num_scalar_prefetch=1, grid=(1,), in_specs=[], out_specs=[ANYWHERE, ANYWHERE],
            scratch_shapes=[pltpu.VMEM((GRAN, WAYS, HEAD), jnp.bfloat16), pltpu.SemaphoreType.DMA]),
        out_shape=[jax.ShapeDtypeStruct(shape, jnp.bfloat16)] * 2,
        compiler_params=pltpu.CompilerParams(vmem_limit_bytes=VMEM_LIMIT),
        cost_estimate=cost(20_000_000),
        name="cleared",
    )(n)


class Lists:
    def __init__(self, n, row0, seq_g):
        self.n, self.row0, self.seq_g = n, row0, seq_g
        self.lap = n // WINDOW
        self.cut = n % WINDOW
        width = jnp.minimum(n // GRAN + 1, WIN_G)
        self.off1 = width[..., 0:1]
        self.off2 = self.off1 + width[..., 1:2]
        self.size = self.off2 + width[..., 2:3]

    def of_row(self, x, r):
        return jnp.where(r == 0, x[..., 0:1], jnp.where(r == 1, x[..., 1:2], x[..., 2:3]))

    def at(self, i):
        r = (i >= self.off1).astype(jnp.int32) + (i >= self.off2).astype(jnp.int32)
        return r, i - jnp.where(r == 0, 0, jnp.where(r == 1, self.off1, self.off2))

    def source(self, i):
        r, g = self.at(i)
        lap, cut = self.of_row(self.lap, r), self.of_row(self.cut, r)
        older = jnp.maximum(lap - 1, 0)
        base = (self.row0 + r) * self.seq_g
        src = base + jnp.minimum(jnp.where(g <= cut // GRAN, lap, older) * WIN_G + g, self.seq_g - 1)
        mixed = jnp.where(lap >= 1, base + older * WIN_G + g, -1)
        return src, jnp.where(g == cut // GRAN, (mixed + 1) * GRAN + cut % GRAN, -1)


def pack_kernel(base, size, steps, source, extra, *refs):
    num = source.num_scalars
    scalars, refs = refs[:num], refs[num:]
    prefills, extras, outs, (buf, older, sems) = refs[:-5 - extra], refs[-5 - extra:-5], refs[-5:-3], refs[-3:]
    at = source.reader(*scalars)
    i = pl.program_id(0)
    total = steps * len(prefills)
    slots = buf.shape[0]
    slot = lax.rem(i, slots)

    def by_tensor(step, do):
        for k, ref in enumerate(prefills):
            pl.when((step >= k * steps) & (step < (k + 1) * steps))(functools.partial(do, k, ref))

    def fetch(step):
        first = base + lax.rem(step, steps) * size
        to = lax.rem(step, slots)

        def from_ref(k, ref):
            for a in BOTH:
                def one(t, found):
                    src, code = at(a, first + t)
                    if not extras:
                        pltpu.make_async_copy(ref.at[src], buf.at[to, a, t], sems.at[0, to]).start()
                    else:
                        @pl.when(src < ELSEWHERE)
                        def _():
                            pltpu.make_async_copy(ref.at[src], buf.at[to, a, t], sems.at[0, to]).start()

                        for e, other in enumerate(extras):

                            @pl.when((src >= ELSEWHERE + e * HALF) & (src < ELSEWHERE + (e + 1) * HALF))
                            def _():
                                pltpu.make_async_copy(other.at[src - ELSEWHERE + (k - e) * HALF], buf.at[to, a, t], sems.at[0, to]).start()
                    mixed = code >= GRAN

                    @pl.when(mixed)
                    def _():
                        pltpu.make_async_copy(ref.at[code // GRAN - 1], older.at[to, a, found], sems.at[2, to]).start()

                    return found + mixed.astype(jnp.int32)

                lax.fori_loop(0, size, one, jnp.int32(0))

        by_tensor(step, from_ref)

    def stores(step):
        to = lax.rem(step, slots)
        return [pltpu.make_async_copy(buf.at[to, a], outs[a].at[pl.ds(step * size, size)], sems.at[1, to]) for a in BOTH]

    @pl.when(i == 0)
    def _():
        fetch(i)

    if total > 1:
        @pl.when(i + 1 < total)
        def _():
            if total > slots:
                @pl.when(i + 1 >= slots)
                def _():
                    for copy in stores(i + 1 - slots):
                        copy.wait()
            fetch(i + 1)

    pltpu.make_async_copy(buf.at[slot], buf.at[slot], sems.at[0, slot]).wait()
    first = base + lax.rem(i, steps) * size
    for a in BOTH:
        def patch(t, found):
            code = at(a, first + t)[1]
            mixed = code >= GRAN

            @pl.when(code >= 0)
            def _():
                @pl.when(mixed)
                def _():
                    pltpu.make_async_copy(older.at[slot, a, found], older.at[slot, a, found], sems.at[2, slot]).wait()

                newer = lax.broadcasted_iota(jnp.int32, (GRAN, HEAD), 0) < lax.rem(code, GRAN)
                rest = jnp.where(mixed, older[slot, a, found].astype(jnp.float32), 0.0)
                buf[slot, a, t] = jnp.where(newer, buf[slot, a, t].astype(jnp.float32), rest).astype(jnp.bfloat16)

            return found + mixed.astype(jnp.int32)

        lax.fori_loop(0, size, patch, jnp.int32(0))
    for copy in stores(i):
        copy.start()

    @pl.when(i == total - 1)
    def _():
        for back in range(min(slots, total)):
            for copy in stores(i - back):
                copy.wait()


class FromTable:
    num_scalars = 2

    def __init__(self, src, mix):
        self.scalars = (src, mix)

    def reader(self, src_ref, mix_ref):
        return lambda a, i: (src_ref[a, i], mix_ref[a, i])


class FromLengths:
    num_scalars = 1

    def __init__(self, lengths, seq_g):
        self.scalars = (lengths,)
        self.seq_g = seq_g

    def reader(self, n_ref):
        me = lax.axis_index('sh').astype(jnp.int32)

        def at(a, i):
            row0 = (me ^ (2 + a)) * ROWS
            n = [n_ref[row0 + r] for r in range(ROWS)]
            ends, end = [], 0
            for x in n:
                end = end + jnp.minimum(x // GRAN + 1, WIN_G)
                ends.append(end)
            r = jnp.where(i >= ends[0], 1, 0) + jnp.where(i >= ends[1], 1, 0)
            g = i - jnp.where(r == 0, 0, jnp.where(r == 1, ends[0], ends[1]))
            length = jnp.where(r == 0, n[0], jnp.where(r == 1, n[1], n[2]))
            lap, cut = length // WINDOW, lax.rem(length, WINDOW)
            older = jnp.maximum(lap - 1, 0)
            first = (row0 + r) * self.seq_g
            src = first + jnp.minimum(jnp.where(g <= cut // GRAN, lap, older) * WIN_G + g, self.seq_g - 1)
            mixed = jnp.where(lap >= 1, first + older * WIN_G + g, -1)
            valid = i < ends[2]
            return jnp.where(valid, src, 0), jnp.where(valid & (g == cut // GRAN), (mixed + 1) * GRAN + lax.rem(cut, GRAN), -1)

        return at


def pack(prefills, source, base, count, extras=()):
    size = next(x for x in (16, 8, 4, 2) if count % x == 0)
    steps = count // size
    total = count * len(prefills)
    return pl.pallas_call(
        functools.partial(pack_kernel, base, size, steps, source, len(extras)),
        grid_spec=pltpu.PrefetchScalarGridSpec(
            num_scalar_prefetch=source.num_scalars,
            grid=(steps * len(prefills),),
            in_specs=[ANYWHERE] * (len(prefills) + len(extras)),
            out_specs=[ANYWHERE] * 2,
            scratch_shapes=[pltpu.VMEM((3, 2, size, GRAN, HEAD), jnp.bfloat16), pltpu.VMEM((3, 2, 2 * ROWS + 1, GRAN, HEAD), jnp.bfloat16), pltpu.SemaphoreType.DMA((3, 3))],
        ),
        out_shape=[jax.ShapeDtypeStruct((total, GRAN, HEAD), jnp.bfloat16)] * 2,
        compiler_params=SERIAL,
        cost_estimate=cost(total * 130_000),
        name="pack",
    )(*source.scalars, *prefills, *extras)


def assemble_kernel(is_key, base, size, steps, segments, final, code_ref, idx_ref, n_ref, me_ref, *refs):
    num_far = 2 * (1 + max(s[2] for s in segments))
    far_refs = refs[:num_far]
    near_ref, own_ref, new_ref, qp_ref, prev_ref, _ = refs[num_far:num_far + 6]
    refs = refs[num_far + 6:]
    if final:
        w_ref, resid_ref, cache_ref, res_ref, xb, mix, ob, acc, sems, w_buf, w_sem = refs
        fetch_w = pltpu.make_async_copy(w_ref, w_buf, w_sem)
    else:
        cache_ref, res_ref, xb, mix, ob, acc, sems = refs
    i = pl.program_id(0)
    me = me_ref[0]
    slot = lax.rem(i, 2)

    def code_at(step, t):
        return code_ref[0, base + step * size + t]

    def active_at(step):
        return functools.reduce(jnp.maximum, [code_at(step, t) for t in range(size)]) >= 0

    def read(step, buf):
        @pl.when(active_at(step))
        def _():
            for begin, end, entry, offsets, count, place in segments:
                @pl.when((step >= begin) & (step < end))
                def _():
                    for d in BOTH:
                        pltpu.make_async_copy(far_refs[2 * entry + d].at[pl.ds(offsets[d] + (step - begin) * size, count)], xb.at[buf, me ^ (2 + d), pl.ds(place, count)], sems.at[0, buf]).start()

            def one(t, carry):
                at = idx_ref[0, base + step * size + t]
                pltpu.make_async_copy(near_ref.at[at], xb.at[buf, me ^ 1, t], sems.at[0, buf]).start()
                pltpu.make_async_copy(own_ref.at[at], xb.at[buf, me, t], sems.at[0, buf]).start()
                return carry

            lax.fori_loop(0, size, one, 0)

    def write(step, t, buf):
        code = code_at(step, t)
        return pltpu.make_async_copy(ob.at[buf, t], cache_ref.at[code // WIN_G, pl.ds(lax.rem(code, WIN_G) * GRAN, GRAN)], sems.at[1, buf])

    def written(step, buf):
        def one(t, carry):
            @pl.when(code_at(step, t) >= 0)
            def _():
                write(step, t, buf).wait()

            return carry

        lax.fori_loop(0, size, one, 0)

    @pl.when(i == 0)
    def _():
        read(i, slot)
        if final:
            fetch_w.start()
        if not is_key:
            acc[...] = prev_ref[...]

    if steps > 1:
        @pl.when(i + 1 < steps)
        def _():
            read(i + 1, 1 - slot)

    if steps > 2:
        @pl.when(i >= 2)
        def _():
            written(i - 2, slot)

    active = active_at(i)

    @pl.when(active)
    def _():
        pltpu.make_async_copy(xb.at[slot], xb.at[slot], sems.at[0, slot]).wait()

        def one(t, carry):
            code = code_at(i, t)

            @pl.when(code < 0)
            def _():
                for h in range(WAYS):
                    xb[slot, h, t] = jnp.zeros((GRAN, HEAD), jnp.bfloat16)

            for r in range(ROWS):
                cut = lax.rem(n_ref[r], WINDOW)

                @pl.when(code == r * WIN_G + cut // GRAN)
                def _():
                    here = lax.broadcasted_iota(jnp.int32, (GRAN, HEAD), 0) == lax.rem(cut, GRAN)
                    for h in range(WAYS):
                        new = jnp.broadcast_to(new_ref[r * WAYS + h], (GRAN, HEAD))
                        xb[slot, h, t] = jnp.where(here, new, xb[slot, h, t].astype(jnp.float32)).astype(jnp.bfloat16)

            @pl.when(code >= 0)
            def _():
                for h in range(WAYS):
                    x = xb[slot, h, t].astype(jnp.float32)
                    for half in BOTH:
                        mix[half, pl.ds(h, GRAN, stride=WAYS), :] = x[:, half * 128:(half + 1) * 128]
                joined = beside([mix[half].astype(jnp.bfloat16) for half in BOTH])
                ob[slot, t] = joined.reshape(GRAN, WAYS, HEAD)
                write(i, t, slot).start()

            return carry

        lax.fori_loop(0, size, one, 0)

        lanes = size * GRAN
        if is_key:
            lane = lax.broadcasted_iota(jnp.int32, (8, lanes), 1)
            row = lax.broadcasted_iota(jnp.int32, (8, lanes), 0) // 2
            code = jnp.full((8, lanes), -1, jnp.int32)
            for t in range(size):
                code = jnp.where(lane // GRAN == t, code_at(i, t), code)
            length = jnp.where(row == 0, n_ref[0], jnp.where(row == 1, n_ref[1], n_ref[2]))
            place = (code % WIN_G) * GRAN + lane % GRAN
            live = (code >= 0) & (code // WIN_G == row) & ((length >= WINDOW) | (place <= length))
            for h in range(WAYS):
                s = lax.dot_general(qp_ref[h], xb[slot, h].reshape(lanes, HEAD), (((1,), (1,)), ((), ())), preferred_element_type=jnp.float32)
                res_ref[h] = jnp.where(live, s / 16.0, -jnp.inf)
        else:
            for h in range(WAYS):
                acc[h] += jnp.dot(qp_ref[h], xb[slot, h].reshape(lanes, HEAD), preferred_element_type=jnp.float32)

    if is_key:
        @pl.when(jnp.logical_not(active))
        def _():
            res_ref[...] = jnp.full_like(res_ref, -jnp.inf)

    @pl.when(i == steps - 1)
    def _():
        if final:
            fetch_w.wait()
            mixed = [acc[h].astype(jnp.bfloat16) for h in range(WAYS)]
            by_group = []
            for g in range(GROUP):
                blocks = [w_buf[(h * GROUP + g) * HEAD:(h * GROUP + g + 1) * HEAD] for h in range(WAYS)]
                by_group.append(functools.reduce(jnp.add, [jnp.dot(x, w, preferred_element_type=jnp.float32) for x, w in zip(mixed, blocks)]))
            rows = [functools.reduce(jnp.add, [by_group[g][r * GROUP + g][None] for g in range(GROUP)]) for r in range(ROWS)]
            res_ref[...] = (resid_ref[...] + jnp.concatenate(rows, axis=0)).astype(jnp.bfloat16)
        elif not is_key:
            res_ref[...] = acc[...]
        if steps >= 2:
            written(i - 1, 1 - slot)
        written(i, slot)


def assemble(is_key, base, codes, places, n, me, far, near, own, new, qp, prev, cache, projection=()):
    total = sum(f[3] for f in far)
    size = min(STEP, total)
    steps = total // size
    segments, at = [], 0
    for entry, (_, _, offsets, count) in enumerate(far):
        if count >= size:
            segments.append((at // size, (at + count) // size, entry, offsets, size, 0))
        else:
            segments.append((at // size, at // size + 1, entry, offsets, count, at % size))
        at += count
    whole = lambda *shape: pl.BlockSpec(shape, lambda i, *_: (0,) * len(shape))
    by_step = pl.BlockSpec((WAYS, 8, size * GRAN), lambda i, *_: (0, 0, base // size + i))
    if is_key:
        qp_spec, prev_spec, res_spec = whole(WAYS, 8, HEAD), ANYWHERE, by_step
    else:
        qp_spec, prev_spec, res_spec = by_step, whole(WAYS, 8, HEAD), whole(WAYS, 8, HEAD)
    after = 4 + 2 * len(far) + 2
    aliases = {after + 3: 0}
    if is_key:
        aliases[after + 2] = 1
    res_shape, scratch = jax.ShapeDtypeStruct(prev.shape, prev.dtype), []
    if projection:
        weights, resid = projection
        res_shape, res_spec = jax.ShapeDtypeStruct(resid.shape, jnp.bfloat16), whole(*resid.shape)
        scratch = [pltpu.VMEM(weights.shape, weights.dtype), pltpu.SemaphoreType.DMA]
    return pl.pallas_call(
        functools.partial(assemble_kernel, is_key, base, size, steps, segments, bool(projection)),
        grid_spec=pltpu.PrefetchScalarGridSpec(
            num_scalar_prefetch=4,
            grid=(steps,),
            in_specs=[ANYWHERE] * (2 * len(far) + 2) + [whole(ROWS * WAYS, 1, HEAD), qp_spec, prev_spec, ANYWHERE] + [ANYWHERE, *[whole(*x.shape) for x in projection[1:]]][:len(projection)],
            out_specs=[ANYWHERE, res_spec],
            scratch_shapes=[
                pltpu.VMEM((2, WAYS, size, GRAN, HEAD), jnp.bfloat16),
                pltpu.VMEM((2, WAYS * GRAN, 128), jnp.float32),
                pltpu.VMEM((2, size, GRAN, WAYS, HEAD), jnp.bfloat16),
                pltpu.VMEM((WAYS, 8, HEAD), jnp.float32),
                pltpu.SemaphoreType.DMA((2, 2)),
            ] + scratch,
        ),
        out_shape=[jax.ShapeDtypeStruct(cache.shape, cache.dtype), res_shape],
        input_output_aliases=aliases,
        compiler_params=SERIAL,
        cost_estimate=cost(steps * 4_000_000),
        name="assemble_keys" if is_key else "assemble_values",
    )(codes, places, n, me, *[x for f in far for x in f[:2]], near, own, new, qp, prev, cache, *projection)


def hand_back_kernel(table_ref, *refs):
    outs, sem = refs[-3:-1], refs[-1]
    arrays = refs[:-3]
    units = len(arrays) // 2

    def one(t, carry):
        for u in range(units):
            size = UNITS[u % len(UNITS)]

            @pl.when(table_ref[0, t] == u)
            def _():
                for k in BOTH:
                    for d in BOTH:
                        pltpu.make_async_copy(arrays[2 * u + d].at[table_ref[1, t] + k * size], outs[k].at[d * HALF + t], sem).start()
        return carry

    def wait(t, carry):
        @pl.when(table_ref[0, t] >= 0)
        def _():
            for k in BOTH:
                for d in BOTH:
                    pltpu.make_async_copy(outs[k].at[d * HALF + t], outs[k].at[d * HALF + t], sem).wait()

        return carry

    lax.fori_loop(0, HALF, one, 0)
    lax.fori_loop(0, HALF, wait, 0)


def hand_back(table, pairs):
    arrays = [x for pair in pairs for x in pair]
    return pl.pallas_call(
        hand_back_kernel,
        grid_spec=pltpu.PrefetchScalarGridSpec(
            num_scalar_prefetch=1, grid=(1,), in_specs=[ANYWHERE] * len(arrays),
            out_specs=[pl.BlockSpec((CROSS, GRAN, HEAD), lambda i, t_ref: (0, 0, 0))] * 2, scratch_shapes=[pltpu.SemaphoreType.DMA]),
        out_shape=[jax.ShapeDtypeStruct((CROSS, GRAN, HEAD), jnp.bfloat16)] * 2,
        compiler_params=pltpu.CompilerParams(vmem_limit_bytes=VMEM_LIMIT),
        cost_estimate=cost(8_000_000),
        name="hand_back",
    )(table, *arrays)


def solution(mesh):
    head_spec = P('dp', None, 'sh', None)
    row_spec = P(('dp', 'sh'))
    full_spec = P(None, None)

    def send(x, d):
        return lax.ppermute(x, 'sh', [(i, i ^ d) for i in range(WAYS)])

    def across(x):
        return lax.ppermute(x, 'dp', [(0, 1), (1, 0)])

    def step(k_prefill, v_prefill, lengths, residual, norm_gain, w_query, w_key, w_value, w_out):
        seq_g = k_prefill.shape[1] // GRAN
        me = lax.axis_index('sh').astype(jnp.int32)
        peers = me ^ jnp.arange(WAYS, dtype=jnp.int32)
        by_peer = lengths[(peers[:, None] * ROWS + jnp.arange(ROWS, dtype=jnp.int32)).reshape(-1)].reshape(WAYS, ROWS)
        mine = by_peer[0]
        prefill = {True: k_prefill.reshape(-1, GRAN, HEAD), False: v_prefill.reshape(-1, GRAN, HEAD)}

        def lists(*ds):
            return Lists(jnp.stack([by_peer[d] for d in ds]), jnp.stack([(me ^ d) * ROWS for d in ds])[:, None], seq_g)

        def span(count):
            return lax.broadcasted_iota(jnp.int32, (1, count), 1)

        def held(which, i):
            src, mixed = which.source(i)
            valid = i < which.size
            return jnp.where(valid, src, 0), jnp.where(valid, mixed, -1)

        far, close, self_list = lists(2, 3), lists(1, 0), lists(0)
        fixed_src, fixed_mix = held(far, span(FIXED))
        close_src, close_mix = held(close, span(ROWS * WIN_G))

        chip, core = me // 2, me % 2

        def rests(lens):
            sizes = jnp.sum(jnp.minimum(lens // GRAN + 1, WIN_G).reshape(WAYS, ROWS), axis=1)
            return jnp.maximum(sizes - FIXED, 0).reshape(WAYS // 2, 2)

        def of_chip(x, c):
            return jnp.where(c == 0, x[0], x[1])

        other_lengths = across(lengths)
        rest, other_rest = rests(lengths), rests(other_lengths)
        need, other_need = jnp.sum(rest, axis=1), jnp.sum(other_rest, axis=1)
        level = jnp.max(jnp.maximum((need + other_need + 4 * QUANTUM - 1) // (4 * QUANTUM), (jnp.maximum(need, other_need) - CROSS + 2 * QUANTUM - 1) // (2 * QUANTUM)))
        spare = QUANTUM * level
        on = active_units(level)
        column = span(SPARE)
        unit = functools.reduce(jnp.add, [(column >= s).astype(jnp.int32) for s in starts_of(UNITS)[1:]])
        skipped, used, place = 0, jnp.zeros_like(column, dtype=bool), column
        for u, size in enumerate(UNITS):
            used = jnp.where(unit == u, on[u], used)
            place = jnp.where(unit == u, column - skipped, place)
            skipped = skipped + jnp.where(on[u], 0, size)
        used = used & (column < sum(UNITS))
        far_n = lax.dynamic_slice_in_dim(lengths, (1 - chip) * 2 * ROWS, 2 * ROWS).reshape(2, ROWS)
        far_lists = Lists(far_n, ((1 - chip) * 2 + jnp.arange(2, dtype=jnp.int32))[:, None] * ROWS, seq_g)
        far_first, far_need = of_chip(rest, 1 - chip)[0], of_chip(need, 1 - chip)
        far_guests = jnp.maximum(of_chip(other_need, 1 - chip) - 2 * spare, 0)

        def from_rest(c):
            second = c >= far_first
            src, mixed = far_lists.source(FIXED + c - jnp.where(second, far_first, 0))
            return tuple(jnp.where(second[0], x[1], x[0]) for x in (src, mixed))

        both_used = beside([used, used])[0]
        z = beside([place + (core ^ a) * spare for a in BOTH])
        src, mixed = from_rest(z)
        order = z[0] - far_need
        hosted, guest = both_used & (order < 0), both_used & (order >= 0) & (order < far_guests)
        spare_src = jnp.where(hosted, src, jnp.where(guest, ELSEWHERE + order, 0)).reshape(2, SPARE)
        spare_mix = jnp.where(hosted, mixed, -1).reshape(2, SPARE)
        z = 2 * spare + span(CROSS)
        src, mixed = from_rest(z)
        hosted = z[0] < far_need
        cross_src, cross_mix = jnp.where(hosted, src, 0).reshape(2, HALF), jnp.where(hosted, mixed, -1).reshape(2, HALF)

        own_first, own_need = of_chip(rest, chip)[0], of_chip(need, chip)

        def belongs(i, valid):
            r, g = self_list.at(i)
            return jnp.where(valid & (i < self_list.size), r * WIN_G + g, -1), jnp.clip(i, 0, ROWS * WIN_G - 1)

        def rest_belongs(c, valid):
            second = c >= own_first
            return belongs(FIXED + c - jnp.where(second, own_first, 0), valid & (c < own_need) & (second == (core == 1)))

        half_span = span(HALF)
        parts = [belongs(span(FIXED), True), rest_belongs(place + core * spare, used), rest_belongs(place + (1 - core) * spare, used)]
        parts += [rest_belongs(2 * spare + x * (HALF) + half_span, True) for x in (core, 1 - core)]
        codes = beside([p[0] for p in parts])
        places = beside([p[1] for p in parts])

        w = core * (HALF) + half_span
        z = own_need + w
        high = (z >= spare).astype(jnp.int32)
        u = z - high * spare
        back_unit, back_at, begin = jnp.full_like(u, -1), jnp.zeros_like(u), 0
        for k, size in enumerate(UNITS):
            inside = (u >= begin) & (u < begin + jnp.where(on[k], size, 0))
            back_unit = jnp.where(inside, k, back_unit)
            back_at = jnp.where(inside, u - begin, back_at)
            begin = begin + jnp.where(on[k], size, 0)
        back_unit = jnp.where(w < jnp.maximum(of_chip(other_need, chip) - 2 * spare, 0), back_unit + len(UNITS) * (high != core).astype(jnp.int32), -1)
        back_table = jnp.concatenate([back_unit, back_at], axis=0)

        fixed_from, close_from = FromTable(fixed_src, fixed_mix), FromTable(close_src, close_mix)
        spare_from, cross_from = FromTable(spare_src, spare_mix), FromTable(cross_src, cross_mix)
        fixed_got = {True: [], False: []}
        packed_values = []
        for i, (base, count) in enumerate(zip(starts_of(K_PIECES), K_PIECES)):
            out = pack([prefill[True]], FromLengths(lengths, seq_g) if i == 0 else fixed_from, base, count)
            a = send(out[0], 2)
            b = send(out[1], 3)
            fixed_got[True].append((a, b))
        cross = pack([prefill[True], prefill[False]], cross_from, 0, HALF)
        guests = []
        for e in BOTH:
            guests.append(across(cross[e]))
        close_got = {}
        for is_key in KV:
            near, own = pack([prefill[is_key]], close_from, 0, ROWS * WIN_G)
            close_got[is_key] = (send(near, 1), own)
        spare_packed = [pack([prefill[True], prefill[False]], spare_from, base, count, guests) for base, count in zip(starts_of(UNITS), UNITS)]
        for base, count in zip(starts_of(V_PIECES), V_PIECES):
            packed_values.append(pack([prefill[False]], fixed_from, base, count))

        residual, cross = lax.optimization_barrier((residual, cross))
        resid_f32 = residual.astype(jnp.float32)
        inv_rms = lax.rsqrt(jnp.mean(resid_f32 * resid_f32, axis=-1, keepdims=True) + EPS)
        normed = (resid_f32 * inv_rms * norm_gain.astype(jnp.float32)).astype(jnp.bfloat16)
        q_group = w_query.shape[1] // (WAYS * HEAD)
        q_heads = jnp.dot(normed, w_query, preferred_element_type=jnp.float32).astype(jnp.bfloat16).reshape(ROWS, WAYS, q_group, HEAD)
        k_new = jnp.dot(normed, w_key, preferred_element_type=jnp.float32).astype(jnp.bfloat16).reshape(ROWS, WAYS, HEAD)
        v_new = jnp.dot(normed, w_value, preferred_element_type=jnp.float32).astype(jnp.bfloat16).reshape(ROWS, WAYS, HEAD)
        q_heads = rotate(q_heads, mine)
        k_new = rotate(k_new, mine)
        new = {True: k_new.astype(jnp.float32).reshape(-1, 1, HEAD), False: v_new.astype(jnp.float32).reshape(-1, 1, HEAD)}
        q_pad = jnp.pad(q_heads.transpose(1, 0, 2, 3).reshape(WAYS, ROWS * q_group, HEAD), ((0, 0), (0, 8 - ROWS * q_group), (0, 0)))
        caches = cleared(mine, (ROWS, WINDOW, WAYS, HEAD))
        scores = blank((WAYS, 8, codes.shape[1] * GRAN), jnp.float32)

        def branch(lvl):
            keep = [bool(x) for x in active_units(lvl)]

            def run(pairs):
                return [(send(a, 2), send(b, 3)) if k else (blank(a.shape, a.dtype), blank(b.shape, b.dtype)) for k, (a, b) in zip(keep, pairs)]

            return run

        spare_packed, packed_values, ready = lax.optimization_barrier((spare_packed, packed_values, (new, q_pad, scores, caches, close_got[True][1], close_got[False][1])))
        new, q_pad, scores, (k_cache, v_cache), own_k, own_v = ready
        own = {True: own_k, False: own_v}
        spare_got = lax.switch(level, [branch(x) for x in range(LEVELS)], spare_packed)
        spare_got, packed_values = lax.optimization_barrier((spare_got, packed_values))
        for a, b in packed_values:
            a = send(a, 2)
            b = send(b, 3)
            fixed_got[False].append((a, b))
        forwarded = [(send(b, 1), send(a, 1)) for a, b in spare_got]
        found = hand_back(back_table, spare_got + forwarded)
        handed, handed_on = [], []
        for k in BOTH:
            handed.append(across(found[k]))
            handed_on.append(send(handed[k], 1))

        me1 = me.reshape(1)

        def run(is_key, base, far_parts, qp, prev, cache, projection=()):
            return assemble(is_key, base, codes, places, mine, me1, far_parts, close_got[is_key][0], own[is_key], new[is_key], qp, prev, cache, projection)

        def fixed(pieces, got):
            return [(a, b, (0, 0), count) for (a, b), count in zip(got, pieces)]

        def spares(is_key):
            runs = []
            for got in (spare_got, forwarded):
                runs += [(a, b, (0, 0) if is_key else (count, count), count) for (a, b), count in zip(got, UNITS)]
                runs.append(runs[-1])
            return runs

        def returned(is_key):
            own_half, other_half = handed[0 if is_key else 1], handed_on[0 if is_key else 1]
            return [(own_half, own_half, (0, HALF), HALF), (other_half, other_half, (HALF, 0), HALF)]


        k_cache, scores = run(True, 0, fixed(K_PIECES, fixed_got[True]), q_pad, scores, k_cache)
        k_cache, scores = run(True, FIXED, spares(True), q_pad, scores, k_cache)
        k_cache, scores = run(True, FIXED + 2 * SPARE, returned(True), q_pad, scores, k_cache)
        exp_scores = jnp.exp(scores - jnp.max(scores, axis=-1, keepdims=True))
        weights = (exp_scores / jnp.sum(exp_scores, axis=-1, keepdims=True)).astype(jnp.bfloat16)
        sums = jnp.zeros((WAYS, 8, HEAD), jnp.float32)
        v_cache, sums = run(False, FIXED, spares(False), weights, sums, v_cache)
        v_cache, sums = run(False, FIXED + 2 * SPARE, returned(False), weights, sums, v_cache)
        *values, last = zip(starts_of(V_PIECES), fixed(V_PIECES, fixed_got[False]))
        for base, part in values:
            v_cache, sums = run(False, base, [part], weights, sums, v_cache)
        v_cache, resid_out = run(False, last[0], [last[1]], weights, sums, v_cache, (w_out, resid_f32))
        return resid_out, k_cache, v_cache

    return jax.shard_map(
        step, mesh=mesh, in_specs=(head_spec, head_spec, P('dp'), P(('dp', 'sh'), None), P(None), full_spec, full_spec, full_spec, full_spec),
        out_specs=(P(('dp', 'sh'), None), row_spec, row_spec), check_vma=False)
```
